256 devices in a mesh: gx: 8 (over z), gy: 4 (over y), gz: 8 (over x, core).
Axes of the slice: x: 4, y: 4, z: 8, core: 2. Of those that a mesh axis runs over, the one named last changes fastest.
Arguments:
- right_side: float32 [4, 192, 96, 192], P(None, 'gx', 'gy', 'gz'), may hold values from -6 to 6
- iterate: float32 [4, 192, 96, 192], P(None, 'gx', 'gy', 'gz'), may hold values from -6 to 6
- coefficient: float32 [192, 96, 192], P('gx', 'gy', 'gz'), may hold values from 0.1 to 2
- ordering: int32 [8, 4, 8, 216], P('gx', 'gy', 'gz'), may hold values from 0 to 215, as said below
- leaf_inverse: float32 [8, 4, 8, 125, 125], P('gx', 'gy', 'gz'), may hold values from -2 to 3
- leaf_first: float32 [8, 4, 8, 125, 50], P('gx', 'gy', 'gz'), may hold values from -0.5 to 0.5
- leaf_second: float32 [8, 4, 8, 125, 60], P('gx', 'gy', 'gz'), may hold values from -0.5 to 0.5
- leaf_top: float32 [8, 4, 8, 125, 72], P('gx', 'gy', 'gz'), may hold values from -0.5 to 0.5
- first_inverse: float32 [8, 4, 200, 200], P('gx', 'gy', 'gz'), may hold values from -2 to 3
- first_second: float32 [8, 4, 8, 25, 60], P('gx', 'gy', 'gz'), may hold values from -1.25 to 1.25
- first_top: float32 [8, 4, 8, 25, 72], P('gx', 'gy', 'gz'), may hold values from -1.25 to 1.25
- second_inverse: float32 [8, 960, 960], P('gx', ('gy', 'gz')), may hold values from -2 to 3
- second_top: float32 [8, 4, 8, 30, 72], P('gx', 'gy', 'gz'), may hold values from -1 to 1
- top_inverse: float32 [9216, 9216], P(('gx', 'gy', 'gz')), may hold values from -2 to 3
Outputs:
- correction: float32 [4, 192, 96, 192], P(None, 'gx', 'gy', 'gz')
The draws below stay inside these ranges and needn't reach their ends.
Inputs may be any that keep to these rules, and one draw needn't show every extreme that they name: `ordering`: each device's row names each of its 216 coarse cells once (cell x 6^2 + y * 6 + z): first the 125 cells with x, y and z all below 5, then the 25 cells with z = 5 and x, y below it, then the 30 cells with y = 5 and x below it, then the 36 cells with x = 5, each group in any order.
All inputs are finite; a program needn't handle non-finite values.
Results may differ from the reference program's by a relative error of at most 0.0003.
Values sent between devices are 32-bit elements; how exact they have to be, the bound alone decides.
No kernel may reach another device: no remote copies, remote signals or barrier semaphores. Data moves between devices by JAX's collectives and lax.ppermute only.
A program may use at most 64 MiB of HBM per device.

```python
import math
import jax
import jax.numpy as jnp
from jax import lax

NRHS = 4
SIDE = 6
COARSE_DEV = 216
FIRST_DEV = 25
SECOND_DEV = 30
TOP_DEV = 36
LEAF = 125
FIRST_SEP = 200
SECOND_SEP = 960
TOP_SEP = 9216
NX = 192
NY = 96
NZ = 192
N_GX = 8
N_GY = 4
N_GZ = 8


def inverse_block(key, leading, extent):
    full_shape = tuple(leading) + (extent, extent)
    jitter = jnp.clip(jax.random.normal(key, full_shape, jnp.float32), -4.0, 4.0) * 0.5
    return jnp.eye(extent, dtype=jnp.float32) + jitter / extent ** 0.5


def draw_leaf_inverse(key, part):
    return inverse_block(jax.random.fold_in(key, 11), (N_GX, N_GY, N_GZ), LEAF)


def draw_first_inverse(key, part):
    return inverse_block(jax.random.fold_in(key, 23), (N_GX, N_GY), FIRST_SEP)


def draw_second_inverse(key, part):
    return inverse_block(jax.random.fold_in(key, 37), (N_GX,), SECOND_SEP)


def draw_top_inverse(key, part):
    return inverse_block(jax.random.fold_in(key, 41), (), TOP_SEP)


def draw_ordering(key, part):
    cells = jnp.arange(COARSE_DEV, dtype=jnp.int32)
    first_coord = cells // (SIDE * SIDE)
    second_coord = cells // SIDE % SIDE
    third_coord = cells % SIDE
    edge = SIDE - 1
    classes = jnp.where(first_coord == edge, 3, jnp.where(second_coord == edge, 2, jnp.where(third_coord == edge, 1, 0))).astype(jnp.int32)
    subkeys = jax.random.split(jax.random.fold_in(key, 53), N_GX * N_GY * N_GZ)

    def one_row(subkey):
        shuffled = jax.random.permutation(subkey, COARSE_DEV).astype(jnp.int32)
        rank = jnp.argsort(classes[shuffled], stable=True)
        return shuffled[rank].astype(jnp.int32)
    return jax.vmap(one_row)(subkeys).reshape(N_GX, N_GY, N_GZ, COARSE_DEV)


def levels(own_key, dims, shards, low, top_value):
    factor_of = 1.0
    for axis_at, blocks in shards:
        draws = jax.random.uniform(jax.random.fold_in(jax.random.fold_in(own_key, 6), axis_at), (blocks,), jnp.float32, low / len(shards), top_value / len(shards))
        factor_of = factor_of * jnp.repeat(jnp.exp(draws), dims[axis_at] // blocks).reshape((-1,) + (1,) * (len(dims) - 1 - axis_at))
    return factor_of


def normal_values(stream_key, dims, scale, most, cuts=(), kind=jnp.bfloat16):
    gain = levels(stream_key, dims, cuts, -0.22, 0.18) if cuts else 1.0
    drawn = jax.random.normal(stream_key, dims, jnp.float32) * scale * gain
    return jnp.minimum(jnp.maximum(drawn, -most), most).astype(kind)


def setup_inputs(seed: int = 0) -> dict:
    keys = jax.random.split(jax.random.key(seed), 15)
    return {
        "right_side": normal_values(keys[0], (NRHS, NX, NY, NZ), 1.0, 6.0, ((1, 8), (2, 4), (3, 8)), jnp.float32),
        "iterate": normal_values(keys[1], (NRHS, NX, NY, NZ), 1.0, 6.0, ((1, 8), (2, 4), (3, 8)), jnp.float32),
        "coefficient": jnp.clip(jnp.exp(math.log(2.0) - 2.9957323 * jax.random.uniform(keys[2], (NX, NY, NZ), jnp.float32) ** levels(keys[2], (NX, NY, NZ), ((0, 8), (1, 4), (2, 8)), -0.2, 0.2)), 0.1, 2.0),
        "ordering": draw_ordering(jax.random.fold_in(keys[14], 71), 0),
        "leaf_inverse": draw_leaf_inverse(jax.random.fold_in(keys[14], 71), 0),
        "leaf_first": normal_values(keys[5], (N_GX, N_GY, N_GZ, LEAF, 2 * FIRST_DEV), LEAF ** -0.5, 0.5, ((0, 8), (1, 4), (2, 8)), jnp.float32),
        "leaf_second": normal_values(keys[6], (N_GX, N_GY, N_GZ, LEAF, 2 * SECOND_DEV), LEAF ** -0.5, 0.5, ((0, 8), (1, 4), (2, 8)), jnp.float32),
        "leaf_top": normal_values(keys[7], (N_GX, N_GY, N_GZ, LEAF, 2 * TOP_DEV), LEAF ** -0.5, 0.5, ((0, 8), (1, 4), (2, 8)), jnp.float32),
        "first_inverse": draw_first_inverse(jax.random.fold_in(keys[14], 71), 0),
        "first_second": normal_values(keys[9], (N_GX, N_GY, N_GZ, FIRST_DEV, 2 * SECOND_DEV), FIRST_DEV ** -0.5, 1.25, ((0, 8), (1, 4), (2, 8)), jnp.float32),
        "first_top": normal_values(keys[10], (N_GX, N_GY, N_GZ, FIRST_DEV, 2 * TOP_DEV), FIRST_DEV ** -0.5, 1.25, ((0, 8), (1, 4), (2, 8)), jnp.float32),
        "second_inverse": draw_second_inverse(jax.random.fold_in(keys[14], 71), 0),
        "second_top": normal_values(keys[12], (N_GX, N_GY, N_GZ, SECOND_DEV, 2 * TOP_DEV), SECOND_DEV ** -0.5, 1.0, ((0, 8), (1, 4), (2, 8)), jnp.float32),
        "top_inverse": draw_top_inverse(jax.random.fold_in(keys[14], 71), 0),
    }


precise = lax.Precision.HIGHEST


def contract(pattern, operand, matrix):
    return jnp.einsum(pattern, operand, matrix, precision=precise, preferred_element_type=jnp.float32)


def weigh(extended, dimension):
    length = extended.shape[dimension] - 1
    previous = lax.slice_in_dim(extended, 0, length, 2, dimension)
    centre = lax.slice_in_dim(extended, 1, length + 1, 2, dimension)
    following = lax.slice_in_dim(extended, 2, length + 1, 2, dimension)
    return 0.25 * previous + 0.5 * centre + 0.25 * following


def spread(extended, dimension):
    length = extended.shape[dimension] - 1
    current = lax.slice_in_dim(extended, 0, length, 1, dimension)
    following = lax.slice_in_dim(extended, 1, length + 1, 1, dimension)
    paired = jnp.stack([current, 0.5 * (current + following)], axis=dimension + 1)
    new_shape = list(current.shape)
    new_shape[dimension] = 2 * length
    return paired.reshape(new_shape)


def restrict(values):
    extended = jnp.pad(values, ((0, 0), (1, 0), (1, 0), (1, 0)))
    for dimension in (1, 2, 3):
        extended = weigh(extended, dimension)
    return extended


def prolong(values):
    extended = jnp.pad(values, ((0, 0), (0, 1), (0, 1), (0, 1)))
    for dimension in (1, 2, 3):
        extended = spread(extended, dimension)
    return extended


def residual_of(right_side, iterate, coefficient):
    padded = jnp.pad(iterate, ((0, 0), (1, 1), (1, 1), (1, 1)))
    beside = padded[:, 2:, 1:-1, 1:-1] + padded[:, :-2, 1:-1, 1:-1]
    beside = beside + padded[:, 1:-1, 2:, 1:-1] + padded[:, 1:-1, :-2, 1:-1]
    beside = beside + padded[:, 1:-1, 1:-1, 2:] + padded[:, 1:-1, 1:-1, :-2]
    return right_side - ((6.0 + coefficient) * iterate - beside)


def from_above(values, axis):
    length = values.shape[axis]
    kept = lax.slice_in_dim(values, 1, length, 1, axis)
    widths = [(0, 0)] * values.ndim
    widths[axis] = (0, 1)
    return jnp.pad(kept, widths)


def from_below(values, axis):
    length = values.shape[axis]
    kept = lax.slice_in_dim(values, 0, length - 1, 1, axis)
    widths = [(0, 0)] * values.ndim
    widths[axis] = (1, 0)
    return jnp.pad(kept, widths)


def reference(right_side, iterate, coefficient, ordering, leaf_inverse, leaf_first, leaf_second, leaf_top, first_inverse, first_second, first_top, second_inverse, second_top, top_inverse):
    coarse = restrict(restrict(residual_of(right_side, iterate, coefficient)))
    blocks = coarse.reshape(NRHS, N_GX, SIDE, N_GY, SIDE, N_GZ, SIDE)
    blocks = blocks.transpose(0, 1, 3, 5, 2, 4, 6).reshape(NRHS, N_GX, N_GY, N_GZ, COARSE_DEV)
    chosen = jnp.take_along_axis(blocks, jnp.broadcast_to(ordering[None], blocks.shape), axis=4)
    first_end = LEAF + FIRST_DEV
    second_end = first_end + SECOND_DEV
    leaf_rhs = chosen[..., :LEAF]
    first_rhs = chosen[..., LEAF:first_end]
    second_rhs = chosen[..., first_end:second_end]
    top_rhs = chosen[..., second_end:]

    leaf_solved = contract('rabcl,abclk->rabck', leaf_rhs, leaf_inverse)
    toward = contract('rabcl,abclk->rabck', leaf_solved, leaf_first)
    first_target = first_rhs - toward[..., :FIRST_DEV] - from_above(toward[..., FIRST_DEV:], 3)
    first_target = first_target.reshape(NRHS, N_GX, N_GY, FIRST_SEP)
    first_solved = contract('rabi,abik->rabk', first_target, first_inverse).reshape(NRHS, N_GX, N_GY, N_GZ, FIRST_DEV)

    toward = contract('rabcl,abclk->rabck', leaf_solved, leaf_second) + contract('rabcl,abclk->rabck', first_solved, first_second)
    second_target = second_rhs - toward[..., :SECOND_DEV] - from_above(toward[..., SECOND_DEV:], 2)
    second_target = second_target.reshape(NRHS, N_GX, SECOND_SEP)
    second_solved = contract('rai,aik->rak', second_target, second_inverse).reshape(NRHS, N_GX, N_GY, N_GZ, SECOND_DEV)

    toward = contract('rabcl,abclk->rabck', leaf_solved, leaf_top) + contract('rabcl,abclk->rabck', first_solved, first_top)
    toward = toward + contract('rabcl,abclk->rabck', second_solved, second_top)
    top_target = top_rhs - toward[..., :TOP_DEV] - from_above(toward[..., TOP_DEV:], 1)
    top_target = top_target.reshape(NRHS, TOP_SEP)
    top_solved = contract('ri,ik->rk', top_target, top_inverse)

    top_back = contract('rk,ik->ri', top_solved, top_inverse).reshape(NRHS, N_GX, N_GY, N_GZ, TOP_DEV)
    top_pair = jnp.concatenate([top_back, from_below(top_back, 1)], axis=4)
    second_gap = second_solved - contract('rabck,abcik->rabci', top_pair, second_top)
    second_gap = second_gap.reshape(NRHS, N_GX, SECOND_SEP)
    second_back = contract('rak,aik->rai', second_gap, second_inverse).reshape(NRHS, N_GX, N_GY, N_GZ, SECOND_DEV)
    second_pair = jnp.concatenate([second_back, from_below(second_back, 2)], axis=4)
    first_gap = first_solved - contract('rabck,abcik->rabci', second_pair, first_second)
    first_gap = first_gap - contract('rabck,abcik->rabci', top_pair, first_top)
    first_gap = first_gap.reshape(NRHS, N_GX, N_GY, FIRST_SEP)
    first_back = contract('rabk,abik->rabi', first_gap, first_inverse).reshape(NRHS, N_GX, N_GY, N_GZ, FIRST_DEV)
    first_pair = jnp.concatenate([first_back, from_below(first_back, 3)], axis=4)
    leaf_gap = leaf_solved - contract('rabck,abcik->rabci', first_pair, leaf_first)
    leaf_gap = leaf_gap - contract('rabck,abcik->rabci', second_pair, leaf_second)
    leaf_gap = leaf_gap - contract('rabck,abcik->rabci', top_pair, leaf_top)
    leaf_back = contract('rabck,abclk->rabcl', leaf_gap, leaf_inverse)

    ordered = jnp.concatenate([leaf_back, first_back, second_back, top_back], axis=4)
    inverse_order = jnp.argsort(ordering, axis=-1).astype(jnp.int32)
    listed = jnp.take_along_axis(ordered, jnp.broadcast_to(inverse_order[None], ordered.shape), axis=4)
    listed = listed.reshape(NRHS, N_GX, N_GY, N_GZ, SIDE, SIDE, SIDE)
    coarse_grid = listed.transpose(0, 1, 4, 2, 5, 3, 6).reshape(NRHS, N_GX * SIDE, N_GY * SIDE, N_GZ * SIDE)
    return prolong(prolong(coarse_grid))
```

```python
import numpy as np
import jax
import jax.numpy as jnp
from jax import lax
from jax.experimental import pallas as pl
from jax.experimental.pallas import tpu as pltpu
from jax.sharding import PartitionSpec as P

PLANE = ("gy", "gz")
precise = lax.Precision.HIGHEST


def shifted(shard, axis, by):
    peers = lax.axis_size(axis)
    pairs = [(i, i + by) for i in range(peers) if 0 <= i + by < peers]
    return lax.ppermute(shard, axis, pairs)


def exchanged(pieces, axis):
    return lax.all_to_all(pieces, axis, split_axis=0, concat_axis=0, tiled=True)


def sent_to_all(shard, axis):
    copies = jnp.broadcast_to(shard, (lax.axis_size(axis), *shard.shape))
    return exchanged(copies, axis)


def product(operand, matrix):
    return jnp.dot(operand, matrix, precision=precise, preferred_element_type=jnp.float32)


def product_back(operand, matrix):
    return lax.dot_general(
        operand,
        matrix,
        (((1,), (1,)), ((), ())),
        precision=precise,
        preferred_element_type=jnp.float32,
    )


def two_restrictions(distance):
    return np.maximum(0.0, 4.0 - np.abs(distance)) / 16.0


def restriction_weights(fine):
    cell = 4.0 * (np.arange(fine // 4 + 2) - 1)[:, None]
    at = np.arange(fine)[None, :]
    own = two_restrictions(cell - at)
    through_before = two_restrictions(cell - (at - 1))
    beside = through_before + two_restrictions(cell - (at + 1))
    before = np.where(at == 0, through_before, 0.0)
    return own, beside, before


def prolongation_weights(fine):
    at = np.arange(fine)[:, None] / 4.0
    cell = np.arange(fine // 4 + 1)[None, :]
    return np.maximum(0.0, 1.0 - np.abs(at - cell))


def by_lane(weights, count):
    coarse, fine = weights.shape
    out = np.zeros((count, fine, coarse, count), np.float32)
    for r in range(count):
        out[r, :, :, r] = weights.T
    return out.reshape(count, fine, coarse * count)


def parts_of(values):
    first = values.astype(jnp.bfloat16)
    rest = values - first.astype(jnp.float32)
    second = rest.astype(jnp.bfloat16)
    third = (rest - second.astype(jnp.float32)).astype(jnp.bfloat16)
    return first, second, third


def dot(left, right):
    return jnp.dot(left, right, preferred_element_type=jnp.float32)


def times_weights(values, weights):
    first, second, third = parts_of(values)
    return dot(first, weights) + (dot(second, weights) + dot(third, weights))


def weights_times(weights, values):
    first, second, third = parts_of(values)
    return dot(weights, first) + (dot(weights, second) + dot(weights, third))


def restrict_body(
    own, beside, before, edge, rhs, iterate, coefficient, z_own, z_beside, z_before,
    y_own, y_beside, y_before, out,
):
    count, fine = rhs.shape[:2]
    coarse = own.shape[0]
    at_x, at_y, at_z = edge[0], edge[1], edge[2]
    beside_sum = None
    own_sum = None
    for r in range(count):
        planes = [iterate[r, x] for x in range(fine)]
        gaps = [rhs[r, x] - (6.0 + coefficient[x]) * planes[x] for x in range(fine)]
        values, cells = [], []
        for i in range(coarse):
            value = cell = None
            for x in range(fine):
                if own[i, x]:
                    term = float(own[i, x]) * gaps[x]
                    value = term if value is None else value + term
                    term = float(own[i, x]) * planes[x]
                    cell = term if cell is None else cell + term
                if beside[i, x]:
                    weight = float(beside[i, x])
                    if before[i, x]:
                        weight = weight - at_x * float(before[i, x])
                    term = weight * planes[x]
                    value = term if value is None else value + term
            values.append(value)
            cells.append(jnp.zeros_like(planes[0]) if cell is None else cell)
        value = jnp.concatenate(values, axis=0)
        cell = jnp.concatenate(cells, axis=0)
        z_pair = (z_beside[r] - at_z * z_before[r]).astype(jnp.bfloat16)
        z_cell = z_own[r].astype(jnp.bfloat16)
        term = times_weights(value, z_cell) + times_weights(cell, z_pair)
        beside_sum = term if beside_sum is None else beside_sum + term
        term = times_weights(cell, z_cell)
        own_sum = term if own_sum is None else own_sum + term
    y_pair = (y_beside[...] - at_y * y_before[...]).astype(jnp.bfloat16)
    y_cell = y_own[...].astype(jnp.bfloat16)
    result = weights_times(y_cell, beside_sum) + weights_times(y_pair, own_sum)
    out[...] = result.reshape(out.shape)


def restricted(edge, right_side, iterate, coefficient):
    count, fine = right_side.shape[:2]
    own, beside, before = restriction_weights(fine)
    coarse = own.shape[0]
    lanes = [by_lane(w, count) for w in (own, beside, before)]
    rows = [np.kron(np.eye(coarse), w).astype(np.float32) for w in (own, beside, before)]

    def body(*refs):
        restrict_body(own, beside, before, *refs)

    vmem = pl.BlockSpec(memory_space=pltpu.VMEM)
    return pl.pallas_call(
        body,
        out_shape=jax.ShapeDtypeStruct((coarse, coarse, coarse * count), jnp.float32),
        in_specs=[pl.BlockSpec(memory_space=pltpu.SMEM)] + [vmem] * 9,
        out_specs=vmem,
        name="restrict_twice",
    )(edge, right_side, iterate, coefficient, *lanes, *rows)


def prolong_body(window, y_weights, z_weights, out):
    count, fine = out.shape[:2]
    cells = window.shape[0]
    flat = window[...].reshape(cells * window.shape[1], window.shape[2])
    along_y = weights_times(y_weights[...].astype(jnp.bfloat16), flat)
    for r in range(count):
        along_z = times_weights(along_y, z_weights[r].astype(jnp.bfloat16))
        planes = [along_z[i * fine : (i + 1) * fine] for i in range(cells)]
        for i in range(cells - 1):
            for q in range(4):
                value = planes[i]
                if q:
                    value = (1.0 - q / 4.0) * value + (q / 4.0) * planes[i + 1]
                out[r, 4 * i + q] = value


def prolonged(window, count, fine):
    cells = window.shape[0]
    weights = prolongation_weights(fine)
    along_y = np.zeros((fine, window.shape[1]))
    along_y[:, :cells] = weights
    rows = np.kron(np.eye(cells), along_y).astype(np.float32)
    lanes = np.zeros((count, window.shape[2], fine), np.float32)
    for r in range(count):
        for k in range(cells):
            lanes[r, k * count + r] = weights[:, k]
    vmem = pl.BlockSpec(memory_space=pltpu.VMEM)
    return pl.pallas_call(
        prolong_body,
        out_shape=jax.ShapeDtypeStruct((count, fine, fine, fine), jnp.float32),
        in_specs=[vmem] * 3,
        out_specs=vmem,
        name="prolong_twice",
    )(window, rows, lanes)


def padded(values, dim, before, after):
    widths = [(0, 0)] * values.ndim
    widths[dim] = (before, after)
    return jnp.pad(values, widths)


def with_neighbours(values, axis, dim, width):
    length = values.shape[dim]
    first = lax.slice_in_dim(values, 0, width, axis=dim)
    last = lax.slice_in_dim(values, length - width, length, axis=dim)
    from_below = shifted(last, axis, 1)
    from_above = shifted(first, axis, -1)
    inner = lax.slice_in_dim(values, width, length - width, axis=dim)
    room = length - 3 * width
    return inner + padded(from_below, dim, 0, room) + padded(from_above, dim, room, 0)


def with_next(values, axis, dim, width):
    first = lax.slice_in_dim(values, 0, width, axis=dim)
    return jnp.concatenate([values, shifted(first, axis, -1)], axis=dim)


def per_device(
    right_side,
    iterate,
    coefficient,
    ordering,
    leaf_inverse,
    leaf_first,
    leaf_second,
    leaf_top,
    first_inverse,
    first_second,
    first_top,
    second_inverse,
    second_top,
    top_inverse,
):
    count, fine = right_side.shape[:2]
    leaf_size = leaf_inverse.shape[-1]
    first_size = first_second.shape[3]
    second_size = second_top.shape[3]
    top_total = top_inverse.shape[1]
    top_size = top_inverse.shape[0]
    side = fine // 4
    cells = side**3
    first_rows = first_inverse[0, 0]
    second_rows = second_inverse[0]
    to_first = leaf_first[0, 0, 0]
    to_second = leaf_second[0, 0, 0]
    to_top = leaf_top[0, 0, 0]
    first_to_second = first_second[0, 0, 0]
    first_to_top = first_top[0, 0, 0]
    second_to_top = second_top[0, 0, 0]
    leaf_block = leaf_inverse[0, 0, 0]

    edge = jnp.stack([lax.axis_index(a) == 0 for a in ("gx", "gy", "gz")]).astype(jnp.float32)
    partial = restricted(edge, right_side, iterate, coefficient)
    coarse = with_neighbours(partial, "gx", 0, 1)
    first_below = shifted(first_rows, "gz", 1)
    second_below = shifted(second_rows, "gy", 1)
    top_rows, coarse = lax.optimization_barrier((top_inverse, coarse))
    top_below = shifted(top_rows, "gx", 1)
    coarse = with_neighbours(coarse, "gy", 1, 1)
    coarse = with_neighbours(coarse, "gz", 2, count)
    natural = coarse.reshape(cells, count).T

    chosen_at = ordering.reshape(-1)[:, None] == jnp.arange(cells, dtype=jnp.int32)[None, :]
    pick = chosen_at.astype(jnp.float32)
    chosen = product_back(natural, pick)
    first_end = leaf_size + first_size
    second_end = first_end + second_size
    leaf_rhs = chosen[:, :leaf_size]
    first_rhs = chosen[:, leaf_size:first_end]
    second_rhs = chosen[:, first_end:second_end]
    top_rhs = chosen[:, second_end:]

    leaf_solved = product(leaf_rhs, leaf_block)
    toward = product(leaf_solved, to_first)
    terms = product(first_rhs - toward[:, :first_size], first_rows)
    terms = terms - product(toward[:, first_size:], first_below)
    peers = lax.axis_size("gz")
    pieces = jnp.moveaxis(terms.reshape(count, peers, first_size), 1, 0)
    first_own = jnp.sum(exchanged(pieces, "gz"), axis=0)

    toward = product(leaf_solved, to_second) + product(first_own, first_to_second)
    terms = product(second_rhs - toward[:, :second_size], second_rows)
    terms = terms - product(toward[:, second_size:], second_below)
    plane_peers = lax.axis_size(PLANE)
    pieces = jnp.moveaxis(terms.reshape(count, plane_peers, second_size), 1, 0)
    second_own = jnp.sum(exchanged(pieces, PLANE), axis=0)

    toward = (
        product(leaf_solved, to_top)
        + product(first_own, first_to_top)
        + product(second_own, second_to_top)
    )
    terms = product(top_rhs - toward[:, :top_size], top_inverse)
    terms = terms - product(toward[:, top_size:], top_below)
    width = 128 * -(-top_total // (128 * plane_peers))
    used = top_total // width
    pieces = jnp.moveaxis(terms.reshape(count, used, width), 1, 0)
    pieces = padded(pieces, 0, 0, plane_peers - used)
    chunk = jnp.sum(exchanged(pieces, PLANE), axis=0)
    chunk = jnp.sum(sent_to_all(chunk, "gx"), axis=0)
    top_whole = jnp.moveaxis(sent_to_all(chunk, PLANE)[:used], 0, 1).reshape(count, top_total)

    top_back = product_back(top_whole, top_inverse)
    top_pair = jnp.concatenate([top_back, product_back(top_whole, top_below)], axis=1)
    second_gap = second_own - product_back(top_pair, second_to_top)
    second_whole = jnp.moveaxis(sent_to_all(second_gap, PLANE), 0, 1).reshape(count, -1)
    second_back = product_back(second_whole, second_rows)
    second_pair = jnp.concatenate([second_back, product_back(second_whole, second_below)], axis=1)
    first_gap = (
        first_own
        - product_back(second_pair, first_to_second)
        - product_back(top_pair, first_to_top)
    )
    first_whole = jnp.moveaxis(sent_to_all(first_gap, "gz"), 0, 1).reshape(count, -1)
    first_back = product_back(first_whole, first_rows)
    first_pair = jnp.concatenate([first_back, product_back(first_whole, first_below)], axis=1)
    leaf_gap = (
        leaf_solved - product_back(first_pair, to_first) - product_back(second_pair, to_second)
    )
    leaf_gap = leaf_gap - product_back(top_pair, to_top)
    leaf_back = product_back(leaf_gap, leaf_block)
    ordered = jnp.concatenate([leaf_back, first_back, second_back, top_back], axis=1)
    natural = product(ordered, pick)

    window = natural.T.reshape(side, side, side * count)
    window = with_next(window, "gx", 0, 1)
    window = with_next(window, "gy", 1, 1)
    window = with_next(window, "gz", 2, count)
    window = jnp.pad(window, ((0, 0), (0, 1), (0, count)))
    return prolonged(window, count, fine)


def solution(mesh):
    blocks = P("gx", "gy", "gz")
    return jax.shard_map(
        per_device,
        mesh=mesh,
        in_specs=(
            P(None, "gx", "gy", "gz"),
            P(None, "gx", "gy", "gz"),
            blocks,
            blocks,
            blocks,
            blocks,
            blocks,
            blocks,
            blocks,
            blocks,
            blocks,
            P("gx", PLANE, None),
            blocks,
            P(("gx", "gy", "gz"), None),
        ),
        out_specs=P(None, "gx", "gy", "gz"),
        check_vma=False,
    )
```

```python
import numpy as np
import jax
import jax.numpy as jnp
from jax import lax
from jax.experimental import pallas as pl
from jax.experimental.pallas import tpu as pltpu
from jax.sharding import PartitionSpec as P

PLANE = ("gy", "gz")
precise = lax.Precision.HIGHEST


def shifted(shard, axis, by):
    peers = lax.axis_size(axis)
    pairs = [(i, i + by) for i in range(peers) if 0 <= i + by < peers]
    return lax.ppermute(shard, axis, pairs)


def exchanged(pieces, axis):
    return lax.all_to_all(pieces, axis, split_axis=0, concat_axis=0, tiled=True)


def sent_to_all(shard, axis):
    copies = jnp.broadcast_to(shard, (lax.axis_size(axis), *shard.shape))
    return exchanged(copies, axis)


def product(operand, matrix):
    return jnp.dot(operand, matrix, precision=precise, preferred_element_type=jnp.float32)


def product_back(operand, matrix):
    return lax.dot_general(
        operand,
        matrix,
        (((1,), (1,)), ((), ())),
        precision=precise,
        preferred_element_type=jnp.float32,
    )


def two_restrictions(distance):
    return np.maximum(0.0, 4.0 - np.abs(distance)) / 16.0


def restriction_weights(fine):
    cell = 4.0 * (np.arange(fine // 4 + 2) - 1)[:, None]
    at = np.arange(fine)[None, :]
    own = two_restrictions(cell - at)
    through_before = two_restrictions(cell - (at - 1))
    beside = through_before + two_restrictions(cell - (at + 1))
    before = np.where(at == 0, through_before, 0.0)
    return own, beside, before


def prolongation_weights(fine):
    at = np.arange(fine)[:, None] / 4.0
    cell = np.arange(fine // 4 + 1)[None, :]
    return np.maximum(0.0, 1.0 - np.abs(at - cell))


def by_lane(weights, count):
    coarse, fine = weights.shape
    out = np.zeros((count, fine, coarse, count), np.float32)
    for r in range(count):
        out[r, :, :, r] = weights.T
    return out.reshape(count, fine, coarse * count)


def parts_of(values):
    first = values.astype(jnp.bfloat16)
    rest = values - first.astype(jnp.float32)
    second = rest.astype(jnp.bfloat16)
    third = (rest - second.astype(jnp.float32)).astype(jnp.bfloat16)
    return first, second, third


def dot(left, right):
    return jnp.dot(left, right, preferred_element_type=jnp.float32)


def times_weights(values, weights):
    first, second, third = parts_of(values)
    return dot(first, weights) + (dot(second, weights) + dot(third, weights))


def weights_times(weights, values):
    first, second, third = parts_of(values)
    return dot(weights, first) + (dot(weights, second) + dot(weights, third))


def restrict_body(
    own, beside, before, edge, rhs, iterate, coefficient, z_own, z_beside, z_before,
    y_own, y_beside, y_before, out,
):
    count, fine = rhs.shape[:2]
    coarse = own.shape[0]
    at_x, at_y, at_z = edge[0], edge[1], edge[2]
    beside_sum = None
    own_sum = None
    for r in range(count):
        planes = [iterate[r, x] for x in range(fine)]
        gaps = [rhs[r, x] - (6.0 + coefficient[x]) * planes[x] for x in range(fine)]
        values, cells = [], []
        for i in range(coarse):
            value = cell = None
            for x in range(fine):
                if own[i, x]:
                    term = float(own[i, x]) * gaps[x]
                    value = term if value is None else value + term
                    term = float(own[i, x]) * planes[x]
                    cell = term if cell is None else cell + term
                if beside[i, x]:
                    weight = float(beside[i, x])
                    if before[i, x]:
                        weight = weight - at_x * float(before[i, x])
                    term = weight * planes[x]
                    value = term if value is None else value + term
            values.append(value)
            cells.append(jnp.zeros_like(planes[0]) if cell is None else cell)
        value = jnp.concatenate(values, axis=0)
        cell = jnp.concatenate(cells, axis=0)
        z_pair = (z_beside[r] - at_z * z_before[r]).astype(jnp.bfloat16)
        z_cell = z_own[r].astype(jnp.bfloat16)
        term = times_weights(value, z_cell) + times_weights(cell, z_pair)
        beside_sum = term if beside_sum is None else beside_sum + term
        term = times_weights(cell, z_cell)
        own_sum = term if own_sum is None else own_sum + term
    y_pair = (y_beside[...] - at_y * y_before[...]).astype(jnp.bfloat16)
    y_cell = y_own[...].astype(jnp.bfloat16)
    result = weights_times(y_cell, beside_sum) + weights_times(y_pair, own_sum)
    out[...] = result.reshape(out.shape)


def restricted(edge, right_side, iterate, coefficient):
    count, fine = right_side.shape[:2]
    own, beside, before = restriction_weights(fine)
    coarse = own.shape[0]
    lanes = [by_lane(w, count) for w in (own, beside, before)]
    rows = [np.kron(np.eye(coarse), w).astype(np.float32) for w in (own, beside, before)]

    def body(*refs):
        restrict_body(own, beside, before, *refs)

    vmem = pl.BlockSpec(memory_space=pltpu.VMEM)
    return pl.pallas_call(
        body,
        out_shape=jax.ShapeDtypeStruct((coarse, coarse, coarse * count), jnp.float32),
        in_specs=[pl.BlockSpec(memory_space=pltpu.SMEM)] + [vmem] * 9,
        out_specs=vmem,
        name="restrict_twice",
    )(edge, right_side, iterate, coefficient, *lanes, *rows)


def prolong_body(window, y_weights, z_weights, out):
    count, fine = out.shape[:2]
    cells = window.shape[0]
    flat = window[...].reshape(cells * window.shape[1], window.shape[2])
    along_y = weights_times(y_weights[...].astype(jnp.bfloat16), flat)
    for r in range(count):
        along_z = times_weights(along_y, z_weights[r].astype(jnp.bfloat16))
        planes = [along_z[i * fine : (i + 1) * fine] for i in range(cells)]
        for i in range(cells - 1):
            for q in range(4):
                value = planes[i]
                if q:
                    value = (1.0 - q / 4.0) * value + (q / 4.0) * planes[i + 1]
                out[r, 4 * i + q] = value


def prolonged(window, count, fine):
    cells = window.shape[0]
    weights = prolongation_weights(fine)
    along_y = np.zeros((fine, window.shape[1]))
    along_y[:, :cells] = weights
    rows = np.kron(np.eye(cells), along_y).astype(np.float32)
    lanes = np.zeros((count, window.shape[2], fine), np.float32)
    for r in range(count):
        for k in range(cells):
            lanes[r, k * count + r] = weights[:, k]
    vmem = pl.BlockSpec(memory_space=pltpu.VMEM)
    return pl.pallas_call(
        prolong_body,
        out_shape=jax.ShapeDtypeStruct((count, fine, fine, fine), jnp.float32),
        in_specs=[vmem] * 3,
        out_specs=vmem,
        name="prolong_twice",
    )(window, rows, lanes)


def padded(values, dim, before, after):
    widths = [(0, 0)] * values.ndim
    widths[dim] = (before, after)
    return jnp.pad(values, widths)


def with_neighbours(values, axis, dim, width):
    length = values.shape[dim]
    first = lax.slice_in_dim(values, 0, width, axis=dim)
    last = lax.slice_in_dim(values, length - width, length, axis=dim)
    from_below = shifted(last, axis, 1)
    from_above = shifted(first, axis, -1)
    inner = lax.slice_in_dim(values, width, length - width, axis=dim)
    room = length - 3 * width
    return inner + padded(from_below, dim, 0, room) + padded(from_above, dim, room, 0)


def with_next(values, axis, dim, width):
    first = lax.slice_in_dim(values, 0, width, axis=dim)
    return jnp.concatenate([values, shifted(first, axis, -1)], axis=dim)


def per_device(
    right_side,
    iterate,
    coefficient,
    ordering,
    leaf_inverse,
    leaf_first,
    leaf_second,
    leaf_top,
    first_inverse,
    first_second,
    first_top,
    second_inverse,
    second_top,
    top_inverse,
):
    count, fine = right_side.shape[:2]
    leaf_size = leaf_inverse.shape[-1]
    first_size = first_second.shape[3]
    second_size = second_top.shape[3]
    top_total = top_inverse.shape[1]
    top_size = top_inverse.shape[0]
    side = fine // 4
    cells = side**3
    first_rows = first_inverse[0, 0]
    second_rows = second_inverse[0]
    to_first = leaf_first[0, 0, 0]
    to_second = leaf_second[0, 0, 0]
    to_top = leaf_top[0, 0, 0]
    first_to_second = first_second[0, 0, 0]
    first_to_top = first_top[0, 0, 0]
    second_to_top = second_top[0, 0, 0]
    leaf_block = leaf_inverse[0, 0, 0]

    top_below = shifted(top_inverse, "gx", 1)
    first_below = shifted(first_rows, "gz", 1)
    second_below = shifted(second_rows, "gy", 1)
    edge = jnp.stack([lax.axis_index(a) == 0 for a in ("gx", "gy", "gz")]).astype(jnp.float32)
    partial = restricted(edge, right_side, iterate, coefficient)
    coarse = with_neighbours(partial, "gz", 2, count)
    coarse = with_neighbours(coarse, "gy", 1, 1)
    coarse = with_neighbours(coarse, "gx", 0, 1)
    natural = coarse.reshape(cells, count).T

    chosen_at = ordering.reshape(-1)[:, None] == jnp.arange(cells, dtype=jnp.int32)[None, :]
    pick = chosen_at.astype(jnp.float32)
    chosen = product_back(natural, pick)
    first_end = leaf_size + first_size
    second_end = first_end + second_size
    leaf_rhs = chosen[:, :leaf_size]
    first_rhs = chosen[:, leaf_size:first_end]
    second_rhs = chosen[:, first_end:second_end]
    top_rhs = chosen[:, second_end:]

    leaf_solved = product(leaf_rhs, leaf_block)
    toward = product(leaf_solved, to_first)
    terms = product(first_rhs - toward[:, :first_size], first_rows)
    terms = terms - product(toward[:, first_size:], first_below)
    peers = lax.axis_size("gz")
    pieces = jnp.moveaxis(terms.reshape(count, peers, first_size), 1, 0)
    first_own = jnp.sum(exchanged(pieces, "gz"), axis=0)

    toward = product(leaf_solved, to_second) + product(first_own, first_to_second)
    terms = product(second_rhs - toward[:, :second_size], second_rows)
    terms = terms - product(toward[:, second_size:], second_below)
    plane_peers = lax.axis_size(PLANE)
    pieces = jnp.moveaxis(terms.reshape(count, plane_peers, second_size), 1, 0)
    second_own = jnp.sum(exchanged(pieces, PLANE), axis=0)

    toward = (
        product(leaf_solved, to_top)
        + product(first_own, first_to_top)
        + product(second_own, second_to_top)
    )
    terms = product(top_rhs - toward[:, :top_size], top_inverse)
    terms = terms - product(toward[:, top_size:], top_below)
    width = 128 * -(-top_total // (128 * plane_peers))
    used = top_total // width
    pieces = jnp.moveaxis(terms.reshape(count, used, width), 1, 0)
    pieces = padded(pieces, 0, 0, plane_peers - used)
    chunk = jnp.sum(exchanged(pieces, PLANE), axis=0)
    chunk = jnp.sum(sent_to_all(chunk, "gx"), axis=0)
    top_whole = jnp.moveaxis(sent_to_all(chunk, PLANE)[:used], 0, 1).reshape(count, top_total)

    top_back = product_back(top_whole, top_inverse)
    top_pair = jnp.concatenate([top_back, product_back(top_whole, top_below)], axis=1)
    second_gap = second_own - product_back(top_pair, second_to_top)
    second_whole = jnp.moveaxis(sent_to_all(second_gap, PLANE), 0, 1).reshape(count, -1)
    second_back = product_back(second_whole, second_rows)
    second_pair = jnp.concatenate([second_back, product_back(second_whole, second_below)], axis=1)
    first_gap = (
        first_own
        - product_back(second_pair, first_to_second)
        - product_back(top_pair, first_to_top)
    )
    first_whole = jnp.moveaxis(sent_to_all(first_gap, "gz"), 0, 1).reshape(count, -1)
    first_back = product_back(first_whole, first_rows)
    first_pair = jnp.concatenate([first_back, product_back(first_whole, first_below)], axis=1)
    leaf_gap = (
        leaf_solved - product_back(first_pair, to_first) - product_back(second_pair, to_second)
    )
    leaf_gap = leaf_gap - product_back(top_pair, to_top)
    leaf_back = product_back(leaf_gap, leaf_block)
    ordered = jnp.concatenate([leaf_back, first_back, second_back, top_back], axis=1)
    natural = product(ordered, pick)

    window = natural.T.reshape(side, side, side * count)
    window = with_next(window, "gx", 0, 1)
    window = with_next(window, "gy", 1, 1)
    window = with_next(window, "gz", 2, count)
    window = jnp.pad(window, ((0, 0), (0, 1), (0, count)))
    return prolonged(window, count, fine)


def solution(mesh):
    blocks = P("gx", "gy", "gz")
    return jax.shard_map(
        per_device,
        mesh=mesh,
        in_specs=(
            P(None, "gx", "gy", "gz"),
            P(None, "gx", "gy", "gz"),
            blocks,
            blocks,
            blocks,
            blocks,
            blocks,
            blocks,
            blocks,
            blocks,
            blocks,
            P("gx", PLANE, None),
            blocks,
            P(("gx", "gy", "gz"), None),
        ),
        out_specs=P(None, "gx", "gy", "gz"),
        check_vma=False,
    )
```

```python
import functools

import numpy as np
import jax
import jax.numpy as jnp
from jax import lax
from jax.experimental import pallas as pl
from jax.experimental.pallas import tpu as pltpu
from jax.sharding import PartitionSpec as P

PLANE = ("gy", "gz")
precise = lax.Precision.HIGHEST
VMEM = pl.BlockSpec(memory_space=pltpu.VMEM)
SMEM = pl.BlockSpec(memory_space=pltpu.SMEM)
LIMIT = pltpu.CompilerParams(vmem_limit_bytes=16 * 1024 * 1024)


def shifted(shard, axis, by):
    peers = lax.axis_size(axis)
    pairs = [(i, i + by) for i in range(peers) if 0 <= i + by < peers]
    return lax.ppermute(shard, axis, pairs)


def exchanged(pieces, axis):
    return lax.all_to_all(pieces, axis, split_axis=0, concat_axis=0, tiled=True)


def sent_to_all(shard, axis):
    copies = jnp.broadcast_to(shard, (lax.axis_size(axis), *shard.shape))
    return exchanged(copies, axis)


def product(operand, matrix):
    return jnp.dot(operand, matrix, precision=precise, preferred_element_type=jnp.float32)


def product_back(operand, matrix):
    return lax.dot_general(
        operand,
        matrix,
        (((1,), (1,)), ((), ())),
        precision=precise,
        preferred_element_type=jnp.float32,
    )


def two_restrictions(distance):
    return np.maximum(0.0, 4.0 - np.abs(distance)) / 16.0


def restriction_weights(fine):
    cell = 4.0 * (np.arange(fine // 4 + 2) - 1)[:, None]
    at = np.arange(fine)[None, :]
    own = two_restrictions(cell - at)
    through_before = two_restrictions(cell - (at - 1))
    beside = through_before + two_restrictions(cell - (at + 1))
    before = np.where(at == 0, through_before, 0.0)
    return own, beside, before


def prolongation_weights(fine):
    at = np.arange(fine)[:, None] / 4.0
    cell = np.arange(fine // 4 + 1)[None, :]
    return np.maximum(0.0, 1.0 - np.abs(at - cell))


def by_lane(weights, count):
    coarse, fine = weights.shape
    out = np.zeros((count, fine, coarse, count), np.float32)
    for r in range(count):
        out[r, :, :, r] = weights.T
    return out.reshape(count, fine, coarse * count)


def parts_of(values):
    first = values.astype(jnp.bfloat16)
    rest = values - first.astype(jnp.float32)
    second = rest.astype(jnp.bfloat16)
    third = (rest - second.astype(jnp.float32)).astype(jnp.bfloat16)
    return first, second, third


def dot(left, right):
    return jnp.dot(left, right, preferred_element_type=jnp.float32)


def dot_back(left, right):
    return lax.dot_general(
        left, right, (((1,), (1,)), ((), ())), preferred_element_type=jnp.float32
    )


def times_weights_back(values, weights):
    first, second, third = parts_of(values)
    return dot_back(first, weights) + (dot_back(second, weights) + dot_back(third, weights))


def weights_times_back(weights, values):
    first, second, third = parts_of(values)
    return dot_back(weights, first) + (dot_back(weights, second) + dot_back(weights, third))


def times_weights(values, weights):
    first, second, third = parts_of(values)
    return dot(first, weights) + (dot(second, weights) + dot(third, weights))


def weights_times(weights, values):
    first, second, third = parts_of(values)
    return dot(weights, first) + (dot(weights, second) + dot(weights, third))


def restrict_body(
    own, beside, before, at, rhs, iterate, coefficient, z_own, z_beside, z_before,
    y_own, y_beside, y_before, inner, upper, lower,
):
    count, fine = rhs.shape[:2]
    coarse = own.shape[0]
    at_x, at_y, at_z = [jnp.where(at[d] == 0, 1.0, 0.0) for d in range(3)]
    beside_sum = None
    own_sum = None
    for r in range(count):
        planes = [iterate[r, x] for x in range(fine)]
        gaps = [rhs[r, x] - (6.0 + coefficient[x]) * planes[x] for x in range(fine)]
        values, cells = [], []
        for i in range(coarse):
            value = cell = None
            for x in range(fine):
                if own[i, x]:
                    term = float(own[i, x]) * gaps[x]
                    value = term if value is None else value + term
                    term = float(own[i, x]) * planes[x]
                    cell = term if cell is None else cell + term
                if beside[i, x]:
                    weight = float(beside[i, x])
                    if before[i, x]:
                        weight = weight - at_x * float(before[i, x])
                    term = weight * planes[x]
                    value = term if value is None else value + term
            values.append(value)
            cells.append(jnp.zeros_like(planes[0]) if cell is None else cell)
        value = jnp.concatenate(values, axis=0)
        cell = jnp.concatenate(cells, axis=0)
        z_pair = (z_beside[r] - at_z * z_before[r]).astype(jnp.bfloat16)
        z_cell = z_own[r].astype(jnp.bfloat16)
        term = times_weights(value, z_cell) + times_weights(cell, z_pair)
        beside_sum = term if beside_sum is None else beside_sum + term
        term = times_weights(cell, z_cell)
        own_sum = term if own_sum is None else own_sum + term
    y_pair = (y_beside[...] - at_y * y_before[...]).astype(jnp.bfloat16)
    y_cell = y_own[...].astype(jnp.bfloat16)
    result = weights_times(y_cell, beside_sum) + weights_times(y_pair, own_sum)
    result = result.reshape(coarse, coarse, coarse * count)
    inner[...] = result[1:-1]
    lower[...] = result[0]
    upper[...] = result[coarse - 1]


def restricted(at, right_side, iterate, coefficient):
    count, fine = right_side.shape[:2]
    own, beside, before = restriction_weights(fine)
    coarse = own.shape[0]
    lanes = [by_lane(w, count) for w in (own, beside, before)]
    rows = [np.kron(np.eye(coarse), w).astype(np.float32) for w in (own, beside, before)]

    def body(*refs):
        restrict_body(own, beside, before, *refs)

    layer = jax.ShapeDtypeStruct((coarse, coarse * count), jnp.float32)
    inner = jax.ShapeDtypeStruct((coarse - 2, coarse, coarse * count), jnp.float32)
    return pl.pallas_call(
        body,
        out_shape=(inner, layer, layer),
        in_specs=[SMEM] + [VMEM] * 9,
        out_specs=(VMEM,) * 3,
        compiler_params=LIMIT,
        name="restrict_twice",
    )(at, right_side, iterate, coefficient, *lanes, *rows)


def numbers(side, kind):
    lane = lax.broadcasted_iota(jnp.int32, (side * 8, 1), 0)
    x, y = lane >> 3, lane & 7
    if kind == "in":
        number = jnp.where((y >= 1) & (y <= side), x * side * side + (y - 1) * side, -1000)
    elif kind == "out":
        number = jnp.where(y < side, x * side * side + y * side, -1000)
    else:
        number = jnp.where(y == 0, x * side * side + (side - 1) * side, -1000)
    return number.astype(jnp.float32)


def one_hot(number, order):
    return jnp.where(number == order, 1.0, 0.0).astype(jnp.bfloat16)


def eye(size):
    rows = lax.broadcasted_iota(jnp.int32, (size, size), 0)
    return jnp.where(rows == lax.broadcasted_iota(jnp.int32, (size, size), 1), 1.0, 0.0).astype(
        jnp.bfloat16
    )


def picked(cells, count, side, number, order, layers=None):
    total = None
    for z in range(side) if layers is None else layers:
        layer = cells[(z + 1) * count : (z + 2) * count]
        term = times_weights(layer, one_hot(number + float(z), order))
        total = term if total is None else total + term
    return total


def split_order(order, sizes):
    out, start = [], 0
    for size in sizes:
        out.append(order[:, start : start + size])
        start += size
    return out


def prepare_body(sizes, side, order, leaf, to_first, first, second, up, down, beside):
    order = order[...].astype(jnp.float32)
    leaf_order = split_order(order, sizes)[0]
    first_size = sizes[1]
    reach = side * 8
    first = first[:, 0, :]
    up[...] = jnp.zeros_like(up)
    up[0:first_size, 0 : first.shape[1]] = first
    up[first_size : first_size + 1, 0 : order.shape[1]] = order
    face = one_hot(numbers(side, "in"), leaf_order)
    rows = weights_times(face, leaf[:, 0, :])
    down[...] = jnp.zeros_like(down)
    down[0:reach, 0 : 2 * first_size] = product_back(rows, to_first[:, 0, :])
    down[reach : reach + first_size, 0 : first.shape[1]] = first
    beside[...] = jnp.zeros_like(beside)
    beside[0 : sizes[2], :] = second[:, 0, :]
    beside[sizes[2] : sizes[2] + 1, 0 : order.shape[1]] = order


def first_body(
    sizes, side, at, inner, arrived, order, leaf, to_first, first, below, above, cells_out, pieces
):
    count = pieces.shape[1] // 4
    peers = pieces.shape[0]
    first_size = sizes[1]
    reach = side * 8
    order = order[...].astype(jnp.float32)
    leaf_order, first_order = split_order(order, sizes)[:2]
    values = inner[...]
    row = lax.broadcasted_iota(jnp.int32, values.shape, 1)
    values = values + jnp.where(row == 1, arrived[...][:, None, :], 0.0)
    lanes = values.shape[2]
    cells = weights_times_back(eye(lanes), values.reshape(reach, lanes))
    cells_out[...] = cells
    number = numbers(side, "in")
    leaf_rhs = picked(cells, count, side, number, leaf_order)
    first_rhs = picked(cells, count, side, number, first_order, [side - 1])
    after = cells[(side + 1) * count : (side + 2) * count]
    before = cells[0:count]
    toward = product_back(product(leaf_rhs, leaf[:, 0, :]), to_first[:, 0, :])
    own_rows = first[:, 0, :]
    whole = own_rows.shape[1]
    below_rows = below[0:first_size, 0:whole]
    below_order = below[first_size : first_size + 1, 0 : order.shape[1]]
    below_order = split_order(below_order, sizes)[1]
    from_before = times_weights(before, one_hot(number + float(side - 1), below_order))
    through = product(after, above[0:reach, 0 : 2 * first_size])
    above_rows = above[reach : reach + first_size, 0:whole]
    terms = product(first_rhs - toward[:, :first_size] - through[:, first_size:], own_rows)
    terms = terms + product(from_before - toward[:, first_size:], below_rows)
    terms = terms - product(through[:, :first_size], above_rows)
    pieces[...] = jnp.zeros_like(pieces)
    place = at[2]
    for p in range(peers):
        pieces[p, 0:count, 0:first_size] = terms[:, p * first_size : (p + 1) * first_size]
        pieces[p, count : 2 * count, 0:reach] = jnp.where(place + 1 == p, after, 0.0)
        pieces[p, 2 * count : 3 * count, 0:reach] = jnp.where(place - 1 == p, before, 0.0)


def second_body(
    sizes, side, gz, at, received, cells, order, leaf, to_second, to_top, first_second, first_top,
    second, below, pieces, leaf_out, first_out, toward_out, top_out,
):
    peers, rows = pieces.shape[:2]
    count = rows // 2
    _, first_size, second_size, top_size = sizes
    reach = side * 8
    total = received[0]
    for p in range(1, received.shape[0]):
        total = total + received[p]
    first_own = total[0:count, 0:first_size]
    cells = cells[...]
    after = total[count : 2 * count, 0:reach]
    before = total[2 * count : 3 * count, 0:reach]
    cells = jnp.concatenate(
        [
            cells[0:count],
            cells[count : 2 * count] + after,
            cells[2 * count : side * count],
            cells[side * count : (side + 1) * count] + before,
            cells[(side + 1) * count :],
        ],
        axis=0,
    )
    order = order[...].astype(jnp.float32)
    leaf_order, _, second_order, top_order = split_order(order, sizes)
    number = numbers(side, "in")
    leaf_solved = product(picked(cells, count, side, number, leaf_order), leaf[:, 0, :])
    second_rhs = picked(cells, count, side, number, second_order)
    top_out[...] = picked(cells, count, side, number, top_order)
    below_order = below[second_size : second_size + 1, 0 : order.shape[1]]
    _, _, below_second, below_top = split_order(below_order, sizes)
    number = numbers(side, "before")
    from_before = picked(cells, count, side, number, below_second)
    top_before = picked(cells, count, side, number, below_top)
    toward = product_back(leaf_solved, to_second[:, 0, :])
    toward = toward + product(first_own, first_second[:, 0, :])
    terms = product(second_rhs - toward[:, :second_size], second[:, 0, :])
    terms = terms + product(from_before - toward[:, second_size:], below[0:second_size, :])
    pieces[...] = jnp.zeros_like(pieces)
    place = (at[1] - 1) * gz + at[2]
    for p in range(peers):
        pieces[p, 0:count, 0:second_size] = terms[:, p * second_size : (p + 1) * second_size]
        pieces[p, count : 2 * count, 0:top_size] = jnp.where(place == p, top_before, 0.0)
    leaf_out[...] = leaf_solved
    first_out[...] = first_own
    toward_out[...] = product_back(leaf_solved, to_top[...]) + product(
        first_own, first_top[:, 0, :]
    )


def top_body(used, received, toward, rhs, second_top, top, below, pieces, second_out):
    count = toward.shape[0]
    second_size = second_out.shape[1]
    top_size = rhs.shape[1]
    total = received[0]
    for p in range(1, received.shape[0]):
        total = total + received[p]
    second_own = total[0:count, 0:second_size]
    second_out[...] = second_own
    toward = toward[...] + product(second_own, second_top[:, 0, :])
    own = rhs[...] + total[count : 2 * count, 0:top_size] - toward[:, :top_size]
    other = toward[:, top_size:]
    width = pieces.shape[2]
    for p in range(used):
        at = slice(p * width, (p + 1) * width)
        pieces[p] = product(own, top[:, at]) - product(other, below[:, at])
    for p in range(used, pieces.shape[0]):
        pieces[p] = jnp.zeros(pieces.shape[1:], jnp.float32)


def spread_sum_body(received, out):
    total = received[0]
    for p in range(1, received.shape[0]):
        total = total + received[p]
    for p in range(out.shape[0]):
        out[p] = total


def top_back_body(
    used, whole, top, below, second_own, first_own, leaf_solved, second_top, first_top, to_top,
    pair_out, second_gap, first_gap, leaf_gap,
):
    count = whole.shape[1]
    width = whole.shape[2]
    top_size = top.shape[0]

    def step(p, sums):
        piece = whole[p]
        start = pl.multiple_of(p * width, 128)
        out = list(sums)
        for t in range(width // 128):
            at = pl.ds(start + t * 128, 128)
            rows, lower = top[:, at], below[:, at]
            for r in range(count):
                line = piece[r : r + 1, t * 128 : (t + 1) * 128]
                out[r] = out[r] + rows * line
                out[count + r] = out[count + r] + lower * line
        return tuple(out)

    zero = jnp.zeros((top_size, 128), jnp.float32)
    sums = lax.fori_loop(0, used, step, (zero,) * (2 * count))
    line = lax.broadcasted_iota(jnp.int32, (count, 128), 0)
    halves = []
    for half in range(2):
        total = None
        for r in range(count):
            ones = jnp.where(line == r, 1.0, 0.0).astype(jnp.bfloat16)
            term = weights_times_back(ones, sums[half * count + r])
            total = term if total is None else total + term
        halves.append(total)
    own, lower = halves
    pair_out[...] = own

    def against(matrix):
        return product_back(own, matrix[:, :top_size]) + product_back(lower, matrix[:, top_size:])

    second_gap[...] = second_own[...] - against(second_top[:, 0, :])
    first_gap[...] = first_own[...] - against(first_top[:, 0, :])
    rows = to_top[...]
    leaf_gap[...] = leaf_solved[...] - (
        product(own, rows[:top_size]) + product(lower, rows[top_size:])
    )


def second_back_body(
    sizes, side, whole, second, below, first_gap, leaf_gap, top_back, order, leaf, to_second,
    first_second, sent, base_out, second_out,
):
    count = whole.shape[0]
    _, first_size, second_size, _ = sizes
    reach = side * 8
    own = product_back(whole[...], second[:, 0, :])
    lower = product_back(whole[...], below[0:second_size, :])
    second_out[...] = own
    weights = first_second[:, 0, :]
    gap = first_gap[...] - product_back(own, weights[:, :second_size])
    gap = gap - product_back(lower, weights[:, second_size:])
    rows = to_second[:, 0, :]
    rest = leaf_gap[...] - product(own, rows[:second_size]) - product(lower, rows[second_size:])
    base = product_back(rest, leaf[:, 0, :])
    base_out[...] = base
    order = order[...].astype(jnp.float32)
    leaf_order, _, second_order, top_order = split_order(order, sizes)
    number = numbers(side, "out")
    face = times_weights_back(base, one_hot(number, leaf_order))
    face = face + times_weights_back(own, one_hot(number, second_order))
    face = face + times_weights_back(top_back[...], one_hot(number, top_order))
    sent[...] = jnp.zeros_like(sent)
    sent[0:count, 0:first_size] = gap
    sent[count : 2 * count, 0:reach] = face


def leaf_back_body(
    sizes, side, at, received, base, second_back, top_back, order, leaf, to_first, first, below,
    above, window,
):
    count = base.shape[0]
    peers = received.shape[0]
    _, first_size, _, _ = sizes
    reach = side * 8
    whole = jnp.concatenate([received[p, 0:count, 0:first_size] for p in range(peers)], axis=1)
    total = whole.shape[1]
    own = product_back(whole, first[:, 0, :])
    lower = product_back(whole, below[0:first_size, 0:total])
    following = product_back(whole, above[reach : reach + first_size, 0:total])
    rows = to_first[:, 0, :]
    rest = product(own, rows[:first_size]) + product(lower, rows[first_size:])
    leaf_back = base[...] - product_back(rest, leaf[:, 0, :])
    face = jnp.zeros((count, reach), jnp.float32)
    for p in range(peers):
        face = face + jnp.where(at[2] + 1 == p, received[p, count : 2 * count, 0:reach], 0.0)
    through = above[0:reach, 0 : 2 * first_size]
    moved = product_back(following, through[:, :first_size])
    moved = moved + product_back(own, through[:, first_size:])
    lane = lax.broadcasted_iota(jnp.int32, (reach, reach), 0)
    shift = jnp.where(lane == lax.broadcasted_iota(jnp.int32, (reach, reach), 1) + 1, 1.0, 0.0)
    face = face - times_weights(moved, shift.astype(jnp.bfloat16))
    order = order[...].astype(jnp.float32)
    orders = split_order(order, sizes)
    number = numbers(side, "out")
    layers = []
    for z in range(side):
        layer = times_weights_back(leaf_back, one_hot(number + float(z), orders[0]))
        layer = layer + times_weights_back(
            second_back[...], one_hot(number + float(z), orders[2])
        )
        layer = layer + times_weights_back(top_back[...], one_hot(number + float(z), orders[3]))
        if z == side - 1:
            layer = layer + times_weights_back(own, one_hot(number + float(z), orders[1]))
        layers.append(layer)
    layers.append(face)
    layers.append(jnp.zeros_like(face))
    cells = jnp.concatenate(layers, axis=0)
    turned = weights_times_back(eye(reach), cells)
    window[...] = turned.reshape(window.shape)


def prolong_body(inner, after_x, after_y, y_weights, z_weights, out):
    count, fine = out.shape[:2]
    cells = inner.shape[0] + 1
    window = jnp.concatenate([inner[...], after_x[...][None]], axis=0)
    row = lax.broadcasted_iota(jnp.int32, window.shape, 1)
    window = jnp.where(row == cells - 1, after_y[...][:, None, :], window)
    flat = window.reshape(cells * window.shape[1], window.shape[2])
    along_y = weights_times(y_weights[...].astype(jnp.bfloat16), flat)
    for r in range(count):
        along_z = times_weights(along_y, z_weights[r].astype(jnp.bfloat16))
        planes = [along_z[i * fine : (i + 1) * fine] for i in range(cells)]
        for i in range(cells - 1):
            for q in range(4):
                value = planes[i]
                if q:
                    value = (1.0 - q / 4.0) * value + (q / 4.0) * planes[i + 1]
                out[r, 4 * i + q] = value


def prolonged(inner, after_x, after_y, count, fine):
    cells = inner.shape[0] + 1
    weights = prolongation_weights(fine)
    along_y = np.zeros((fine, inner.shape[1]))
    along_y[:, :cells] = weights
    rows = np.kron(np.eye(cells), along_y).astype(np.float32)
    lanes = np.zeros((count, inner.shape[2], fine), np.float32)
    for r in range(count):
        for k in range(cells):
            lanes[r, k * count + r] = weights[:, k]
    return pl.pallas_call(
        prolong_body,
        out_shape=jax.ShapeDtypeStruct((count, fine, fine, fine), jnp.float32),
        in_specs=[VMEM] * 5,
        out_specs=VMEM,
        compiler_params=LIMIT,
        name="prolong_twice",
    )(inner, after_x, after_y, rows, lanes)


def padded(values, dim, before, after):
    widths = [(0, 0)] * values.ndim
    widths[dim] = (before, after)
    return jnp.pad(values, widths)


def call(body, scalars, outs, *operands):
    shapes = tuple(jax.ShapeDtypeStruct(o, jnp.float32) for o in outs)
    return pl.pallas_call(
        body,
        out_shape=shapes,
        in_specs=[SMEM] * scalars + [VMEM] * (len(operands) - scalars),
        out_specs=(VMEM,) * len(shapes),
        compiler_params=LIMIT,
    )(*operands)


def per_device(
    right_side,
    iterate,
    coefficient,
    ordering,
    leaf_inverse,
    leaf_first,
    leaf_second,
    leaf_top,
    first_inverse,
    first_second,
    first_top,
    second_inverse,
    second_top,
    top_inverse,
):
    count, fine = right_side.shape[:2]
    leaf_size = leaf_inverse.shape[-1]
    first_size = first_second.shape[3]
    second_size = second_top.shape[3]
    top_size, top_total = top_inverse.shape
    sizes = (leaf_size, first_size, second_size, top_size)
    side = fine // 4
    cells = side**3
    reach = side * 8
    lanes = (side + 2) * count
    gz = lax.axis_size("gz")
    plane_peers = lax.axis_size(PLANE)

    def rows_of(block):
        return jnp.transpose(block, (0, 1, 3, 2, 4)).reshape(block.shape[3], 1, block.shape[4])

    def columns_of(block):
        return jnp.transpose(block, (0, 1, 4, 2, 3)).reshape(block.shape[4], 1, block.shape[3])

    leaf = rows_of(leaf_inverse)
    to_first = columns_of(leaf_first)
    to_second = columns_of(leaf_second)
    to_top = jnp.swapaxes(leaf_top[0, 0, 0], 0, 1)
    first_to_second = rows_of(first_second)
    first_to_top = rows_of(first_top)
    second_to_top = rows_of(second_top)
    first = jnp.transpose(first_inverse, (0, 2, 1, 3)).reshape(first_size, 1, -1)
    second = jnp.transpose(second_inverse, (1, 0, 2))
    order = ordering.reshape(1, cells)

    at = jnp.stack([lax.axis_index(a) for a in ("gx", "gy", "gz")]).astype(jnp.int32)
    inner, upper, lower = restricted(at, right_side, iterate, coefficient)
    from_below = shifted(upper, "gx", 1)
    from_above = shifted(lower, "gx", -1)
    whole_first = -(-max(first.shape[2], cells) // 128) * 128
    up, down, beside = call(
        functools.partial(prepare_body, sizes, side),
        0,
        [(32, whole_first), (reach + 32, whole_first), (32, second.shape[2])],
        order,
        leaf,
        to_first,
        first,
        second,
    )
    first_below = shifted(up, "gz", 1)
    first_above = shifted(down, "gz", -1)
    second_below = shifted(beside, "gy", 1)
    top_below = shifted(top_inverse, "gx", 1)
    inner = inner + padded(from_below[None], 0, 0, side - 1)
    inner = inner + padded(from_above[None], 0, side - 1, 0)
    arrived = shifted(inner[:, side + 1], "gy", 1)

    turned, pieces = call(
        functools.partial(first_body, sizes, side),
        1,
        [(lanes, reach), (gz, 4 * count, 128)],
        at,
        inner,
        arrived,
        order,
        leaf,
        to_first,
        first,
        first_below,
        first_above,
    )
    received = exchanged(pieces, "gz")
    pieces, leaf_solved, first_own, toward, top_rhs = call(
        functools.partial(second_body, sizes, side, gz),
        1,
        [
            (plane_peers, 2 * count, 128),
            (count, leaf_size),
            (count, first_size),
            (count, 2 * top_size),
            (count, top_size),
        ],
        at,
        received,
        turned,
        order,
        leaf,
        to_second,
        to_top,
        first_to_second,
        first_to_top,
        second,
        second_below,
    )
    received = exchanged(pieces, PLANE)
    width = 128 * -(-top_total // (128 * plane_peers))
    used = top_total // width
    pieces, second_own = call(
        functools.partial(top_body, used),
        0,
        [(plane_peers, count, width), (count, second_size)],
        received,
        toward,
        top_rhs,
        second_to_top,
        top_inverse,
        top_below,
    )
    received = exchanged(pieces, PLANE)
    (pieces,) = call(spread_sum_body, 0, [(lax.axis_size("gx"), count, width)], received)
    received = exchanged(pieces, "gx")
    (pieces,) = call(spread_sum_body, 0, [(plane_peers, count, width)], received)
    received = exchanged(pieces, PLANE)
    top_back, second_gap, first_gap, leaf_gap = call(
        functools.partial(top_back_body, used),
        0,
        [(count, top_size), (count, second_size), (count, first_size), (count, leaf_size)],
        received,
        top_inverse,
        top_below,
        second_own,
        first_own,
        leaf_solved,
        second_to_top,
        first_to_top,
        to_top,
    )
    second_whole = jnp.moveaxis(sent_to_all(second_gap, PLANE), 0, 1).reshape(count, -1)
    sent, base, second_back = call(
        functools.partial(second_back_body, sizes, side),
        0,
        [(2 * count, 128), (count, leaf_size), (count, second_size)],
        second_whole,
        second,
        second_below,
        first_gap,
        leaf_gap,
        top_back,
        order,
        leaf,
        to_second,
        first_to_second,
    )
    received = sent_to_all(sent, "gz")
    (window,) = call(
        functools.partial(leaf_back_body, sizes, side),
        1,
        [(side, 8, lanes)],
        at,
        received,
        base,
        second_back,
        top_back,
        order,
        leaf,
        to_first,
        first,
        first_below,
        first_above,
    )
    after_x = shifted(window[0], "gx", -1)
    layer = jnp.concatenate([window[:, 0], after_x[0:1]], axis=0)
    after_y = shifted(layer, "gy", -1)
    return prolonged(window, after_x, after_y, count, fine)


def solution(mesh):
    blocks = P("gx", "gy", "gz")
    return jax.shard_map(
        per_device,
        mesh=mesh,
        in_specs=(
            P(None, "gx", "gy", "gz"),
            P(None, "gx", "gy", "gz"),
            blocks,
            blocks,
            blocks,
            blocks,
            blocks,
            blocks,
            blocks,
            blocks,
            blocks,
            P("gx", PLANE, None),
            blocks,
            P(("gx", "gy", "gz"), None),
        ),
        out_specs=P(None, "gx", "gy", "gz"),
        check_vma=False,
    )
```

```python
import functools

import numpy as np
import jax
import jax.numpy as jnp
from jax import lax
from jax.experimental import pallas as pl
from jax.experimental.pallas import tpu as pltpu
from jax.sharding import PartitionSpec as P

PLANE = ("gy", "gz")
AXES = ("gx", "gy", "gz")
precise = lax.Precision.HIGHEST
VMEM = pl.BlockSpec(memory_space=pltpu.VMEM)
HBM = pl.BlockSpec(memory_space=pltpu.HBM)
FULL = pltpu.CompilerParams(vmem_limit_bytes=67043328 - 1000 * 1024)
LIMIT = pltpu.CompilerParams(vmem_limit_bytes=16 * 1024 * 1024)


def shifted(shard, axis, by):
    peers = lax.axis_size(axis)
    pairs = [(i, i + by) for i in range(peers) if 0 <= i + by < peers]
    return lax.ppermute(shard, axis, pairs)


def exchanged(pieces, axis):
    return lax.all_to_all(pieces, axis, split_axis=0, concat_axis=0, tiled=True)


def sent_to_all(shard, axis):
    copies = jnp.broadcast_to(shard, (lax.axis_size(axis), *shard.shape))
    return exchanged(copies, axis)


def product(operand, matrix):
    return jnp.dot(operand, matrix, precision=precise, preferred_element_type=jnp.float32)


def product_back(operand, matrix):
    return lax.dot_general(
        operand,
        matrix,
        (((1,), (1,)), ((), ())),
        precision=precise,
        preferred_element_type=jnp.float32,
    )


def two_restrictions(distance):
    return np.maximum(0.0, 4.0 - np.abs(distance)) / 16.0


def restriction_weights(fine):
    cell = 4.0 * (np.arange(fine // 4 + 2) - 1)[:, None]
    at = np.arange(fine)[None, :]
    own = two_restrictions(cell - at)
    through_before = two_restrictions(cell - (at - 1))
    beside = through_before + two_restrictions(cell - (at + 1))
    before = np.where(at == 0, through_before, 0.0)
    return own, beside, before


def weight_rows(coarse, fine, kind, missing):
    rows = lax.broadcasted_iota(jnp.int32, (coarse * coarse, coarse * fine), 0)
    columns = lax.broadcasted_iota(jnp.int32, (coarse * coarse, coarse * fine), 1)
    at = columns - (rows >> 3) * fine
    weights = weights_at(4 * ((rows & 7) - 1), at, kind, missing)
    return jnp.where((at >= 0) & (at < fine), weights, 0.0).astype(jnp.bfloat16)


def weight_lanes(coarse, fine, count, r, kind, missing):
    at = lax.broadcasted_iota(jnp.int32, (fine, coarse * count), 0)
    lane = lax.broadcasted_iota(jnp.int32, (fine, coarse * count), 1)
    weights = weights_at(4 * ((lane >> 2) - 1), at, kind, missing)
    return jnp.where((lane & 3) == r, weights, 0.0).astype(jnp.bfloat16)


def weights_at(cell, at, kind, missing):
    def weight(distance):
        return jnp.maximum(4.0 - jnp.abs(distance).astype(jnp.float32), 0.0) * 0.0625

    if kind == "own":
        return weight(cell - at)
    before = jnp.where(at == 0, missing, 0.0)
    return weight(cell - at - 1) + (1.0 - before) * weight(cell - at + 1)


def parts_of(values):
    first = values.astype(jnp.bfloat16)
    rest = values - first.astype(jnp.float32)
    second = rest.astype(jnp.bfloat16)
    third = (rest - second.astype(jnp.float32)).astype(jnp.bfloat16)
    return first, second, third


def dot(left, right):
    return jnp.dot(left, right, preferred_element_type=jnp.float32)


def dot_back(left, right):
    return lax.dot_general(
        left, right, (((1,), (1,)), ((), ())), preferred_element_type=jnp.float32
    )


def times_weights_back(values, weights):
    first, second, third = parts_of(values)
    return dot_back(first, weights) + (dot_back(second, weights) + dot_back(third, weights))


def weights_times_back(weights, values):
    first, second, third = parts_of(values)
    return dot_back(weights, first) + (dot_back(weights, second) + dot_back(weights, third))


def times_weights(values, weights):
    first, second, third = parts_of(values)
    return dot(first, weights) + (dot(second, weights) + dot(third, weights))


def weights_times(weights, values):
    first, second, third = parts_of(values)
    return dot(weights, first) + (dot(weights, second) + dot(weights, third))


def restrict_body(
    own, beside, before, order, rhs_in, iterate_in, coefficient_in, inner, upper,
    rhs, iterate, coefficient, arrived,
):
    count, fine = rhs.shape[:2]
    coarse = own.shape[0]
    half = fine // 2
    copies = [pltpu.make_async_copy(coefficient_in, coefficient, arrived.at[0])]
    for r in range(count):
        for source, room in ((iterate_in, iterate), (rhs_in, rhs)):
            for start in (0, half):
                part = pl.ds(start, half)
                copies.append(
                    pltpu.make_async_copy(
                        source.at[r, part], room.at[r, part], arrived.at[len(copies)]
                    )
                )
    for copy in copies:
        copy.start()
    at_x, at_y, at_z = [jnp.where(lax.axis_index(a) == 0, 1.0, 0.0) for a in AXES]
    layer, lanes = inner.shape[1:]
    top_size = coarse - 2
    top_size = top_size * top_size
    upper[...] = jnp.zeros_like(upper)
    orders = order[...].astype(jnp.float32)
    upper[layer : layer + 1, 0:top_size] = orders[:, orders.shape[1] - top_size :]
    y_cell = weight_rows(coarse, fine, "own", None)
    y_pair = weight_rows(coarse, fine, "beside", at_y)
    z_cells = [weight_lanes(coarse, fine, count, r, "own", None) for r in range(count)]
    z_pairs = [weight_lanes(coarse, fine, count, r, "beside", at_z) for r in range(count)]
    copies[0].wait()
    beside_sum = None
    own_sum = None
    for r in range(count):
        for copy in copies[4 * r + 1 : 4 * r + 5]:
            copy.wait()
        planes = [iterate[r, x] for x in range(fine)]
        gaps = [rhs[r, x] - (6.0 + coefficient[x]) * planes[x] for x in range(fine)]
        values, cells = [], []
        for i in range(coarse):
            value = cell = None
            for x in range(fine):
                if own[i, x]:
                    term = float(own[i, x]) * gaps[x]
                    value = term if value is None else value + term
                    term = float(own[i, x]) * planes[x]
                    cell = term if cell is None else cell + term
                if beside[i, x]:
                    weight = float(beside[i, x])
                    if before[i, x]:
                        weight = weight - at_x * float(before[i, x])
                    term = weight * planes[x]
                    value = term if value is None else value + term
            values.append(value)
            cells.append(jnp.zeros_like(planes[0]) if cell is None else cell)
        value = jnp.concatenate(values, axis=0)
        cell = jnp.concatenate(cells, axis=0)
        term = times_weights(value, z_cells[r]) + times_weights(cell, z_pairs[r])
        beside_sum = term if beside_sum is None else beside_sum + term
        term = times_weights(cell, z_cells[r])
        own_sum = term if own_sum is None else own_sum + term
    result = weights_times(y_cell, beside_sum) + weights_times(y_pair, own_sum)
    result = result.reshape(coarse, coarse, coarse * count)
    inner[...] = result[:-1]
    upper[0:layer, 0:lanes] = result[coarse - 1]


def restricted(order, right_side, iterate, coefficient):
    count, fine = right_side.shape[:2]
    own, beside, before = restriction_weights(fine)
    coarse = own.shape[0]

    def body(*refs):
        restrict_body(own, beside, before, *refs)

    inner = jax.ShapeDtypeStruct((coarse - 1, coarse, coarse * count), jnp.float32)
    upper = jax.ShapeDtypeStruct((2 * coarse, 128), jnp.float32)
    return pl.pallas_call(
        body,
        out_shape=(inner, upper),
        in_specs=[VMEM] + [HBM] * 3,
        out_specs=(VMEM,) * 2,
        scratch_shapes=[
            pltpu.VMEM(right_side.shape, jnp.float32),
            pltpu.VMEM(iterate.shape, jnp.float32),
            pltpu.VMEM(coefficient.shape, jnp.float32),
            pltpu.SemaphoreType.DMA((4 * count + 1,)),
        ],
        compiler_params=FULL,
        name="restrict_twice",
    )(order, right_side, iterate, coefficient)


def numbers(side, kind):
    lane = lax.broadcasted_iota(jnp.int32, (lanes_of(side, kind), 1), 0)
    x, y = lane >> 3, lane & 7
    if kind == "out":
        number = jnp.where(y < side, x * side * side + y * side, -1000)
        return number.astype(jnp.float32)
    x, y = x - 1, y - 1
    last = side - 1
    along_y = (y >= 0) & (y < side)
    if kind == "in":
        number = jnp.where((x >= 0) & along_y, x * side * side + y * side, -1000)
    elif kind == "before_y":
        number = jnp.where((x >= 0) & (y < 0), x * side * side + last * side, -1000)
    else:
        number = jnp.where((x < 0) & along_y, last * side * side + y * side, -1000)
    return number.astype(jnp.float32)


def lanes_of(side, kind="in"):
    return side * 8 if kind == "out" else (side + 1) * 8


def one_hot(number, order):
    return jnp.where(number == order, 1.0, 0.0).astype(jnp.bfloat16)


def eye(size):
    rows = lax.broadcasted_iota(jnp.int32, (size, size), 0)
    return jnp.where(rows == lax.broadcasted_iota(jnp.int32, (size, size), 1), 1.0, 0.0).astype(
        jnp.bfloat16
    )


def picked(cells, count, side, number, order, layers=None):
    total = None
    for z in range(side) if layers is None else layers:
        layer = cells[(z + 1) * count : (z + 2) * count]
        term = times_weights(layer, one_hot(number + float(z), order))
        total = term if total is None else total + term
    return total


LEAF, TO_FIRST, TO_SECOND, TO_TOP = 0, 128, 184, 248
FIRST_SECOND, FIRST_TOP, SECOND_TOP, ORDER, PACKED = 320, 352, 384, 416, 424


def split_order(order, sizes):
    out, start = [], 0
    for size in sizes:
        out.append(order[:, start : start + size])
        start += size
    return out


def packed_order(pack, sizes):
    leaf_size = sizes[0]
    leaf_order = pack[ORDER : ORDER + 1, 0:leaf_size]
    rest = pack[ORDER + 1 : ORDER + 2, 0 : sum(sizes[1:])]
    return [leaf_order] + split_order(rest, sizes[1:])


def prepare_body(sizes, side, *refs):
    sources, (up, down, beside, pack) = refs[:10], refs[10:14]
    held, arrived = refs[14:24], refs[24]
    copies = [
        pltpu.make_async_copy(source, room, arrived.at[n])
        for n, (source, room) in enumerate(zip(sources, held))
    ]
    for copy in copies:
        copy.start()
    up[...] = jnp.zeros_like(up)
    down[...] = jnp.zeros_like(down)
    beside[sizes[2] :, :] = jnp.zeros_like(beside[sizes[2] :, :])
    for copy in copies:
        copy.wait()
    order, leaf, to_first, first, second = held[:5]
    to_second, to_top, first_second, first_top, second_top = held[5:]
    order = order[...].astype(jnp.float32)
    leaf_size, first_size, second_size = sizes[:3]
    leaf_rows, first_columns = leaf[:, 0, :], to_first[:, 0, :]
    first_rows = first[:, 0, :]
    face = one_hot(numbers(side, "in"), order[:, :leaf_size])
    rows = weights_times(face, leaf_rows)
    up[0:first_size, 0 : first_rows.shape[1]] = first_rows
    up[first_size : first_size + 1, 0 : order.shape[1]] = order
    total = first_rows.shape[1]
    down[:, total : total + 2 * first_size] = product_back(rows, first_columns)
    down[0:first_size, 0:total] = first_rows
    beside[0:second_size, :] = second[:, 0, :]
    beside[second_size : second_size + 1, 0 : order.shape[1]] = order
    pack[ORDER : ORDER + 1, 0:leaf_size] = order[:, :leaf_size]
    pack[ORDER + 1 : ORDER + 2, 0 : order.shape[1] - leaf_size] = order[:, leaf_size:]
    for start, rows in (
        (LEAF, leaf_rows),
        (TO_FIRST, first_columns),
        (TO_SECOND, to_second[:, 0, :]),
        (TO_TOP, to_top[...]),
        (FIRST_SECOND, first_second[:, 0, :]),
        (FIRST_TOP, first_top[:, 0, :]),
        (SECOND_TOP, second_top[:, 0, :]),
    ):
        pack[start : start + rows.shape[0], 0 : rows.shape[1]] = rows


def prepared(sizes, side, width, *sources):
    leaf_size, first_size, second_size, top_size = sizes
    assert leaf_size <= 128 and first_size < 32 and second_size < 32 and top_size <= 36
    shapes = (
        (32, width),
        (lanes_of(side), width),
        (32, sources[4].shape[2]),
        (PACKED, 128),
    )
    return pl.pallas_call(
        functools.partial(prepare_body, sizes, side),
        out_shape=tuple(jax.ShapeDtypeStruct(o, jnp.float32) for o in shapes),
        in_specs=[HBM] * len(sources),
        out_specs=(VMEM,) * len(shapes),
        scratch_shapes=[pltpu.VMEM(x.shape, x.dtype) for x in sources]
        + [pltpu.SemaphoreType.DMA((len(sources),))],
        compiler_params=LIMIT,
        name="prepare",
    )(*sources)


def first_body(
    sizes, side, total, inner, from_x, from_y, pack, first, below, above, cells_out, pieces
):
    count = pieces.shape[1] // 4
    peers = pieces.shape[0]
    first_size = sizes[1]
    leaf_size = sizes[0]
    leaf_order, first_order = packed_order(pack, sizes)[:2]
    values = inner[...]
    across, along, lanes = values.shape
    reach = across * along
    row = lax.broadcasted_iota(jnp.int32, values.shape, 0)
    values = values + jnp.where(row == 1, from_x[0:along, 0:lanes][None], 0.0)
    row = lax.broadcasted_iota(jnp.int32, values.shape, 1)
    values = values + jnp.where(row == 1, from_y[...][:, None, :], 0.0)
    cells = weights_times_back(eye(lanes), values.reshape(reach, lanes))
    cells_out[...] = cells
    number = numbers(side, "in")
    leaf_rhs = picked(cells, count, side, number, leaf_order)
    first_rhs = picked(cells, count, side, number, first_order, [side - 1])
    after = cells[(side + 1) * count : (side + 2) * count]
    before = cells[0:count]
    leaf = pack[LEAF : LEAF + leaf_size, 0:leaf_size]
    to_first = pack[TO_FIRST : TO_FIRST + 2 * first_size, 0:leaf_size]
    toward = product_back(product(leaf_rhs, leaf), to_first)
    whole = total
    own_rows = first[0:first_size, 0:whole]
    below_rows = below[0:first_size, 0:whole]
    below_order = below[first_size : first_size + 1, 0 : sum(sizes)]
    below_order = split_order(below_order, sizes)[1]
    from_before = times_weights(before, one_hot(number + float(side - 1), below_order))
    through = product(after, above[:, whole : whole + 2 * first_size])
    above_rows = above[0:first_size, 0:whole]
    terms = product(first_rhs - toward[:, :first_size] - through[:, first_size:], own_rows)
    terms = terms + product(from_before - toward[:, first_size:], below_rows)
    terms = terms - product(through[:, :first_size], above_rows)
    pieces[...] = jnp.zeros_like(pieces)
    place = lax.axis_index("gz")
    for p in range(peers):
        pieces[p, 0:count, 0:first_size] = terms[:, p * first_size : (p + 1) * first_size]
        pieces[p, count : 2 * count, 0:reach] = jnp.where(place + 1 == p, after, 0.0)
        pieces[p, 2 * count : 3 * count, 0:reach] = jnp.where(place - 1 == p, before, 0.0)


def second_body(
    sizes, side, gz, received, cells, from_x, pack, second, below, pieces, leaf_out, first_out,
    toward_out, top_out,
):
    peers, rows = pieces.shape[:2]
    count = rows // 2
    leaf_size, first_size, second_size, top_size = sizes
    reach = cells.shape[1]
    total = received[0]
    for p in range(1, received.shape[0]):
        total = total + received[p]
    first_own = total[0:count, 0:first_size]
    cells = cells[...]
    after = total[count : 2 * count, 0:reach]
    before = total[2 * count : 3 * count, 0:reach]
    cells = jnp.concatenate(
        [
            cells[0:count],
            cells[count : 2 * count] + after,
            cells[2 * count : side * count],
            cells[side * count : (side + 1) * count] + before,
            cells[(side + 1) * count :],
        ],
        axis=0,
    )
    leaf_order, _, second_order, top_order = packed_order(pack, sizes)
    number = numbers(side, "in")
    leaf = pack[LEAF : LEAF + leaf_size, 0:leaf_size]
    to_second = pack[TO_SECOND : TO_SECOND + 2 * second_size, 0:leaf_size]
    to_top = pack[TO_TOP : TO_TOP + 2 * top_size, 0:leaf_size]
    first_second = pack[FIRST_SECOND : FIRST_SECOND + first_size, 0 : 2 * second_size]
    first_top = pack[FIRST_TOP : FIRST_TOP + first_size, 0 : 2 * top_size]
    leaf_solved = product(picked(cells, count, side, number, leaf_order), leaf)
    second_rhs = picked(cells, count, side, number, second_order)
    top_out[...] = picked(cells, count, side, number, top_order)
    below_order = below[second_size : second_size + 1, 0 : sum(sizes)]
    _, _, below_second, below_top = split_order(below_order, sizes)
    number = numbers(side, "before_y")
    from_before = picked(cells, count, side, number, below_second)
    top_before = picked(cells, count, side, number, below_top)
    toward = product_back(leaf_solved, to_second) + product(first_own, first_second)
    terms = product(second_rhs - toward[:, :second_size], second[0:second_size, :])
    terms = terms + product(from_before - toward[:, second_size:], below[0:second_size, :])
    pieces[...] = jnp.zeros_like(pieces)
    place = (lax.axis_index("gy") - 1) * gz + lax.axis_index("gz")
    for p in range(peers):
        pieces[p, 0:count, 0:second_size] = terms[:, p * second_size : (p + 1) * second_size]
        pieces[p, count : 2 * count, 0:top_size] = jnp.where(place == p, top_before, 0.0)
    leaf_out[...] = leaf_solved
    first_out[...] = first_own
    toward = product_back(leaf_solved, to_top) + product(first_own, first_top)
    order_x = from_x[8:9, 0:top_size]
    before_x = picked(cells, count, side, numbers(side, "before_x"), order_x)
    toward_out[:, :top_size] = toward[:, :top_size]
    toward_out[:, top_size:] = toward[:, top_size:] - before_x


def top_body(used, received, toward, rhs, pack, top, below, pieces, second_out):
    count = toward.shape[0]
    second_size = second_out.shape[1]
    top_size = rhs.shape[1]
    total = received[0]
    for p in range(1, received.shape[0]):
        total = total + received[p]
    second_own = total[0:count, 0:second_size]
    second_out[...] = second_own
    second_top = pack[SECOND_TOP : SECOND_TOP + second_size, 0 : 2 * top_size]
    toward = toward[...] + product(second_own, second_top)
    own = rhs[...] + total[count : 2 * count, 0:top_size] - toward[:, :top_size]
    other = toward[:, top_size:]
    width = pieces.shape[2]
    for p in range(used):
        at = slice(p * width, (p + 1) * width)
        pieces[p] = product(own, top[:, at]) - product(other, below[:, at])
    for p in range(used, pieces.shape[0]):
        pieces[p] = jnp.zeros(pieces.shape[1:], jnp.float32)


def spread_sum_body(received, out):
    total = received[0]
    for p in range(1, received.shape[0]):
        total = total + received[p]
    for p in range(out.shape[0]):
        out[p] = total


def top_back_body(
    used, whole, top, below, second_own, first_own, leaf_solved, pack, pair_out, second_gap,
    first_gap, leaf_gap,
):
    count = whole.shape[1]
    width = whole.shape[2]
    top_size = top.shape[0]

    def step(p, sums):
        piece = whole[p]
        start = pl.multiple_of(p * width, 128)
        out = list(sums)
        for t in range(width // 128):
            at = pl.ds(start + t * 128, 128)
            rows, lower = top[:, at], below[:, at]
            for r in range(count):
                line = piece[r : r + 1, t * 128 : (t + 1) * 128]
                out[r] = out[r] + rows * line
                out[count + r] = out[count + r] + lower * line
        return tuple(out)

    zero = jnp.zeros((top_size, 128), jnp.float32)
    sums = lax.fori_loop(0, used, step, (zero,) * (2 * count))
    line = lax.broadcasted_iota(jnp.int32, (count, 128), 0)
    halves = []
    for half in range(2):
        total = None
        for r in range(count):
            ones = jnp.where(line == r, 1.0, 0.0).astype(jnp.bfloat16)
            term = weights_times_back(ones, sums[half * count + r])
            total = term if total is None else total + term
        halves.append(total)
    own, lower = halves
    pair_out[...] = own

    def against(matrix):
        return product_back(own, matrix[:, :top_size]) + product_back(lower, matrix[:, top_size:])

    second_rows, first_rows = second_own.shape[1], first_own.shape[1]
    second_gap[...] = second_own[...] - against(
        pack[SECOND_TOP : SECOND_TOP + second_rows, 0 : 2 * top_size]
    )
    first_gap[...] = first_own[...] - against(
        pack[FIRST_TOP : FIRST_TOP + first_rows, 0 : 2 * top_size]
    )
    rows = pack[TO_TOP : TO_TOP + 2 * top_size, 0 : leaf_solved.shape[1]]
    leaf_gap[...] = leaf_solved[...] - (
        product(own, rows[:top_size]) + product(lower, rows[top_size:])
    )


def second_back_body(
    sizes, side, whole, second, below, first_gap, leaf_gap, top_back, pack, sent, base_out,
    second_out,
):
    count = whole.shape[0]
    leaf_size, first_size, second_size, _ = sizes
    reach = side * 8
    own = product_back(whole[...], second[0:second_size, :])
    lower = product_back(whole[...], below[0:second_size, :])
    second_out[...] = own
    weights = pack[FIRST_SECOND : FIRST_SECOND + first_size, 0 : 2 * second_size]
    gap = first_gap[...] - product_back(own, weights[:, :second_size])
    gap = gap - product_back(lower, weights[:, second_size:])
    rows = pack[TO_SECOND : TO_SECOND + 2 * second_size, 0:leaf_size]
    rest = leaf_gap[...] - product(own, rows[:second_size]) - product(lower, rows[second_size:])
    base = product_back(rest, pack[LEAF : LEAF + leaf_size, 0:leaf_size])
    base_out[...] = base
    leaf_order, _, second_order, top_order = packed_order(pack, sizes)
    number = numbers(side, "out")
    face = times_weights_back(base, one_hot(number, leaf_order))
    face = face + times_weights_back(own, one_hot(number, second_order))
    face = face + times_weights_back(top_back[...], one_hot(number, top_order))
    sent[...] = jnp.zeros_like(sent)
    sent[0:count, 0:first_size] = gap
    sent[count : 2 * count, 0:reach] = face


def leaf_back_body(
    sizes, side, received, base, second_back, top_back, pack, first, below, above, window,
):
    count = base.shape[0]
    peers = received.shape[0]
    leaf_size, first_size, _, _ = sizes
    reach = side * 8
    whole = jnp.concatenate([received[p, 0:count, 0:first_size] for p in range(peers)], axis=1)
    total = whole.shape[1]
    own = product_back(whole, first[0:first_size, 0:total])
    lower = product_back(whole, below[0:first_size, 0:total])
    following = product_back(whole, above[0:first_size, 0:total])
    rows = pack[TO_FIRST : TO_FIRST + 2 * first_size, 0:leaf_size]
    rest = product(own, rows[:first_size]) + product(lower, rows[first_size:])
    leaf_back = base[...] - product_back(rest, pack[LEAF : LEAF + leaf_size, 0:leaf_size])
    face = jnp.zeros((count, reach), jnp.float32)
    place = lax.axis_index("gz") + 1
    for p in range(peers):
        face = face + jnp.where(place == p, received[p, count : 2 * count, 0:reach], 0.0)
    through = above[:, total : total + 2 * first_size]
    moved = product_back(following, through[:, :first_size])
    moved = moved + product_back(own, through[:, first_size:])
    lane = lax.broadcasted_iota(jnp.int32, (through.shape[0], reach), 0)
    other = lax.broadcasted_iota(jnp.int32, (through.shape[0], reach), 1)
    shift = jnp.where(lane == other + 9, 1.0, 0.0)
    face = face - times_weights(moved, shift.astype(jnp.bfloat16))
    orders = packed_order(pack, sizes)
    number = numbers(side, "out")
    layers = []
    for z in range(side):
        layer = times_weights_back(leaf_back, one_hot(number + float(z), orders[0]))
        layer = layer + times_weights_back(
            second_back[...], one_hot(number + float(z), orders[2])
        )
        layer = layer + times_weights_back(top_back[...], one_hot(number + float(z), orders[3]))
        if z == side - 1:
            layer = layer + times_weights_back(own, one_hot(number + float(z), orders[1]))
        layers.append(layer)
    layers.append(face)
    layers.append(jnp.zeros_like(face))
    cells = jnp.concatenate(layers, axis=0)
    turned = weights_times_back(eye(reach), cells)
    window[...] = turned.reshape(window.shape)


def tent(at, cell):
    distance = jnp.abs(at - 4 * cell).astype(jnp.float32)
    return jnp.maximum(1.0 - 0.25 * distance, 0.0)


def prolong_body(inner, after_x, after_y, target, out, sent):
    count, fine = out.shape[:2]
    copies = []
    cells = inner.shape[0] + 1
    window = jnp.concatenate([inner[...], after_x[...][None]], axis=0)
    row = lax.broadcasted_iota(jnp.int32, window.shape, 1)
    window = jnp.where(row == cells - 1, after_y[...][:, None, :], window)
    flat = window.reshape(cells * window.shape[1], window.shape[2])
    rows = lax.broadcasted_iota(jnp.int32, (cells * fine, cells * 8), 0)
    columns = lax.broadcasted_iota(jnp.int32, (cells * fine, cells * 8), 1)
    at = rows - (columns >> 3) * fine
    inside = (at >= 0) & (at < fine) & ((columns & 7) < cells)
    y_weights = jnp.where(inside, tent(at, columns & 7), 0.0).astype(jnp.bfloat16)
    along_y = weights_times(y_weights, flat)
    lane = lax.broadcasted_iota(jnp.int32, (window.shape[2], fine), 0)
    at = lax.broadcasted_iota(jnp.int32, (window.shape[2], fine), 1)
    for r in range(count):
        inside = ((lane & 3) == r) & ((lane >> 2) < cells)
        z_weights = jnp.where(inside, tent(at, lane >> 2), 0.0).astype(jnp.bfloat16)
        along_z = times_weights(along_y, z_weights)
        planes = [along_z[i * fine : (i + 1) * fine] for i in range(cells)]
        for i in range(cells - 1):
            for q in range(4):
                value = planes[i]
                if q:
                    value = (1.0 - q / 4.0) * value + (q / 4.0) * planes[i + 1]
                out[r, 4 * i + q] = value
        copies.append(pltpu.make_async_copy(out.at[r], target.at[r], sent.at[r]))
        copies[r].start()
    for copy in copies:
        copy.wait()


def prolonged(inner, after_x, after_y, count, fine):
    return pl.pallas_call(
        prolong_body,
        out_shape=jax.ShapeDtypeStruct((count, fine, fine, fine), jnp.float32),
        in_specs=[VMEM] * 3,
        out_specs=HBM,
        scratch_shapes=[
            pltpu.VMEM((count, fine, fine, fine), jnp.float32),
            pltpu.SemaphoreType.DMA((count,)),
        ],
        compiler_params=LIMIT,
        name="prolong_twice",
    )(inner, after_x, after_y)


def padded(values, dim, before, after):
    widths = [(0, 0)] * values.ndim
    widths[dim] = (before, after)
    return jnp.pad(values, widths)


def call(body, outs, *operands):
    shapes = tuple(jax.ShapeDtypeStruct(o, jnp.float32) for o in outs)
    return pl.pallas_call(
        body,
        out_shape=shapes,
        in_specs=[VMEM] * len(operands),
        out_specs=(VMEM,) * len(shapes),
        compiler_params=LIMIT,
    )(*operands)


def per_device(
    right_side,
    iterate,
    coefficient,
    ordering,
    leaf_inverse,
    leaf_first,
    leaf_second,
    leaf_top,
    first_inverse,
    first_second,
    first_top,
    second_inverse,
    second_top,
    top_inverse,
):
    count, fine = right_side.shape[:2]
    leaf_size = leaf_inverse.shape[-1]
    first_size = first_second.shape[3]
    second_size = second_top.shape[3]
    top_size, top_total = top_inverse.shape
    sizes = (leaf_size, first_size, second_size, top_size)
    side = fine // 4
    cells = side**3
    lanes = (side + 2) * count
    gz = lax.axis_size("gz")
    plane_peers = lax.axis_size(PLANE)

    def rows_of(block):
        return jnp.transpose(block, (0, 1, 3, 2, 4)).reshape(block.shape[3], 1, block.shape[4])

    def columns_of(block):
        return jnp.transpose(block, (0, 1, 4, 2, 3)).reshape(block.shape[4], 1, block.shape[3])

    leaf = rows_of(leaf_inverse)
    to_first = columns_of(leaf_first)
    to_second = columns_of(leaf_second)
    to_top = jnp.swapaxes(leaf_top[0, 0, 0], 0, 1)
    first_to_second = rows_of(first_second)
    first_to_top = rows_of(first_top)
    second_to_top = rows_of(second_top)
    first = jnp.transpose(first_inverse, (0, 2, 1, 3)).reshape(first_size, 1, -1)
    second = jnp.transpose(second_inverse, (1, 0, 2))
    order = ordering.reshape(1, cells)

    inner, upper = restricted(order, right_side, iterate, coefficient)
    from_x = shifted(upper, "gx", 1)
    whole_first = -(-max(first.shape[2] + 2 * first_size, cells) // 128) * 128
    up, down, beside, pack = prepared(
        sizes,
        side,
        whole_first,
        order,
        leaf,
        to_first,
        first,
        second,
        to_second,
        to_top,
        first_to_second,
        first_to_top,
        second_to_top,
    )
    first_below = shifted(up, "gz", 1)
    first_above = shifted(down, "gz", -1)
    second_below = shifted(beside, "gy", 1)
    top_below = shifted(top_inverse, "gx", 1)
    last = side + 1
    row = inner[:, last] + padded(from_x[last : last + 1, :lanes], 0, 1, side - 1)
    from_y = shifted(row, "gy", 1)

    turned, pieces = call(
        functools.partial(first_body, sizes, side, first.shape[2]),
        [(lanes, lanes_of(side)), (gz, 4 * count, 128)],
        inner,
        from_x,
        from_y,
        pack,
        up,
        first_below,
        first_above,
    )
    pieces, second_below = lax.optimization_barrier((pieces, second_below))
    received = exchanged(pieces, "gz")
    pieces, leaf_solved, first_own, toward, top_rhs = call(
        functools.partial(second_body, sizes, side, gz),
        [
            (plane_peers, 2 * count, 128),
            (count, leaf_size),
            (count, first_size),
            (count, 2 * top_size),
            (count, top_size),
        ],
        received,
        turned,
        from_x,
        pack,
        beside,
        second_below,
    )
    received = exchanged(pieces, PLANE)
    width = 128 * -(-top_total // (128 * plane_peers))
    used = top_total // width
    pieces, second_own = call(
        functools.partial(top_body, used),
        [(plane_peers, count, width), (count, second_size)],
        received,
        toward,
        top_rhs,
        pack,
        top_inverse,
        top_below,
    )
    received = exchanged(pieces, PLANE)
    (pieces,) = call(spread_sum_body, [(lax.axis_size("gx"), count, width)], received)
    received = exchanged(pieces, "gx")
    (pieces,) = call(spread_sum_body, [(plane_peers, count, width)], received)
    received = exchanged(pieces, PLANE)
    top_back, second_gap, first_gap, leaf_gap = call(
        functools.partial(top_back_body, used),
        [(count, top_size), (count, second_size), (count, first_size), (count, leaf_size)],
        received,
        top_inverse,
        top_below,
        second_own,
        first_own,
        leaf_solved,
        pack,
    )
    second_whole = jnp.moveaxis(sent_to_all(second_gap, PLANE), 0, 1).reshape(count, -1)
    sent, base, second_back = call(
        functools.partial(second_back_body, sizes, side),
        [(2 * count, 128), (count, leaf_size), (count, second_size)],
        second_whole,
        beside,
        second_below,
        first_gap,
        leaf_gap,
        top_back,
        pack,
    )
    received = sent_to_all(sent, "gz")
    (window,) = call(
        functools.partial(leaf_back_body, sizes, side),
        [(side, 8, lanes)],
        received,
        base,
        second_back,
        top_back,
        pack,
        up,
        first_below,
        first_above,
    )
    after_x = shifted(window[0], "gx", -1)
    layer = jnp.concatenate([window[:, 0], after_x[0:1]], axis=0)
    after_y = shifted(layer, "gy", -1)
    return prolonged(window, after_x, after_y, count, fine)


def solution(mesh):
    blocks = P("gx", "gy", "gz")
    return jax.shard_map(
        per_device,
        mesh=mesh,
        in_specs=(
            P(None, "gx", "gy", "gz"),
            P(None, "gx", "gy", "gz"),
            blocks,
            blocks,
            blocks,
            blocks,
            blocks,
            blocks,
            blocks,
            blocks,
            blocks,
            P("gx", PLANE, None),
            blocks,
            P(("gx", "gy", "gz"), None),
        ),
        out_specs=P(None, "gx", "gy", "gz"),
        check_vma=False,
    )
```

```python
import functools

import numpy as np
import jax
import jax.numpy as jnp
from jax import lax
from jax.experimental import pallas as pl
from jax.experimental.pallas import tpu as pltpu
from jax.sharding import PartitionSpec as P

PLANE = ("gy", "gz")
AXES = ("gx", "gy", "gz")
VMEM = pl.BlockSpec(memory_space=pltpu.VMEM)
HBM = pl.BlockSpec(memory_space=pltpu.HBM)
LIMIT = pltpu.CompilerParams(vmem_limit_bytes=16 * 1024 * 1024)


def in_hbm(values):
    return pltpu.with_memory_space_constraint(values, pltpu.HBM)


def shifted(shard, axis, by):
    peers = lax.axis_size(axis)
    pairs = [(i, i + by) for i in range(peers) if 0 <= i + by < peers]
    return lax.ppermute(shard, axis, pairs)


def exchanged(pieces, axis):
    return lax.all_to_all(pieces, axis, split_axis=0, concat_axis=0, tiled=True)


def sent_to_all(shard, axis):
    copies = jnp.broadcast_to(shard, (lax.axis_size(axis), *shard.shape))
    return exchanged(copies, axis)


def parts_of(values):
    first = values.astype(jnp.bfloat16)
    second = (values - first.astype(jnp.float32)).astype(jnp.bfloat16)
    return first, second


def dot(left, right):
    return jnp.dot(left, right, preferred_element_type=jnp.float32)


def dot_back(left, right):
    return lax.dot_general(
        left, right, (((1,), (1,)), ((), ())), preferred_element_type=jnp.float32
    )


def product(operand, matrix):
    high, low = parts_of(operand)
    first, second = parts_of(matrix)
    return dot(high, first) + (dot(high, second) + dot(low, first))


def product_back(operand, matrix):
    high, low = parts_of(operand)
    first, second = parts_of(matrix)
    return dot_back(high, first) + (dot_back(high, second) + dot_back(low, first))


def times_weights(values, weights):
    first, second = parts_of(values)
    return dot(first, weights) + dot(second, weights)


def weights_times(weights, values):
    first, second = parts_of(values)
    return dot(weights, first) + dot(weights, second)


def times_weights_back(values, weights):
    first, second = parts_of(values)
    return dot_back(first, weights) + dot_back(second, weights)


def weights_times_back(weights, values):
    first, second = parts_of(values)
    return dot_back(weights, first) + dot_back(weights, second)


def two_restrictions(distance):
    return np.maximum(0.0, 4.0 - np.abs(distance)) / 16.0


def restriction_weights(fine):
    cell = 4.0 * (np.arange(fine // 4 + 2) - 1)[:, None]
    at = np.arange(fine)[None, :]
    own = two_restrictions(cell - at)
    through_before = two_restrictions(cell - (at - 1))
    beside = through_before + two_restrictions(cell - (at + 1))
    before = np.where(at == 0, through_before, 0.0)
    return own, beside, before


def weight_rows(coarse, fine, kind, missing):
    rows = lax.broadcasted_iota(jnp.int32, (coarse * coarse, coarse * fine), 0)
    columns = lax.broadcasted_iota(jnp.int32, (coarse * coarse, coarse * fine), 1)
    at = columns - (rows >> 3) * fine
    weights = weights_at(4 * ((rows & 7) - 1), at, kind, missing)
    return jnp.where((at >= 0) & (at < fine), weights, 0.0).astype(jnp.bfloat16)


def weight_lanes(coarse, fine, count, r, kind, missing):
    at = lax.broadcasted_iota(jnp.int32, (fine, coarse * count), 0)
    lane = lax.broadcasted_iota(jnp.int32, (fine, coarse * count), 1)
    weights = weights_at(4 * ((lane >> 2) - 1), at, kind, missing)
    return jnp.where((lane & 3) == r, weights, 0.0).astype(jnp.bfloat16)


def weights_at(cell, at, kind, missing):
    def weight(distance):
        return jnp.maximum(4.0 - jnp.abs(distance).astype(jnp.float32), 0.0) * 0.0625

    if kind == "own":
        return weight(cell - at)
    before = jnp.where(at == 0, missing, 0.0)
    return weight(cell - at - 1) + (1.0 - before) * weight(cell - at + 1)


def restrict_body(
    own, beside, before, order_in, rhs_in, iterate_in, coefficient_in, inner, upper,
    rhs, iterate, coefficient, order, arrived,
):
    count, fine = rhs.shape[:2]
    coarse = own.shape[0]
    half = fine // 2
    copies = [pltpu.make_async_copy(coefficient_in, coefficient, arrived.at[0])]
    for r in range(count):
        for source, room in ((iterate_in, iterate), (rhs_in, rhs)):
            for start in (0, half):
                part = pl.ds(start, half)
                copies.append(
                    pltpu.make_async_copy(
                        source.at[r, part], room.at[r, part], arrived.at[len(copies)]
                    )
                )
    copies.append(pltpu.make_async_copy(order_in, order, arrived.at[len(copies)]))
    for copy in copies:
        copy.start()
    at_x, at_y, at_z = [jnp.where(lax.axis_index(a) == 0, 1.0, 0.0) for a in AXES]
    layer, lanes = inner.shape[1:]
    top_size = coarse - 2
    top_size = top_size * top_size
    upper[...] = jnp.zeros_like(upper)
    y_cell = weight_rows(coarse, fine, "own", None)
    y_pair = weight_rows(coarse, fine, "beside", at_y)
    z_cells = [weight_lanes(coarse, fine, count, r, "own", None) for r in range(count)]
    z_pairs = [weight_lanes(coarse, fine, count, r, "beside", at_z) for r in range(count)]
    copies[0].wait()
    beside_sum = None
    own_sum = None
    for r in range(count):
        for copy in copies[4 * r + 1 : 4 * r + 5]:
            copy.wait()
        planes = [iterate[r, x] for x in range(fine)]
        gaps = [rhs[r, x] - (6.0 + coefficient[x]) * planes[x] for x in range(fine)]
        values, cells = [], []
        for i in range(coarse):
            value = cell = None
            for x in range(fine):
                if own[i, x]:
                    term = float(own[i, x]) * gaps[x]
                    value = term if value is None else value + term
                    term = float(own[i, x]) * planes[x]
                    cell = term if cell is None else cell + term
                if beside[i, x]:
                    weight = float(beside[i, x])
                    if before[i, x]:
                        weight = weight - at_x * float(before[i, x])
                    term = weight * planes[x]
                    value = term if value is None else value + term
            values.append(value)
            cells.append(jnp.zeros_like(planes[0]) if cell is None else cell)
        value = jnp.concatenate(values, axis=0)
        cell = jnp.concatenate(cells, axis=0)
        term = times_weights(value, z_cells[r]) + times_weights(cell, z_pairs[r])
        beside_sum = term if beside_sum is None else beside_sum + term
        term = times_weights(cell, z_cells[r])
        own_sum = term if own_sum is None else own_sum + term
    result = weights_times(y_cell, beside_sum) + weights_times(y_pair, own_sum)
    result = result.reshape(coarse, coarse, coarse * count)
    inner[...] = result[:-1]
    upper[0:layer, 0:lanes] = result[coarse - 1]
    copies[-1].wait()
    orders = order[...].astype(jnp.float32)
    upper[layer : layer + 1, 0:top_size] = orders[:, orders.shape[1] - top_size :]


def restricted(order, right_side, iterate, coefficient):
    count, fine = right_side.shape[:2]
    own, beside, before = restriction_weights(fine)
    coarse = own.shape[0]

    def body(*refs):
        restrict_body(own, beside, before, *refs)

    inner = jax.ShapeDtypeStruct((coarse - 1, coarse, coarse * count), jnp.float32)
    upper = jax.ShapeDtypeStruct((2 * coarse, 128), jnp.float32)
    return pl.pallas_call(
        body,
        out_shape=(inner, upper),
        in_specs=[HBM] * 4,
        out_specs=(VMEM,) * 2,
        scratch_shapes=[
            pltpu.VMEM(right_side.shape, jnp.float32),
            pltpu.VMEM(iterate.shape, jnp.float32),
            pltpu.VMEM(coefficient.shape, jnp.float32),
            pltpu.VMEM(order.shape, order.dtype),
            pltpu.SemaphoreType.DMA((4 * count + 2,)),
        ],
        compiler_params=LIMIT,
        name="restrict_twice",
    )(*map(in_hbm, (order, right_side, iterate, coefficient)))


def numbers(side, kind):
    lane = lax.broadcasted_iota(jnp.int32, (lanes_of(side, kind), 1), 0)
    x, y = lane >> 3, lane & 7
    if kind == "out":
        number = jnp.where(y < side, x * side * side + y * side, -1000)
        return number.astype(jnp.float32)
    x, y = x - 1, y - 1
    last = side - 1
    along_y = (y >= 0) & (y < side)
    if kind == "in":
        number = jnp.where((x >= 0) & along_y, x * side * side + y * side, -1000)
    elif kind == "before_y":
        number = jnp.where((x >= 0) & (y < 0), x * side * side + last * side, -1000)
    else:
        number = jnp.where((x < 0) & along_y, last * side * side + y * side, -1000)
    return number.astype(jnp.float32)


def lanes_of(side, kind="in"):
    return side * 8 if kind == "out" else (side + 1) * 8


def one_hot(number, order):
    return jnp.where(number == order, 1.0, 0.0).astype(jnp.bfloat16)


def eye(size):
    rows = lax.broadcasted_iota(jnp.int32, (size, size), 0)
    return jnp.where(rows == lax.broadcasted_iota(jnp.int32, (size, size), 1), 1.0, 0.0).astype(
        jnp.bfloat16
    )


def picked(cells, count, side, number, order, layers=None):
    total = None
    for z in range(side) if layers is None else layers:
        layer = cells[(z + 1) * count : (z + 2) * count]
        term = times_weights(layer, one_hot(number + float(z), order))
        total = term if total is None else total + term
    return total


LEAF, TO_FIRST, TO_SECOND, TO_TOP = 0, 128, 184, 248
FIRST_SECOND, FIRST_TOP, SECOND_TOP, ORDER, PACKED = 320, 352, 384, 416, 424


def split_order(order, sizes):
    out, start = [], 0
    for size in sizes:
        out.append(order[:, start : start + size])
        start += size
    return out


def packed_order(pack, sizes):
    leaf_size = sizes[0]
    leaf_order = pack[ORDER : ORDER + 1, 0:leaf_size]
    rest = pack[ORDER + 1 : ORDER + 2, 0 : sum(sizes[1:])]
    return [leaf_order] + split_order(rest, sizes[1:])


def prepare_body(sizes, side, *refs):
    sources, (up, down, beside, pack) = refs[:10], refs[10:14]
    held, arrived = refs[14:24], refs[24]
    copies = [
        pltpu.make_async_copy(source, room, arrived.at[n])
        for n, (source, room) in enumerate(zip(sources, held))
    ]
    for copy in copies:
        copy.start()
    up[...] = jnp.zeros_like(up)
    down[...] = jnp.zeros_like(down)
    beside[sizes[2] :, :] = jnp.zeros_like(beside[sizes[2] :, :])
    for copy in copies:
        copy.wait()
    order, leaf, to_first, first, second = held[:5]
    to_second, to_top, first_second, first_top, second_top = held[5:]
    order = order[...].astype(jnp.float32)
    leaf_size, first_size, second_size = sizes[:3]
    leaf_rows, first_columns = leaf[:, 0, :], to_first[:, 0, :]
    first_rows = first[:, 0, :]
    face = one_hot(numbers(side, "in"), order[:, :leaf_size])
    rows = weights_times(face, leaf_rows)
    up[0:first_size, 0 : first_rows.shape[1]] = first_rows
    up[first_size : first_size + 1, 0 : order.shape[1]] = order
    total = first_rows.shape[1]
    down[:, total : total + 2 * first_size] = product_back(rows, first_columns)
    down[0:first_size, 0:total] = first_rows
    beside[0:second_size, :] = second[:, 0, :]
    beside[second_size : second_size + 1, 0 : order.shape[1]] = order
    pack[ORDER : ORDER + 1, 0:leaf_size] = order[:, :leaf_size]
    pack[ORDER + 1 : ORDER + 2, 0 : order.shape[1] - leaf_size] = order[:, leaf_size:]
    for start, rows in (
        (LEAF, leaf_rows),
        (TO_FIRST, first_columns),
        (TO_SECOND, to_second[:, 0, :]),
        (TO_TOP, to_top[...]),
        (FIRST_SECOND, first_second[:, 0, :]),
        (FIRST_TOP, first_top[:, 0, :]),
        (SECOND_TOP, second_top[:, 0, :]),
    ):
        pack[start : start + rows.shape[0], 0 : rows.shape[1]] = rows


def prepared(sizes, side, width, *sources):
    leaf_size, first_size, second_size, top_size = sizes
    assert leaf_size <= 128 and first_size < 32 and second_size < 32 and top_size <= 36
    shapes = (
        (32, width),
        (lanes_of(side), width),
        (40, sources[4].shape[2]),
        (PACKED, 128),
    )
    return pl.pallas_call(
        functools.partial(prepare_body, sizes, side),
        out_shape=tuple(jax.ShapeDtypeStruct(o, jnp.float32) for o in shapes),
        in_specs=[HBM] * len(sources),
        out_specs=(VMEM,) * len(shapes),
        scratch_shapes=[pltpu.VMEM(x.shape, x.dtype) for x in sources]
        + [pltpu.SemaphoreType.DMA((len(sources),))],
        compiler_params=LIMIT,
        name="prepare",
    )(*sources)


LAYER = 32


def message_body(inner, from_x, _, message):
    along, lanes = inner.shape[1:]
    rows = inner[:, along - 1, :]
    row = lax.broadcasted_iota(jnp.int32, rows.shape, 0)
    rows = rows + jnp.where(row == 1, from_x[along - 1 : along, 0:lanes], 0.0)
    message[LAYER : LAYER + rows.shape[0], 0:lanes] = rows


def with_layer(inner, from_x, beside):
    return pl.pallas_call(
        message_body,
        out_shape=jax.ShapeDtypeStruct(beside.shape, jnp.float32),
        in_specs=[VMEM] * 3,
        out_specs=VMEM,
        input_output_aliases={2: 0},
        compiler_params=LIMIT,
        name="y_message",
    )(inner, from_x, beside)


def first_body(
    sizes, side, total, inner, from_x, from_y, pack, first, below, above, cells_out, pieces
):
    count = pieces.shape[1] // 4
    peers = pieces.shape[0]
    first_size = sizes[1]
    leaf_size = sizes[0]
    leaf_order, first_order = packed_order(pack, sizes)[:2]
    values = inner[...]
    across, along, lanes = values.shape
    reach = across * along
    row = lax.broadcasted_iota(jnp.int32, values.shape, 0)
    values = values + jnp.where(row == 1, from_x[0:along, 0:lanes][None], 0.0)
    row = lax.broadcasted_iota(jnp.int32, values.shape, 1)
    layer = from_y[LAYER : LAYER + across, 0:lanes]
    values = values + jnp.where(row == 1, layer[:, None, :], 0.0)
    cells = weights_times_back(eye(lanes), values.reshape(reach, lanes))
    cells_out[...] = cells
    number = numbers(side, "in")
    leaf_rhs = picked(cells, count, side, number, leaf_order)
    first_rhs = picked(cells, count, side, number, first_order, [side - 1])
    after = cells[(side + 1) * count : (side + 2) * count]
    before = cells[0:count]
    leaf = pack[LEAF : LEAF + leaf_size, 0:leaf_size]
    to_first = pack[TO_FIRST : TO_FIRST + 2 * first_size, 0:leaf_size]
    toward = product_back(product(leaf_rhs, leaf), to_first)
    whole = total
    own_rows = first[0:first_size, 0:whole]
    below_rows = below[0:first_size, 0:whole]
    below_order = below[first_size : first_size + 1, 0 : sum(sizes)]
    below_order = split_order(below_order, sizes)[1]
    from_before = times_weights(before, one_hot(number + float(side - 1), below_order))
    through = product(after, above[:, whole : whole + 2 * first_size])
    above_rows = above[0:first_size, 0:whole]
    terms = product(first_rhs - toward[:, :first_size] - through[:, first_size:], own_rows)
    terms = terms + product(from_before - toward[:, first_size:], below_rows)
    terms = terms - product(through[:, :first_size], above_rows)
    pieces[...] = jnp.zeros_like(pieces)
    place = lax.axis_index("gz")
    for p in range(peers):
        pieces[p, 0:count, 0:first_size] = terms[:, p * first_size : (p + 1) * first_size]
        pieces[p, count : 2 * count, 0:reach] = jnp.where(place + 1 == p, after, 0.0)
        pieces[p, 2 * count : 3 * count, 0:reach] = jnp.where(place - 1 == p, before, 0.0)


def second_body(
    sizes, side, gz, received, cells, from_x, pack, second, below, pieces, leaf_out, first_out,
    toward_out, top_out,
):
    peers, rows = pieces.shape[:2]
    count = rows // 2
    leaf_size, first_size, second_size, top_size = sizes
    reach = cells.shape[1]
    total = received[0]
    for p in range(1, received.shape[0]):
        total = total + received[p]
    first_own = total[0:count, 0:first_size]
    cells = cells[...]
    after = total[count : 2 * count, 0:reach]
    before = total[2 * count : 3 * count, 0:reach]
    cells = jnp.concatenate(
        [
            cells[0:count],
            cells[count : 2 * count] + after,
            cells[2 * count : side * count],
            cells[side * count : (side + 1) * count] + before,
            cells[(side + 1) * count :],
        ],
        axis=0,
    )
    leaf_order, _, second_order, top_order = packed_order(pack, sizes)
    number = numbers(side, "in")
    leaf = pack[LEAF : LEAF + leaf_size, 0:leaf_size]
    to_second = pack[TO_SECOND : TO_SECOND + 2 * second_size, 0:leaf_size]
    to_top = pack[TO_TOP : TO_TOP + 2 * top_size, 0:leaf_size]
    first_second = pack[FIRST_SECOND : FIRST_SECOND + first_size, 0 : 2 * second_size]
    first_top = pack[FIRST_TOP : FIRST_TOP + first_size, 0 : 2 * top_size]
    leaf_solved = product(picked(cells, count, side, number, leaf_order), leaf)
    second_rhs = picked(cells, count, side, number, second_order)
    top_out[...] = picked(cells, count, side, number, top_order)
    below_order = below[second_size : second_size + 1, 0 : sum(sizes)]
    _, _, below_second, below_top = split_order(below_order, sizes)
    number = numbers(side, "before_y")
    from_before = picked(cells, count, side, number, below_second)
    top_before = picked(cells, count, side, number, below_top)
    toward = product_back(leaf_solved, to_second) + product(first_own, first_second)
    terms = product(second_rhs - toward[:, :second_size], second[0:second_size, :])
    terms = terms + product(from_before - toward[:, second_size:], below[0:second_size, :])
    pieces[...] = jnp.zeros_like(pieces)
    place = (lax.axis_index("gy") - 1) * gz + lax.axis_index("gz")
    for p in range(peers):
        pieces[p, 0:count, 0:second_size] = terms[:, p * second_size : (p + 1) * second_size]
        pieces[p, count : 2 * count, 0:top_size] = jnp.where(place == p, top_before, 0.0)
    leaf_out[...] = leaf_solved
    first_out[...] = first_own
    toward = product_back(leaf_solved, to_top) + product(first_own, first_top)
    order_x = from_x[8:9, 0:top_size]
    before_x = picked(cells, count, side, numbers(side, "before_x"), order_x)
    toward_out[:, :top_size] = toward[:, :top_size]
    toward_out[:, top_size:] = toward[:, top_size:] - before_x


def top_body(used, received, toward, rhs, pack, top, below, pieces, second_out):
    count = toward.shape[0]
    second_size = second_out.shape[1]
    top_size = rhs.shape[1]
    total = received[0]
    for p in range(1, received.shape[0]):
        total = total + received[p]
    second_own = total[0:count, 0:second_size]
    second_out[...] = second_own
    second_top = pack[SECOND_TOP : SECOND_TOP + second_size, 0 : 2 * top_size]
    toward = toward[...] + product(second_own, second_top)
    own = rhs[...] + total[count : 2 * count, 0:top_size] - toward[:, :top_size]
    other = toward[:, top_size:]
    width = pieces.shape[2]
    vectors = []
    for vector in (own, -other):
        high, low = parts_of(vector)
        both = jnp.concatenate([high.astype(jnp.float32), low.astype(jnp.float32)], axis=0)
        vectors.append((both.astype(jnp.bfloat16), high))
    for p in range(used):
        at = slice(p * width, (p + 1) * width)
        total = None
        for (both, high), rows in zip(vectors, (top, below)):
            first, second = parts_of(rows[:, at])
            term = dot(both, first)
            term = term[:count] + (term[count:] + dot(high, second))
            total = term if total is None else total + term
        pieces[p] = total
    for p in range(used, pieces.shape[0]):
        pieces[p] = jnp.zeros(pieces.shape[1:], jnp.float32)


def spread_sum_body(received, out):
    total = received[0]
    for p in range(1, received.shape[0]):
        total = total + received[p]
    for p in range(out.shape[0]):
        out[p] = total


def top_back_body(
    used, whole, top, below, second_own, first_own, leaf_solved, pack, pair_out, second_gap,
    first_gap, leaf_gap,
):
    count = whole.shape[1]
    width = whole.shape[2]
    top_size = top.shape[0]

    def step(p, sums):
        piece = whole[p]
        start = pl.multiple_of(p * width, 128)
        out = list(sums)
        for t in range(width // 128):
            at = pl.ds(start + t * 128, 128)
            rows, lower = top[:, at], below[:, at]
            for r in range(count):
                line = piece[r : r + 1, t * 128 : (t + 1) * 128]
                out[r] = out[r] + rows * line
                out[count + r] = out[count + r] + lower * line
        return tuple(out)

    zero = jnp.zeros((top_size, 128), jnp.float32)
    sums = lax.fori_loop(0, used, step, (zero,) * (2 * count))
    line = lax.broadcasted_iota(jnp.int32, (count, 128), 0)
    halves = []
    for half in range(2):
        total = None
        for r in range(count):
            ones = jnp.where(line == r, 1.0, 0.0).astype(jnp.bfloat16)
            term = weights_times_back(ones, sums[half * count + r])
            total = term if total is None else total + term
        halves.append(total)
    own, lower = halves
    pair_out[...] = own

    def against(matrix):
        return product_back(own, matrix[:, :top_size]) + product_back(lower, matrix[:, top_size:])

    second_rows, first_rows = second_own.shape[1], first_own.shape[1]
    second_gap[...] = second_own[...] - against(
        pack[SECOND_TOP : SECOND_TOP + second_rows, 0 : 2 * top_size]
    )
    first_gap[...] = first_own[...] - against(
        pack[FIRST_TOP : FIRST_TOP + first_rows, 0 : 2 * top_size]
    )
    rows = pack[TO_TOP : TO_TOP + 2 * top_size, 0 : leaf_solved.shape[1]]
    leaf_gap[...] = leaf_solved[...] - (
        product(own, rows[:top_size]) + product(lower, rows[top_size:])
    )


def second_back_body(
    sizes, side, whole, second, below, first_gap, leaf_gap, top_back, pack, sent, base_out,
    second_out,
):
    count = whole.shape[0]
    leaf_size, first_size, second_size, _ = sizes
    reach = side * 8
    own = product_back(whole[...], second[0:second_size, :])
    lower = product_back(whole[...], below[0:second_size, :])
    second_out[...] = own
    weights = pack[FIRST_SECOND : FIRST_SECOND + first_size, 0 : 2 * second_size]
    gap = first_gap[...] - product_back(own, weights[:, :second_size])
    gap = gap - product_back(lower, weights[:, second_size:])
    rows = pack[TO_SECOND : TO_SECOND + 2 * second_size, 0:leaf_size]
    rest = leaf_gap[...] - product(own, rows[:second_size]) - product(lower, rows[second_size:])
    base = product_back(rest, pack[LEAF : LEAF + leaf_size, 0:leaf_size])
    base_out[...] = base
    leaf_order, _, second_order, top_order = packed_order(pack, sizes)
    number = numbers(side, "out")
    face = times_weights_back(base, one_hot(number, leaf_order))
    face = face + times_weights_back(own, one_hot(number, second_order))
    face = face + times_weights_back(top_back[...], one_hot(number, top_order))
    sent[...] = jnp.zeros_like(sent)
    sent[0:count, 0:first_size] = gap
    sent[count : 2 * count, 0:reach] = face


def leaf_back_body(
    sizes, side, received, base, second_back, top_back, pack, first, below, above, window,
):
    count = base.shape[0]
    peers = received.shape[0]
    leaf_size, first_size, _, _ = sizes
    reach = side * 8
    whole = jnp.concatenate([received[p, 0:count, 0:first_size] for p in range(peers)], axis=1)
    total = whole.shape[1]
    own = product_back(whole, first[0:first_size, 0:total])
    lower = product_back(whole, below[0:first_size, 0:total])
    following = product_back(whole, above[0:first_size, 0:total])
    rows = pack[TO_FIRST : TO_FIRST + 2 * first_size, 0:leaf_size]
    rest = product(own, rows[:first_size]) + product(lower, rows[first_size:])
    leaf_back = base[...] - product_back(rest, pack[LEAF : LEAF + leaf_size, 0:leaf_size])
    face = jnp.zeros((count, reach), jnp.float32)
    place = lax.axis_index("gz") + 1
    for p in range(peers):
        face = face + jnp.where(place == p, received[p, count : 2 * count, 0:reach], 0.0)
    through = above[:, total : total + 2 * first_size]
    moved = product_back(following, through[:, :first_size])
    moved = moved + product_back(own, through[:, first_size:])
    lane = lax.broadcasted_iota(jnp.int32, (through.shape[0], reach), 0)
    other = lax.broadcasted_iota(jnp.int32, (through.shape[0], reach), 1)
    shift = jnp.where(lane == other + 9, 1.0, 0.0)
    face = face - times_weights(moved, shift.astype(jnp.bfloat16))
    orders = packed_order(pack, sizes)
    number = numbers(side, "out")
    layers = []
    for z in range(side):
        layer = times_weights_back(leaf_back, one_hot(number + float(z), orders[0]))
        layer = layer + times_weights_back(
            second_back[...], one_hot(number + float(z), orders[2])
        )
        layer = layer + times_weights_back(top_back[...], one_hot(number + float(z), orders[3]))
        if z == side - 1:
            layer = layer + times_weights_back(own, one_hot(number + float(z), orders[1]))
        layers.append(layer)
    layers.append(face)
    layers.append(jnp.zeros_like(face))
    cells = jnp.concatenate(layers, axis=0)
    turned = weights_times_back(eye(reach), cells)
    window[...] = turned.reshape(window.shape)


def tent(at, cell):
    distance = jnp.abs(at - 4 * cell).astype(jnp.float32)
    return jnp.maximum(1.0 - 0.25 * distance, 0.0)


def prolong_body(inner, after_x, after_y, target, out, sent):
    count, fine = out.shape[:2]
    copies = []
    cells = inner.shape[0] + 1
    window = jnp.concatenate([inner[...], after_x[...][None]], axis=0)
    row = lax.broadcasted_iota(jnp.int32, window.shape, 1)
    window = jnp.where(row == cells - 1, after_y[...][:, None, :], window)
    flat = window.reshape(cells * window.shape[1], window.shape[2])
    rows = lax.broadcasted_iota(jnp.int32, (cells * fine, cells * 8), 0)
    columns = lax.broadcasted_iota(jnp.int32, (cells * fine, cells * 8), 1)
    at = rows - (columns >> 3) * fine
    inside = (at >= 0) & (at < fine) & ((columns & 7) < cells)
    y_weights = jnp.where(inside, tent(at, columns & 7), 0.0).astype(jnp.bfloat16)
    along_y = weights_times(y_weights, flat)
    lane = lax.broadcasted_iota(jnp.int32, (window.shape[2], fine), 0)
    at = lax.broadcasted_iota(jnp.int32, (window.shape[2], fine), 1)
    for r in range(count):
        inside = ((lane & 3) == r) & ((lane >> 2) < cells)
        z_weights = jnp.where(inside, tent(at, lane >> 2), 0.0).astype(jnp.bfloat16)
        along_z = times_weights(along_y, z_weights)
        planes = [along_z[i * fine : (i + 1) * fine] for i in range(cells)]
        for i in range(cells - 1):
            for q in range(4):
                value = planes[i]
                if q:
                    value = (1.0 - q / 4.0) * value + (q / 4.0) * planes[i + 1]
                out[r, 4 * i + q] = value
        copies.append(pltpu.make_async_copy(out.at[r], target.at[r], sent.at[r]))
        copies[r].start()
    for copy in copies:
        copy.wait()


def prolonged(inner, after_x, after_y, count, fine):
    return pl.pallas_call(
        prolong_body,
        out_shape=jax.ShapeDtypeStruct((count, fine, fine, fine), jnp.float32),
        in_specs=[VMEM] * 3,
        out_specs=HBM,
        scratch_shapes=[
            pltpu.VMEM((count, fine, fine, fine), jnp.float32),
            pltpu.SemaphoreType.DMA((count,)),
        ],
        compiler_params=LIMIT,
        name="prolong_twice",
    )(inner, after_x, after_y)


def call(body, outs, *operands):
    shapes = tuple(jax.ShapeDtypeStruct(o, jnp.float32) for o in outs)
    return pl.pallas_call(
        body,
        out_shape=shapes,
        in_specs=[VMEM] * len(operands),
        out_specs=(VMEM,) * len(shapes),
        compiler_params=LIMIT,
    )(*operands)


def per_device(
    right_side,
    iterate,
    coefficient,
    ordering,
    leaf_inverse,
    leaf_first,
    leaf_second,
    leaf_top,
    first_inverse,
    first_second,
    first_top,
    second_inverse,
    second_top,
    top_inverse,
):
    count, fine = right_side.shape[:2]
    leaf_size = leaf_inverse.shape[-1]
    first_size = first_second.shape[3]
    second_size = second_top.shape[3]
    top_size, top_total = top_inverse.shape
    sizes = (leaf_size, first_size, second_size, top_size)
    side = fine // 4
    cells = side**3
    lanes = (side + 2) * count
    gz = lax.axis_size("gz")
    plane_peers = lax.axis_size(PLANE)

    def rows_of(block):
        return jnp.transpose(block, (0, 1, 3, 2, 4)).reshape(block.shape[3], 1, block.shape[4])

    def columns_of(block):
        return jnp.transpose(block, (0, 1, 4, 2, 3)).reshape(block.shape[4], 1, block.shape[3])

    leaf = rows_of(leaf_inverse)
    to_first = columns_of(leaf_first)
    to_second = columns_of(leaf_second)
    to_top = jnp.swapaxes(leaf_top[0, 0, 0], 0, 1)
    first_to_second = rows_of(first_second)
    first_to_top = rows_of(first_top)
    second_to_top = rows_of(second_top)
    first = jnp.transpose(first_inverse, (0, 2, 1, 3)).reshape(first_size, 1, -1)
    second = jnp.transpose(second_inverse, (1, 0, 2))
    order = ordering.reshape(1, cells)

    inner, upper = restricted(order, right_side, iterate, coefficient)
    from_x = shifted(upper, "gx", 1)
    whole_first = -(-max(first.shape[2] + 2 * first_size, cells) // 128) * 128
    up, down, beside, pack = prepared(
        sizes,
        side,
        whole_first,
        order,
        leaf,
        to_first,
        first,
        second,
        to_second,
        to_top,
        first_to_second,
        first_to_top,
        second_to_top,
    )
    first_below = shifted(up, "gz", 1)
    first_above = shifted(down, "gz", -1)
    top_below = shifted(top_inverse, "gx", 1)
    beside = with_layer(inner, from_x, beside)
    second_below = shifted(beside, "gy", 1)

    turned, pieces = call(
        functools.partial(first_body, sizes, side, first.shape[2]),
        [(lanes, lanes_of(side)), (gz, 4 * count, 128)],
        inner,
        from_x,
        second_below,
        pack,
        up,
        first_below,
        first_above,
    )
    received = exchanged(pieces, "gz")
    pieces, leaf_solved, first_own, toward, top_rhs = call(
        functools.partial(second_body, sizes, side, gz),
        [
            (plane_peers, 2 * count, 128),
            (count, leaf_size),
            (count, first_size),
            (count, 2 * top_size),
            (count, top_size),
        ],
        received,
        turned,
        from_x,
        pack,
        beside,
        second_below,
    )
    received = exchanged(pieces, PLANE)
    width = 128 * -(-top_total // (128 * plane_peers))
    used = top_total // width
    pieces, second_own = call(
        functools.partial(top_body, used),
        [(plane_peers, count, width), (count, second_size)],
        received,
        toward,
        top_rhs,
        pack,
        top_inverse,
        top_below,
    )
    received = exchanged(pieces, PLANE)
    (pieces,) = call(spread_sum_body, [(lax.axis_size("gx"), count, width)], received)
    received = exchanged(pieces, "gx")
    (pieces,) = call(spread_sum_body, [(plane_peers, count, width)], received)
    received = exchanged(pieces, PLANE)
    top_back, second_gap, first_gap, leaf_gap = call(
        functools.partial(top_back_body, used),
        [(count, top_size), (count, second_size), (count, first_size), (count, leaf_size)],
        received,
        top_inverse,
        top_below,
        second_own,
        first_own,
        leaf_solved,
        pack,
    )
    second_whole = jnp.moveaxis(sent_to_all(second_gap, PLANE), 0, 1).reshape(count, -1)
    sent, base, second_back = call(
        functools.partial(second_back_body, sizes, side),
        [(2 * count, 128), (count, leaf_size), (count, second_size)],
        second_whole,
        beside,
        second_below,
        first_gap,
        leaf_gap,
        top_back,
        pack,
    )
    received = sent_to_all(sent, "gz")
    (window,) = call(
        functools.partial(leaf_back_body, sizes, side),
        [(side, 8, lanes)],
        received,
        base,
        second_back,
        top_back,
        pack,
        up,
        first_below,
        first_above,
    )
    after_x = shifted(window[0], "gx", -1)
    layer = jnp.concatenate([window[:, 0], after_x[0:1]], axis=0)
    after_y = shifted(layer, "gy", -1)
    return prolonged(window, after_x, after_y, count, fine)


def solution(mesh):
    blocks = P("gx", "gy", "gz")
    return jax.shard_map(
        per_device,
        mesh=mesh,
        in_specs=(
            P(None, "gx", "gy", "gz"),
            P(None, "gx", "gy", "gz"),
            blocks,
            blocks,
            blocks,
            blocks,
            blocks,
            blocks,
            blocks,
            blocks,
            blocks,
            P("gx", PLANE, None),
            blocks,
            P(("gx", "gy", "gz"), None),
        ),
        out_specs=P(None, "gx", "gy", "gz"),
        check_vma=False,
    )
```

```python
import functools

import numpy as np
import jax
import jax.numpy as jnp
from jax import lax
from jax.experimental import pallas as pl
from jax.experimental.pallas import tpu as pltpu
from jax.sharding import PartitionSpec as P

PLANE = ("gy", "gz")
AXES = ("gx", "gy", "gz")
VMEM = pl.BlockSpec(memory_space=pltpu.VMEM)
HBM = pl.BlockSpec(memory_space=pltpu.HBM)
LIMIT = pltpu.CompilerParams(vmem_limit_bytes=16 * 1024 * 1024)


def in_hbm(values):
    return pltpu.with_memory_space_constraint(values, pltpu.HBM)


def shifted(shard, axis, by):
    peers = lax.axis_size(axis)
    pairs = [(i, i + by) for i in range(peers) if 0 <= i + by < peers]
    return lax.ppermute(shard, axis, pairs)


def exchanged(pieces, axis):
    return lax.all_to_all(pieces, axis, split_axis=0, concat_axis=0, tiled=True)


def sent_to_all(shard, axis):
    copies = jnp.broadcast_to(shard, (lax.axis_size(axis), *shard.shape))
    return exchanged(copies, axis)


def parts_of(values):
    first = values.astype(jnp.bfloat16)
    second = (values - first.astype(jnp.float32)).astype(jnp.bfloat16)
    return first, second


def dot(left, right):
    return jnp.dot(left, right, preferred_element_type=jnp.float32)


def dot_back(left, right):
    return lax.dot_general(
        left, right, (((1,), (1,)), ((), ())), preferred_element_type=jnp.float32
    )


def product(operand, matrix):
    high, low = parts_of(operand)
    first, second = parts_of(matrix)
    return dot(high, first) + (dot(high, second) + dot(low, first))


def product_back(operand, matrix):
    high, low = parts_of(operand)
    first, second = parts_of(matrix)
    return dot_back(high, first) + (dot_back(high, second) + dot_back(low, first))


def times_weights(values, weights):
    first, second = parts_of(values)
    return dot(first, weights) + dot(second, weights)


def weights_times(weights, values):
    first, second = parts_of(values)
    return dot(weights, first) + dot(weights, second)


def times_weights_back(values, weights):
    first, second = parts_of(values)
    return dot_back(first, weights) + dot_back(second, weights)


def weights_times_back(weights, values):
    first, second = parts_of(values)
    return dot_back(weights, first) + dot_back(weights, second)


def two_restrictions(distance):
    return np.maximum(0.0, 4.0 - np.abs(distance)) / 16.0


def restriction_weights(fine):
    cell = 4.0 * (np.arange(fine // 4 + 2) - 1)[:, None]
    at = np.arange(fine)[None, :]
    own = two_restrictions(cell - at)
    through_before = two_restrictions(cell - (at - 1))
    beside = through_before + two_restrictions(cell - (at + 1))
    before = np.where(at == 0, through_before, 0.0)
    return own, beside, before


def weight_rows(coarse, fine, kind, missing):
    rows = lax.broadcasted_iota(jnp.int32, (coarse * coarse, coarse * fine), 0)
    columns = lax.broadcasted_iota(jnp.int32, (coarse * coarse, coarse * fine), 1)
    at = columns - (rows >> 3) * fine
    weights = weights_at(4 * ((rows & 7) - 1), at, kind, missing)
    return jnp.where((at >= 0) & (at < fine), weights, 0.0).astype(jnp.bfloat16)


def weight_lanes(coarse, fine, count, r, kind, missing):
    at = lax.broadcasted_iota(jnp.int32, (fine, coarse * count), 0)
    lane = lax.broadcasted_iota(jnp.int32, (fine, coarse * count), 1)
    weights = weights_at(4 * ((lane >> 2) - 1), at, kind, missing)
    return jnp.where((lane & 3) == r, weights, 0.0).astype(jnp.bfloat16)


def weights_at(cell, at, kind, missing):
    def weight(distance):
        return jnp.maximum(4.0 - jnp.abs(distance).astype(jnp.float32), 0.0) * 0.0625

    if kind == "own":
        return weight(cell - at)
    before = jnp.where(at == 0, missing, 0.0)
    return weight(cell - at - 1) + (1.0 - before) * weight(cell - at + 1)


def restrict_body(
    own, beside, before, order_in, rhs_in, iterate_in, coefficient_in, inner, upper,
    rhs, iterate, coefficient, order, arrived,
):
    count, fine = rhs.shape[:2]
    coarse = own.shape[0]
    half = fine // 2
    copies = [pltpu.make_async_copy(coefficient_in, coefficient, arrived.at[0])]
    for r in range(count):
        for source, room in ((iterate_in, iterate), (rhs_in, rhs)):
            for start in (0, half):
                part = pl.ds(start, half)
                copies.append(
                    pltpu.make_async_copy(
                        source.at[r, part], room.at[r, part], arrived.at[len(copies)]
                    )
                )
    copies.append(pltpu.make_async_copy(order_in, order, arrived.at[len(copies)]))
    for copy in copies:
        copy.start()
    at_x, at_y, at_z = [jnp.where(lax.axis_index(a) == 0, 1.0, 0.0) for a in AXES]
    layer, lanes = inner.shape[1:]
    top_size = coarse - 2
    top_size = top_size * top_size
    upper[...] = jnp.zeros_like(upper)
    y_cell = weight_rows(coarse, fine, "own", None)
    y_pair = weight_rows(coarse, fine, "beside", at_y)
    z_cells = [weight_lanes(coarse, fine, count, r, "own", None) for r in range(count)]
    z_pairs = [weight_lanes(coarse, fine, count, r, "beside", at_z) for r in range(count)]
    copies[0].wait()
    beside_sum = None
    own_sum = None
    for r in range(count):
        for copy in copies[4 * r + 1 : 4 * r + 5]:
            copy.wait()
        planes = [iterate[r, x] for x in range(fine)]
        gaps = [rhs[r, x] - (6.0 + coefficient[x]) * planes[x] for x in range(fine)]
        values, cells = [], []
        for i in range(coarse):
            value = cell = None
            for x in range(fine):
                if own[i, x]:
                    term = float(own[i, x]) * gaps[x]
                    value = term if value is None else value + term
                    term = float(own[i, x]) * planes[x]
                    cell = term if cell is None else cell + term
                if beside[i, x]:
                    weight = float(beside[i, x])
                    if before[i, x]:
                        weight = weight - at_x * float(before[i, x])
                    term = weight * planes[x]
                    value = term if value is None else value + term
            values.append(value)
            cells.append(jnp.zeros_like(planes[0]) if cell is None else cell)
        value = jnp.concatenate(values, axis=0)
        cell = jnp.concatenate(cells, axis=0)
        term = times_weights(value, z_cells[r]) + times_weights(cell, z_pairs[r])
        beside_sum = term if beside_sum is None else beside_sum + term
        term = times_weights(cell, z_cells[r])
        own_sum = term if own_sum is None else own_sum + term
    result = weights_times(y_cell, beside_sum) + weights_times(y_pair, own_sum)
    result = result.reshape(coarse, coarse, coarse * count)
    inner[...] = result[:-1]
    upper[0:layer, 0:lanes] = result[coarse - 1]
    copies[-1].wait()
    orders = order[...].astype(jnp.float32)
    upper[layer : layer + 1, 0:top_size] = orders[:, orders.shape[1] - top_size :]


def restricted(order, right_side, iterate, coefficient):
    count, fine = right_side.shape[:2]
    own, beside, before = restriction_weights(fine)
    coarse = own.shape[0]

    def body(*refs):
        restrict_body(own, beside, before, *refs)

    inner = jax.ShapeDtypeStruct((coarse - 1, coarse, coarse * count), jnp.float32)
    upper = jax.ShapeDtypeStruct((2 * coarse, 128), jnp.float32)
    return pl.pallas_call(
        body,
        out_shape=(inner, upper),
        in_specs=[HBM] * 4,
        out_specs=(VMEM,) * 2,
        scratch_shapes=[
            pltpu.VMEM(right_side.shape, jnp.float32),
            pltpu.VMEM(iterate.shape, jnp.float32),
            pltpu.VMEM(coefficient.shape, jnp.float32),
            pltpu.VMEM(order.shape, order.dtype),
            pltpu.SemaphoreType.DMA((4 * count + 2,)),
        ],
        compiler_params=LIMIT,
        name="restrict_twice",
    )(*map(in_hbm, (order, right_side, iterate, coefficient)))


def numbers(side, kind):
    lane = lax.broadcasted_iota(jnp.int32, (lanes_of(side, kind), 1), 0)
    x, y = lane >> 3, lane & 7
    if kind == "out":
        number = jnp.where(y < side, x * side * side + y * side, -1000)
        return number.astype(jnp.float32)
    x, y = x - 1, y - 1
    last = side - 1
    along_y = (y >= 0) & (y < side)
    if kind == "in":
        number = jnp.where((x >= 0) & along_y, x * side * side + y * side, -1000)
    elif kind == "before_y":
        number = jnp.where((x >= 0) & (y < 0), x * side * side + last * side, -1000)
    else:
        number = jnp.where((x < 0) & along_y, last * side * side + y * side, -1000)
    return number.astype(jnp.float32)


def lanes_of(side, kind="in"):
    return side * 8 if kind == "out" else (side + 1) * 8


def one_hot(number, order):
    return jnp.where(number == order, 1.0, 0.0).astype(jnp.bfloat16)


def eye(size):
    rows = lax.broadcasted_iota(jnp.int32, (size, size), 0)
    return jnp.where(rows == lax.broadcasted_iota(jnp.int32, (size, size), 1), 1.0, 0.0).astype(
        jnp.bfloat16
    )


def layers_in(order, side):
    return order - side * jnp.floor((order + 0.5) * (1.0 / side))


def on_own_layer(rows, order, count, side):
    row = lax.broadcasted_iota(jnp.int32, (rows, order.shape[1]), 0)
    return (row // count).astype(jnp.float32) == layers_in(order, side)


def picked(cells, count, side, number, order):
    layers = cells[count : (side + 1) * count]
    lanes = one_hot(number, order - layers_in(order, side))
    values = times_weights(layers, lanes)
    values = jnp.where(on_own_layer(side * count, order, count, side), values, 0.0)
    total = values[0:count]
    for z in range(1, side):
        total = total + values[z * count : (z + 1) * count]
    return total


def placed(values, count, side, number, order):
    values = jnp.concatenate([values] * side, axis=0)
    values = jnp.where(on_own_layer(side * count, order, count, side), values, 0.0)
    return times_weights_back(values, one_hot(number, order - layers_in(order, side)))


LEAF, TO_FIRST, TO_SECOND, TO_TOP = 0, 128, 184, 248
FIRST_SECOND, FIRST_TOP, SECOND_TOP, ORDER, PACKED = 320, 352, 384, 416, 424


def split_order(order, sizes):
    out, start = [], 0
    for size in sizes:
        out.append(order[:, start : start + size])
        start += size
    return out


def packed_order(pack, sizes):
    leaf_size = sizes[0]
    leaf_order = pack[ORDER : ORDER + 1, 0:leaf_size]
    rest = pack[ORDER + 1 : ORDER + 2, 0 : sum(sizes[1:])]
    return [leaf_order] + split_order(rest, sizes[1:])


def prepare_body(sizes, side, *refs):
    order, leaf, to_first, first, second = refs[:5]
    to_second, to_top, first_second, first_top, second_top = refs[5:10]
    up, down, beside, pack = refs[10:]
    up[...] = jnp.zeros_like(up)
    down[...] = jnp.zeros_like(down)
    beside[sizes[2] :, :] = jnp.zeros_like(beside[sizes[2] :, :])
    order = order[...].astype(jnp.float32)
    leaf_size, first_size, second_size = sizes[:3]
    leaf_rows, first_columns = leaf[:, 0, :], to_first[:, 0, :]
    first_rows = first[:, 0, :]
    face = one_hot(numbers(side, "in"), order[:, :leaf_size])
    rows = weights_times(face, leaf_rows)
    up[0:first_size, 0 : first_rows.shape[1]] = first_rows
    up[first_size : first_size + 1, 0 : order.shape[1]] = order
    total = first_rows.shape[1]
    down[:, total : total + 2 * first_size] = product_back(rows, first_columns)
    down[0:first_size, 0:total] = first_rows
    beside[0:second_size, :] = second[:, 0, :]
    beside[second_size : second_size + 1, 0 : order.shape[1]] = order
    pack[ORDER : ORDER + 1, 0:leaf_size] = order[:, :leaf_size]
    pack[ORDER + 1 : ORDER + 2, 0 : order.shape[1] - leaf_size] = order[:, leaf_size:]
    for start, rows in (
        (LEAF, leaf_rows),
        (TO_FIRST, first_columns),
        (TO_SECOND, to_second[:, 0, :]),
        (TO_TOP, to_top[...]),
        (FIRST_SECOND, first_second[:, 0, :]),
        (FIRST_TOP, first_top[:, 0, :]),
        (SECOND_TOP, second_top[:, 0, :]),
    ):
        pack[start : start + rows.shape[0], 0 : rows.shape[1]] = rows


def prepared(sizes, side, width, *sources):
    leaf_size, first_size, second_size, top_size = sizes
    assert leaf_size <= 128 and first_size < 32 and second_size < 32 and top_size <= 36
    shapes = (
        (32, width),
        (lanes_of(side), width),
        (40, sources[4].shape[2]),
        (PACKED, 128),
    )
    return pl.pallas_call(
        functools.partial(prepare_body, sizes, side),
        out_shape=tuple(jax.ShapeDtypeStruct(o, jnp.float32) for o in shapes),
        in_specs=[VMEM] * len(sources),
        out_specs=(VMEM,) * len(shapes),
        compiler_params=LIMIT,
        name="prepare",
    )(*sources)


LAYER = 32


def message_body(inner, from_x, _, message):
    along, lanes = inner.shape[1:]
    rows = inner[:, along - 1, :]
    row = lax.broadcasted_iota(jnp.int32, rows.shape, 0)
    rows = rows + jnp.where(row == 1, from_x[along - 1 : along, 0:lanes], 0.0)
    message[LAYER : LAYER + rows.shape[0], 0:lanes] = rows


def with_layer(inner, from_x, beside):
    return pl.pallas_call(
        message_body,
        out_shape=jax.ShapeDtypeStruct(beside.shape, jnp.float32),
        in_specs=[VMEM] * 3,
        out_specs=VMEM,
        input_output_aliases={2: 0},
        compiler_params=LIMIT,
        name="y_message",
    )(inner, from_x, beside)


def first_body(
    sizes, side, total, inner, from_x, from_y, pack, first, below, above, cells_out, pieces
):
    count = pieces.shape[1] // 4
    peers = pieces.shape[0]
    first_size = sizes[1]
    leaf_size = sizes[0]
    leaf_order, first_order = packed_order(pack, sizes)[:2]
    values = inner[...]
    across, along, lanes = values.shape
    reach = across * along
    row = lax.broadcasted_iota(jnp.int32, values.shape, 0)
    values = values + jnp.where(row == 1, from_x[0:along, 0:lanes][None], 0.0)
    row = lax.broadcasted_iota(jnp.int32, values.shape, 1)
    layer = from_y[LAYER : LAYER + across, 0:lanes]
    values = values + jnp.where(row == 1, layer[:, None, :], 0.0)
    cells = weights_times_back(eye(lanes), values.reshape(reach, lanes))
    cells_out[...] = cells
    number = numbers(side, "in")
    leaf_rhs = picked(cells, count, side, number, leaf_order)
    first_rhs = picked(cells, count, side, number, first_order)
    after = cells[(side + 1) * count : (side + 2) * count]
    before = cells[0:count]
    leaf = pack[LEAF : LEAF + leaf_size, 0:leaf_size]
    to_first = pack[TO_FIRST : TO_FIRST + 2 * first_size, 0:leaf_size]
    toward = product_back(product(leaf_rhs, leaf), to_first)
    whole = total
    own_rows = first[0:first_size, 0:whole]
    below_rows = below[0:first_size, 0:whole]
    below_order = below[first_size : first_size + 1, 0 : sum(sizes)]
    below_order = split_order(below_order, sizes)[1]
    from_before = times_weights(before, one_hot(number + float(side - 1), below_order))
    through = product(after, above[:, whole : whole + 2 * first_size])
    above_rows = above[0:first_size, 0:whole]
    terms = product(first_rhs - toward[:, :first_size] - through[:, first_size:], own_rows)
    terms = terms + product(from_before - toward[:, first_size:], below_rows)
    terms = terms - product(through[:, :first_size], above_rows)
    pieces[...] = jnp.zeros_like(pieces)
    place = lax.axis_index("gz")
    for p in range(peers):
        pieces[p, 0:count, 0:first_size] = terms[:, p * first_size : (p + 1) * first_size]
        pieces[p, count : 2 * count, 0:reach] = jnp.where(place + 1 == p, after, 0.0)
        pieces[p, 2 * count : 3 * count, 0:reach] = jnp.where(place - 1 == p, before, 0.0)


def second_body(
    sizes, side, gz, received, cells, from_x, pack, second, below, pieces, leaf_out, first_out,
    toward_out, top_out,
):
    peers, rows = pieces.shape[:2]
    count = rows // 2
    leaf_size, first_size, second_size, top_size = sizes
    reach = cells.shape[1]
    total = received[0]
    for p in range(1, received.shape[0]):
        total = total + received[p]
    first_own = total[0:count, 0:first_size]
    cells = cells[...]
    after = total[count : 2 * count, 0:reach]
    before = total[2 * count : 3 * count, 0:reach]
    cells = jnp.concatenate(
        [
            cells[0:count],
            cells[count : 2 * count] + after,
            cells[2 * count : side * count],
            cells[side * count : (side + 1) * count] + before,
            cells[(side + 1) * count :],
        ],
        axis=0,
    )
    leaf_order, _, second_order, top_order = packed_order(pack, sizes)
    number = numbers(side, "in")
    leaf = pack[LEAF : LEAF + leaf_size, 0:leaf_size]
    to_second = pack[TO_SECOND : TO_SECOND + 2 * second_size, 0:leaf_size]
    to_top = pack[TO_TOP : TO_TOP + 2 * top_size, 0:leaf_size]
    first_second = pack[FIRST_SECOND : FIRST_SECOND + first_size, 0 : 2 * second_size]
    first_top = pack[FIRST_TOP : FIRST_TOP + first_size, 0 : 2 * top_size]
    leaf_solved = product(picked(cells, count, side, number, leaf_order), leaf)
    second_rhs = picked(cells, count, side, number, second_order)
    top_out[...] = picked(cells, count, side, number, top_order)
    below_order = below[second_size : second_size + 1, 0 : sum(sizes)]
    _, _, below_second, below_top = split_order(below_order, sizes)
    number = numbers(side, "before_y")
    from_before = picked(cells, count, side, number, below_second)
    top_before = picked(cells, count, side, number, below_top)
    toward = product_back(leaf_solved, to_second) + product(first_own, first_second)
    terms = product(second_rhs - toward[:, :second_size], second[0:second_size, :])
    terms = terms + product(from_before - toward[:, second_size:], below[0:second_size, :])
    pieces[...] = jnp.zeros_like(pieces)
    place = (lax.axis_index("gy") - 1) * gz + lax.axis_index("gz")
    for p in range(peers):
        pieces[p, 0:count, 0:second_size] = terms[:, p * second_size : (p + 1) * second_size]
        pieces[p, count : 2 * count, 0:top_size] = jnp.where(place == p, top_before, 0.0)
    leaf_out[...] = leaf_solved
    first_out[...] = first_own
    toward = product_back(leaf_solved, to_top) + product(first_own, first_top)
    order_x = from_x[8:9, 0:top_size]
    before_x = picked(cells, count, side, numbers(side, "before_x"), order_x)
    toward_out[:, :top_size] = toward[:, :top_size]
    toward_out[:, top_size:] = toward[:, top_size:] - before_x


def fold_body(top, out):
    rows, columns = top.shape
    full = rows // 8
    for g in range(full):
        out[:, g * columns : (g + 1) * columns] = top[8 * g : 8 * g + 8, :]
    half = columns // 2
    start = full * columns
    out[0:4, start : start + half] = top[8 * full : rows, 0:half]
    out[4:8, start : start + half] = top[8 * full : rows, half:columns]


def folded(top):
    rows, columns = top.shape
    assert rows % 8 == 4
    return pl.pallas_call(
        fold_body,
        out_shape=jax.ShapeDtypeStruct((8, columns * rows // 8), jnp.float32),
        in_specs=[VMEM],
        out_specs=VMEM,
        compiler_params=LIMIT,
        name="fold",
    )(top)


def unfolded(folds, rows, columns, start, width):
    full = rows // 8
    parts = []
    for g in range(full):
        at = g * columns + start
        parts.append(folds[:, at : at + width])
    half = start // (columns // 2)
    at = full * columns + start - half * (columns // 2)
    parts.append(folds[4 * half : 4 * half + 4, at : at + width])
    return jnp.concatenate(parts, axis=0)


def top_body(used, received, toward, rhs, pack, top, below, pieces, second_out):
    count = toward.shape[0]
    second_size = second_out.shape[1]
    top_size = rhs.shape[1]
    total = received[0]
    for p in range(1, received.shape[0]):
        total = total + received[p]
    second_own = total[0:count, 0:second_size]
    second_out[...] = second_own
    second_top = pack[SECOND_TOP : SECOND_TOP + second_size, 0 : 2 * top_size]
    toward = toward[...] + product(second_own, second_top)
    own = rhs[...] + total[count : 2 * count, 0:top_size] - toward[:, :top_size]
    other = toward[:, top_size:]
    width = pieces.shape[2]
    vectors = []
    for vector in (own, -other):
        high, low = parts_of(vector)
        both = jnp.concatenate([high.astype(jnp.float32), low.astype(jnp.float32)], axis=0)
        vectors.append((both.astype(jnp.bfloat16), high))
    for p in range(used):
        at = slice(p * width, (p + 1) * width)
        total = None
        lower = unfolded(below, *top.shape, p * width, width)
        for (both, high), rows in zip(vectors, (top[:, at], lower)):
            first, second = parts_of(rows)
            term = dot(both, first)
            term = term[:count] + (term[count:] + dot(high, second))
            total = term if total is None else total + term
        pieces[p] = total
    for p in range(used, pieces.shape[0]):
        pieces[p] = jnp.zeros(pieces.shape[1:], jnp.float32)


def spread_sum_body(received, out):
    total = received[0]
    for p in range(1, received.shape[0]):
        total = total + received[p]
    for p in range(out.shape[0]):
        out[p] = total


def top_back_body(
    used, whole, top, below, second_own, first_own, leaf_solved, pack, pair_out, second_gap,
    first_gap, leaf_gap,
):
    count = whole.shape[1]
    width = whole.shape[2]
    top_size = top.shape[0]

    halves = []
    for fold in (False, True):
        total = None
        for p in range(used):
            at = slice(p * width, (p + 1) * width)
            high, low = parts_of(whole[p])
            both = jnp.concatenate([high.astype(jnp.float32), low.astype(jnp.float32)], axis=0)
            rows = unfolded(below, *top.shape, p * width, width) if fold else top[:, at]
            first, second = parts_of(rows)
            term = dot_back(both.astype(jnp.bfloat16), first)
            term = term[:count] + (term[count:] + dot_back(high, second))
            total = term if total is None else total + term
        halves.append(total)
    own, lower = halves
    pair_out[...] = own

    def against(matrix):
        return product_back(own, matrix[:, :top_size]) + product_back(lower, matrix[:, top_size:])

    second_rows, first_rows = second_own.shape[1], first_own.shape[1]
    second_gap[...] = second_own[...] - against(
        pack[SECOND_TOP : SECOND_TOP + second_rows, 0 : 2 * top_size]
    )
    first_gap[...] = first_own[...] - against(
        pack[FIRST_TOP : FIRST_TOP + first_rows, 0 : 2 * top_size]
    )
    rows = pack[TO_TOP : TO_TOP + 2 * top_size, 0 : leaf_solved.shape[1]]
    leaf_gap[...] = leaf_solved[...] - (
        product(own, rows[:top_size]) + product(lower, rows[top_size:])
    )


def second_back_body(
    sizes, side, whole, second, below, first_gap, leaf_gap, top_back, pack, sent, base_out,
    second_out,
):
    count = whole.shape[0]
    leaf_size, first_size, second_size, _ = sizes
    reach = side * 8
    own = product_back(whole[...], second[0:second_size, :])
    lower = product_back(whole[...], below[0:second_size, :])
    second_out[...] = own
    weights = pack[FIRST_SECOND : FIRST_SECOND + first_size, 0 : 2 * second_size]
    gap = first_gap[...] - product_back(own, weights[:, :second_size])
    gap = gap - product_back(lower, weights[:, second_size:])
    rows = pack[TO_SECOND : TO_SECOND + 2 * second_size, 0:leaf_size]
    rest = leaf_gap[...] - product(own, rows[:second_size]) - product(lower, rows[second_size:])
    base = product_back(rest, pack[LEAF : LEAF + leaf_size, 0:leaf_size])
    base_out[...] = base
    leaf_order, _, second_order, top_order = packed_order(pack, sizes)
    number = numbers(side, "out")
    face = times_weights_back(base, one_hot(number, leaf_order))
    face = face + times_weights_back(own, one_hot(number, second_order))
    face = face + times_weights_back(top_back[...], one_hot(number, top_order))
    sent[...] = jnp.zeros_like(sent)
    sent[0:count, 0:first_size] = gap
    sent[count : 2 * count, 0:reach] = face


def leaf_back_body(
    sizes, side, received, base, second_back, top_back, pack, first, below, above, window,
):
    count = base.shape[0]
    peers = received.shape[0]
    leaf_size, first_size, _, _ = sizes
    reach = side * 8
    whole = jnp.concatenate([received[p, 0:count, 0:first_size] for p in range(peers)], axis=1)
    total = whole.shape[1]
    own = product_back(whole, first[0:first_size, 0:total])
    lower = product_back(whole, below[0:first_size, 0:total])
    following = product_back(whole, above[0:first_size, 0:total])
    rows = pack[TO_FIRST : TO_FIRST + 2 * first_size, 0:leaf_size]
    rest = product(own, rows[:first_size]) + product(lower, rows[first_size:])
    leaf_back = base[...] - product_back(rest, pack[LEAF : LEAF + leaf_size, 0:leaf_size])
    face = jnp.zeros((count, reach), jnp.float32)
    place = lax.axis_index("gz") + 1
    for p in range(peers):
        face = face + jnp.where(place == p, received[p, count : 2 * count, 0:reach], 0.0)
    through = above[:, total : total + 2 * first_size]
    moved = product_back(following, through[:, :first_size])
    moved = moved + product_back(own, through[:, first_size:])
    lane = lax.broadcasted_iota(jnp.int32, (through.shape[0], reach), 0)
    other = lax.broadcasted_iota(jnp.int32, (through.shape[0], reach), 1)
    shift = jnp.where(lane == other + 9, 1.0, 0.0)
    face = face - times_weights(moved, shift.astype(jnp.bfloat16))
    orders = packed_order(pack, sizes)
    number = numbers(side, "out")
    layers = placed(leaf_back, count, side, number, orders[0])
    layers = layers + placed(own, count, side, number, orders[1])
    layers = layers + placed(second_back[...], count, side, number, orders[2])
    layers = layers + placed(top_back[...], count, side, number, orders[3])
    cells = jnp.concatenate([layers, face, jnp.zeros_like(face)], axis=0)
    turned = weights_times_back(eye(reach), cells)
    window[...] = turned.reshape(window.shape)


def tent(at, cell):
    distance = jnp.abs(at - 4 * cell).astype(jnp.float32)
    return jnp.maximum(1.0 - 0.25 * distance, 0.0)


def prolong_body(inner, after_x, after_y, target, out, sent):
    count, fine = out.shape[:2]
    copies = []
    cells = inner.shape[0] + 1
    window = jnp.concatenate([inner[...], after_x[...][None]], axis=0)
    row = lax.broadcasted_iota(jnp.int32, window.shape, 1)
    window = jnp.where(row == cells - 1, after_y[...][:, None, :], window)
    flat = window.reshape(cells * window.shape[1], window.shape[2])
    rows = lax.broadcasted_iota(jnp.int32, (cells * fine, cells * 8), 0)
    columns = lax.broadcasted_iota(jnp.int32, (cells * fine, cells * 8), 1)
    at = rows - (columns >> 3) * fine
    inside = (at >= 0) & (at < fine) & ((columns & 7) < cells)
    y_weights = jnp.where(inside, tent(at, columns & 7), 0.0).astype(jnp.bfloat16)
    along_y = weights_times(y_weights, flat)
    lane = lax.broadcasted_iota(jnp.int32, (window.shape[2], fine), 0)
    at = lax.broadcasted_iota(jnp.int32, (window.shape[2], fine), 1)
    for r in range(count):
        inside = ((lane & 3) == r) & ((lane >> 2) < cells)
        z_weights = jnp.where(inside, tent(at, lane >> 2), 0.0).astype(jnp.bfloat16)
        along_z = times_weights(along_y, z_weights)
        planes = [along_z[i * fine : (i + 1) * fine] for i in range(cells)]
        for i in range(cells - 1):
            for q in range(4):
                value = planes[i]
                if q:
                    value = (1.0 - q / 4.0) * value + (q / 4.0) * planes[i + 1]
                out[r, 4 * i + q] = value
        copies.append(pltpu.make_async_copy(out.at[r], target.at[r], sent.at[r]))
        copies[r].start()
    for copy in copies:
        copy.wait()


def prolonged(inner, after_x, after_y, count, fine):
    return pl.pallas_call(
        prolong_body,
        out_shape=jax.ShapeDtypeStruct((count, fine, fine, fine), jnp.float32),
        in_specs=[VMEM] * 3,
        out_specs=HBM,
        scratch_shapes=[
            pltpu.VMEM((count, fine, fine, fine), jnp.float32),
            pltpu.SemaphoreType.DMA((count,)),
        ],
        compiler_params=LIMIT,
        name="prolong_twice",
    )(inner, after_x, after_y)


def call(body, outs, *operands):
    shapes = tuple(jax.ShapeDtypeStruct(o, jnp.float32) for o in outs)
    return pl.pallas_call(
        body,
        out_shape=shapes,
        in_specs=[VMEM] * len(operands),
        out_specs=(VMEM,) * len(shapes),
        compiler_params=LIMIT,
    )(*operands)


def per_device(
    right_side,
    iterate,
    coefficient,
    ordering,
    leaf_inverse,
    leaf_first,
    leaf_second,
    leaf_top,
    first_inverse,
    first_second,
    first_top,
    second_inverse,
    second_top,
    top_inverse,
):
    count, fine = right_side.shape[:2]
    leaf_size = leaf_inverse.shape[-1]
    first_size = first_second.shape[3]
    second_size = second_top.shape[3]
    top_size, top_total = top_inverse.shape
    sizes = (leaf_size, first_size, second_size, top_size)
    side = fine // 4
    cells = side**3
    lanes = (side + 2) * count
    gz = lax.axis_size("gz")
    plane_peers = lax.axis_size(PLANE)

    def rows_of(block):
        return jnp.transpose(block, (0, 1, 3, 2, 4)).reshape(block.shape[3], 1, block.shape[4])

    def columns_of(block):
        return jnp.transpose(block, (0, 1, 4, 2, 3)).reshape(block.shape[4], 1, block.shape[3])

    leaf = rows_of(leaf_inverse)
    to_first = columns_of(leaf_first)
    to_second = columns_of(leaf_second)
    to_top = jnp.swapaxes(leaf_top[0, 0, 0], 0, 1)
    first_to_second = rows_of(first_second)
    first_to_top = rows_of(first_top)
    second_to_top = rows_of(second_top)
    first = jnp.transpose(first_inverse, (0, 2, 1, 3)).reshape(first_size, 1, -1)
    second = jnp.transpose(second_inverse, (1, 0, 2))
    order = ordering.reshape(1, cells)

    inner, upper = restricted(order, right_side, iterate, coefficient)
    from_x = shifted(upper, "gx", 1)
    whole_first = -(-max(first.shape[2] + 2 * first_size, cells) // 128) * 128
    up, down, beside, pack = prepared(
        sizes,
        side,
        whole_first,
        order,
        leaf,
        to_first,
        first,
        second,
        to_second,
        to_top,
        first_to_second,
        first_to_top,
        second_to_top,
    )
    first_below = shifted(up, "gz", 1)
    first_above = shifted(down, "gz", -1)
    folds = folded(top_inverse)
    top_below = shifted(folds, "gx", 1)
    beside = with_layer(inner, from_x, beside)
    second_below = shifted(beside, "gy", 1)

    turned, pieces = call(
        functools.partial(first_body, sizes, side, first.shape[2]),
        [(lanes, lanes_of(side)), (gz, 4 * count, 128)],
        inner,
        from_x,
        second_below,
        pack,
        up,
        first_below,
        first_above,
    )
    received = exchanged(pieces, "gz")
    pieces, leaf_solved, first_own, toward, top_rhs = call(
        functools.partial(second_body, sizes, side, gz),
        [
            (plane_peers, 2 * count, 128),
            (count, leaf_size),
            (count, first_size),
            (count, 2 * top_size),
            (count, top_size),
        ],
        received,
        turned,
        from_x,
        pack,
        beside,
        second_below,
    )
    received = exchanged(pieces, PLANE)
    width = 128 * -(-top_total // (128 * plane_peers))
    used = top_total // width
    pieces, second_own = call(
        functools.partial(top_body, used),
        [(plane_peers, count, width), (count, second_size)],
        received,
        toward,
        top_rhs,
        pack,
        top_inverse,
        top_below,
    )
    received = exchanged(pieces, PLANE)
    (pieces,) = call(spread_sum_body, [(lax.axis_size("gx"), count, width)], received)
    received = exchanged(pieces, "gx")
    (pieces,) = call(spread_sum_body, [(plane_peers, count, width)], received)
    received = exchanged(pieces, PLANE)
    top_back, second_gap, first_gap, leaf_gap = call(
        functools.partial(top_back_body, used),
        [(count, top_size), (count, second_size), (count, first_size), (count, leaf_size)],
        received,
        top_inverse,
        top_below,
        second_own,
        first_own,
        leaf_solved,
        pack,
    )
    second_whole = jnp.moveaxis(sent_to_all(second_gap, PLANE), 0, 1).reshape(count, -1)
    sent, base, second_back = call(
        functools.partial(second_back_body, sizes, side),
        [(2 * count, 128), (count, leaf_size), (count, second_size)],
        second_whole,
        beside,
        second_below,
        first_gap,
        leaf_gap,
        top_back,
        pack,
    )
    received = sent_to_all(sent, "gz")
    (window,) = call(
        functools.partial(leaf_back_body, sizes, side),
        [(side, 8, lanes)],
        received,
        base,
        second_back,
        top_back,
        pack,
        up,
        first_below,
        first_above,
    )
    after_x = shifted(window[0], "gx", -1)
    layer = jnp.concatenate([window[:, 0], after_x[0:1]], axis=0)
    after_y = shifted(layer, "gy", -1)
    return prolonged(window, after_x, after_y, count, fine)


def solution(mesh):
    blocks = P("gx", "gy", "gz")
    return jax.shard_map(
        per_device,
        mesh=mesh,
        in_specs=(
            P(None, "gx", "gy", "gz"),
            P(None, "gx", "gy", "gz"),
            blocks,
            blocks,
            blocks,
            blocks,
            blocks,
            blocks,
            blocks,
            blocks,
            blocks,
            P("gx", PLANE, None),
            blocks,
            P(("gx", "gy", "gz"), None),
        ),
        out_specs=P(None, "gx", "gy", "gz"),
        check_vma=False,
    )
```

```python
import functools

import jax
import jax.numpy as jnp
from jax import lax
from jax.experimental import pallas as pl
from jax.experimental.pallas import tpu as pltpu
from jax.sharding import PartitionSpec as P

PLANE = ("gy", "gz")
AXES = ("gx", "gy", "gz")
VMEM = pl.BlockSpec(memory_space=pltpu.VMEM)
HBM = pl.BlockSpec(memory_space=pltpu.HBM)
LIMIT = pltpu.CompilerParams(vmem_limit_bytes=16 * 1024 * 1024)


def in_hbm(values):
    return pltpu.with_memory_space_constraint(values, pltpu.HBM)


def shifted(shard, axis, by):
    peers = lax.axis_size(axis)
    pairs = [(i, i + by) for i in range(peers) if 0 <= i + by < peers]
    return lax.ppermute(shard, axis, pairs)


def exchanged(pieces, axis):
    return lax.all_to_all(pieces, axis, split_axis=0, concat_axis=0, tiled=True)


def sent_to_all(shard, axis):
    copies = jnp.broadcast_to(shard, (lax.axis_size(axis), *shard.shape))
    return exchanged(copies, axis)


def parts_of(values):
    first = values.astype(jnp.bfloat16)
    second = (values - first.astype(jnp.float32)).astype(jnp.bfloat16)
    return first, second


def dot(left, right):
    return jnp.dot(left, right, preferred_element_type=jnp.float32)


def dot_back(left, right):
    return lax.dot_general(
        left, right, (((1,), (1,)), ((), ())), preferred_element_type=jnp.float32
    )


def product(operand, matrix):
    high, low = parts_of(operand)
    first, second = parts_of(matrix)
    return dot(high, first) + (dot(high, second) + dot(low, first))


def product_back(operand, matrix):
    high, low = parts_of(operand)
    first, second = parts_of(matrix)
    return dot_back(high, first) + (dot_back(high, second) + dot_back(low, first))


def times_weights(values, weights):
    first, second = parts_of(values)
    return dot(first, weights) + dot(second, weights)


def weights_times(weights, values):
    first, second = parts_of(values)
    return dot(weights, first) + dot(weights, second)


def times_weights_back(values, weights):
    first, second = parts_of(values)
    return dot_back(first, weights) + dot_back(second, weights)


def weights_times_back(weights, values):
    first, second = parts_of(values)
    return dot_back(weights, first) + dot_back(weights, second)


def weight_rows(coarse, fine, kind, missing):
    rows = lax.broadcasted_iota(jnp.int32, (coarse * coarse, coarse * fine), 0)
    columns = lax.broadcasted_iota(jnp.int32, (coarse * coarse, coarse * fine), 1)
    at = columns - (rows >> 3) * fine
    weights = weights_at(4 * ((rows & 7) - 1), at, kind, missing)
    return jnp.where((at >= 0) & (at < fine), weights, 0.0).astype(jnp.bfloat16)


def weight_lanes(coarse, fine, count, r, kind, missing):
    at = lax.broadcasted_iota(jnp.int32, (fine, coarse * count), 0)
    lane = lax.broadcasted_iota(jnp.int32, (fine, coarse * count), 1)
    weights = weights_at(4 * ((lane >> 2) - 1), at, kind, missing)
    return jnp.where((lane & 3) == r, weights, 0.0).astype(jnp.bfloat16)


def weights_at(cell, at, kind, missing):
    def weight(distance):
        return jnp.maximum(4.0 - jnp.abs(distance).astype(jnp.float32), 0.0) * 0.0625

    if kind == "own":
        return weight(cell - at)
    before = jnp.where(at == 0, missing, 0.0)
    return weight(cell - at - 1) + (1.0 - before) * weight(cell - at + 1)


def restricted_layers(layers):
    out = {}
    for x, layer in layers.items():
        if x % 2 == 0:
            shares = [(x // 2, 0.5)]
        else:
            shares = [((x - 1) // 2, 0.25), ((x + 1) // 2, 0.25)]
        for cell, weight in shares:
            term = weight * layer
            out[cell] = out[cell] + term if cell in out else term
    return out


def restrict_body(
    order_in, rhs_in, iterate_in, coefficient_in, inner, upper,
    rhs, iterate, coefficient, order, arrived,
):
    count, fine = rhs.shape[:2]
    coarse = inner.shape[1]
    half = fine // 2
    copies = [pltpu.make_async_copy(coefficient_in, coefficient, arrived.at[0])]
    for r in range(count):
        for source, room in ((iterate_in, iterate), (rhs_in, rhs)):
            for start in (0, half):
                part = pl.ds(start, half)
                copies.append(
                    pltpu.make_async_copy(
                        source.at[r, part], room.at[r, part], arrived.at[len(copies)]
                    )
                )
    copies.append(pltpu.make_async_copy(order_in, order, arrived.at[len(copies)]))
    for copy in copies:
        copy.start()
    at_x, at_y, at_z = [jnp.where(lax.axis_index(a) == 0, 1.0, 0.0) for a in AXES]
    layer, lanes = inner.shape[1:]
    top_size = coarse - 2
    top_size = top_size * top_size
    upper[...] = jnp.zeros_like(upper)
    y_cell = weight_rows(coarse, fine, "own", None)
    y_pair = weight_rows(coarse, fine, "beside", at_y)
    z_cells = [weight_lanes(coarse, fine, count, r, "own", None) for r in range(count)]
    z_pairs = [weight_lanes(coarse, fine, count, r, "beside", at_z) for r in range(count)]
    copies[0].wait()
    beside_sum = None
    own_sum = None
    for r in range(count):
        for copy in copies[4 * r + 1 : 4 * r + 5]:
            copy.wait()
        planes = [iterate[r, x] for x in range(fine)]
        gaps = [rhs[r, x] - (6.0 + coefficient[x]) * planes[x] for x in range(fine)]
        sums = {-1: (1.0 - at_x) * planes[0], fine: planes[-1]}
        for x in range(fine):
            total = gaps[x]
            for beside in (x - 1, x + 1):
                if 0 <= beside < fine:
                    total = total + planes[beside]
            sums[x] = total
        values = restricted_layers(restricted_layers(sums))
        cells = restricted_layers(restricted_layers(dict(enumerate(planes))))
        values = [values[i] for i in range(-1, coarse - 1)]
        cells = [jnp.zeros_like(planes[0])] + [cells[i] for i in range(coarse - 1)]
        value = jnp.concatenate(values, axis=0)
        cell = jnp.concatenate(cells, axis=0)
        term = times_weights(value, z_cells[r]) + times_weights(cell, z_pairs[r])
        beside_sum = term if beside_sum is None else beside_sum + term
        term = times_weights(cell, z_cells[r])
        own_sum = term if own_sum is None else own_sum + term
    result = weights_times(y_cell, beside_sum) + weights_times(y_pair, own_sum)
    result = result.reshape(coarse, coarse, coarse * count)
    inner[...] = result[:-1]
    upper[0:layer, 0:lanes] = result[coarse - 1]
    copies[-1].wait()
    orders = order[...].astype(jnp.float32)
    upper[layer : layer + 1, 0:top_size] = orders[:, orders.shape[1] - top_size :]


def restricted(order, right_side, iterate, coefficient):
    count, fine = right_side.shape[:2]
    coarse = fine // 4 + 2

    inner = jax.ShapeDtypeStruct((coarse - 1, coarse, coarse * count), jnp.float32)
    upper = jax.ShapeDtypeStruct((2 * coarse, 128), jnp.float32)
    return pl.pallas_call(
        restrict_body,
        out_shape=(inner, upper),
        in_specs=[HBM] * 4,
        out_specs=(VMEM,) * 2,
        scratch_shapes=[
            pltpu.VMEM(right_side.shape, jnp.float32),
            pltpu.VMEM(iterate.shape, jnp.float32),
            pltpu.VMEM(coefficient.shape, jnp.float32),
            pltpu.VMEM(order.shape, order.dtype),
            pltpu.SemaphoreType.DMA((4 * count + 2,)),
        ],
        compiler_params=LIMIT,
        name="restrict_twice",
    )(*map(in_hbm, (order, right_side, iterate, coefficient)))


def numbers(side, kind):
    lane = lax.broadcasted_iota(jnp.int32, (lanes_of(side, kind), 1), 0)
    x, y = lane >> 3, lane & 7
    if kind == "out":
        number = jnp.where(y < side, x * side * side + y * side, -1000)
        return number.astype(jnp.float32)
    x, y = x - 1, y - 1
    last = side - 1
    along_y = (y >= 0) & (y < side)
    if kind == "in":
        number = jnp.where((x >= 0) & along_y, x * side * side + y * side, -1000)
    elif kind == "before_y":
        number = jnp.where((x >= 0) & (y < 0), x * side * side + last * side, -1000)
    else:
        number = jnp.where((x < 0) & along_y, last * side * side + y * side, -1000)
    return number.astype(jnp.float32)


def lanes_of(side, kind="in"):
    return side * 8 if kind == "out" else (side + 1) * 8


def one_hot(number, order):
    return jnp.where(number == order, 1.0, 0.0).astype(jnp.bfloat16)


def eye(size):
    rows = lax.broadcasted_iota(jnp.int32, (size, size), 0)
    return jnp.where(rows == lax.broadcasted_iota(jnp.int32, (size, size), 1), 1.0, 0.0).astype(
        jnp.bfloat16
    )


def layers_in(order, side):
    return order - side * jnp.floor((order + 0.5) * (1.0 / side))


def on_own_layer(rows, order, count, side):
    row = lax.broadcasted_iota(jnp.int32, (rows, order.shape[1]), 0)
    return (row // count).astype(jnp.float32) == layers_in(order, side)


def picked(cells, count, side, number, order):
    layers = cells[count : (side + 1) * count]
    lanes = one_hot(number, order - layers_in(order, side))
    values = times_weights(layers, lanes)
    values = jnp.where(on_own_layer(side * count, order, count, side), values, 0.0)
    total = values[0:count]
    for z in range(1, side):
        total = total + values[z * count : (z + 1) * count]
    return total


def placed(values, count, side, number, order):
    values = jnp.concatenate([values] * side, axis=0)
    values = jnp.where(on_own_layer(side * count, order, count, side), values, 0.0)
    return times_weights_back(values, one_hot(number, order - layers_in(order, side)))


LEAF, TO_FIRST, TO_SECOND, TO_TOP = 0, 128, 184, 248
FIRST_SECOND, FIRST_TOP, SECOND_TOP, ORDER, PACKED = 320, 352, 384, 416, 424


def split_order(order, sizes):
    out, start = [], 0
    for size in sizes:
        out.append(order[:, start : start + size])
        start += size
    return out


def packed_order(pack, sizes):
    leaf_size = sizes[0]
    leaf_order = pack[ORDER : ORDER + 1, 0:leaf_size]
    rest = pack[ORDER + 1 : ORDER + 2, 0 : sum(sizes[1:])]
    return [leaf_order] + split_order(rest, sizes[1:])


def prepare_body(sizes, side, *refs):
    order, leaf, to_first, first, second = refs[:5]
    to_second, to_top, first_second, first_top, second_top = refs[5:10]
    up, down, beside, pack = refs[10:]
    up[...] = jnp.zeros_like(up)
    down[...] = jnp.zeros_like(down)
    beside[sizes[2] :, :] = jnp.zeros_like(beside[sizes[2] :, :])
    order = order[...].astype(jnp.float32)
    leaf_size, first_size, second_size = sizes[:3]
    leaf_rows, first_columns = leaf[:, 0, :], to_first[:, 0, :]
    first_rows = first[:, 0, :]
    face = one_hot(numbers(side, "in"), order[:, :leaf_size])
    rows = weights_times(face, leaf_rows)
    up[0:first_size, 0 : first_rows.shape[1]] = first_rows
    up[first_size : first_size + 1, 0 : order.shape[1]] = order
    total = first_rows.shape[1]
    down[:, total : total + 2 * first_size] = product_back(rows, first_columns)
    down[0:first_size, 0:total] = first_rows
    beside[0:second_size, :] = second[:, 0, :]
    beside[second_size : second_size + 1, 0 : order.shape[1]] = order
    pack[ORDER : ORDER + 1, 0:leaf_size] = order[:, :leaf_size]
    pack[ORDER + 1 : ORDER + 2, 0 : order.shape[1] - leaf_size] = order[:, leaf_size:]
    for start, rows in (
        (LEAF, leaf_rows),
        (TO_FIRST, first_columns),
        (TO_SECOND, to_second[:, 0, :]),
        (TO_TOP, to_top[...]),
        (FIRST_SECOND, first_second[:, 0, :]),
        (FIRST_TOP, first_top[:, 0, :]),
        (SECOND_TOP, second_top[:, 0, :]),
    ):
        pack[start : start + rows.shape[0], 0 : rows.shape[1]] = rows


def prepared(sizes, side, width, *sources):
    leaf_size, first_size, second_size, top_size = sizes
    assert leaf_size <= 128 and first_size < 32 and second_size < 32 and top_size <= 36
    shapes = (
        (32, width),
        (lanes_of(side), width),
        (40, sources[4].shape[2]),
        (PACKED, 128),
    )
    return pl.pallas_call(
        functools.partial(prepare_body, sizes, side),
        out_shape=tuple(jax.ShapeDtypeStruct(o, jnp.float32) for o in shapes),
        in_specs=[VMEM] * len(sources),
        out_specs=(VMEM,) * len(shapes),
        compiler_params=LIMIT,
        name="prepare",
    )(*sources)


AFTER, BEFORE, RIDING = 32, 128, 64

LAYER = 32


def message_body(inner, from_x, _, message):
    along, lanes = inner.shape[1:]
    rows = inner[:, along - 1, :]
    row = lax.broadcasted_iota(jnp.int32, rows.shape, 0)
    rows = rows + jnp.where(row == 1, from_x[along - 1 : along, 0:lanes], 0.0)
    message[LAYER : LAYER + rows.shape[0], 0:lanes] = rows


def with_layer(inner, from_x, beside):
    return pl.pallas_call(
        message_body,
        out_shape=jax.ShapeDtypeStruct(beside.shape, jnp.float32),
        in_specs=[VMEM] * 3,
        out_specs=VMEM,
        input_output_aliases={2: 0},
        compiler_params=LIMIT,
        name="y_message",
    )(inner, from_x, beside)


def own_body(sizes, side, total, inner, from_x, from_y, pack, first, cells_out, terms, other):
    leaf_size, first_size = sizes[:2]
    leaf_order, first_order = packed_order(pack, sizes)[:2]
    values = inner[...]
    across, along, lanes = values.shape
    reach = across * along
    count = terms.shape[0]
    row = lax.broadcasted_iota(jnp.int32, values.shape, 0)
    values = values + jnp.where(row == 1, from_x[0:along, 0:lanes][None], 0.0)
    row = lax.broadcasted_iota(jnp.int32, values.shape, 1)
    layer = from_y[LAYER : LAYER + across, 0:lanes]
    values = values + jnp.where(row == 1, layer[:, None, :], 0.0)
    cells = weights_times_back(eye(lanes), values.reshape(reach, lanes))
    cells_out[...] = cells
    number = numbers(side, "in")
    leaf_rhs = picked(cells, count, side, number, leaf_order)
    first_rhs = picked(cells, count, side, number, first_order)
    leaf = pack[LEAF : LEAF + leaf_size, 0:leaf_size]
    to_first = pack[TO_FIRST : TO_FIRST + 2 * first_size, 0:leaf_size]
    toward = product_back(product(leaf_rhs, leaf), to_first)
    terms[...] = product(first_rhs - toward[:, :first_size], first[0:first_size, 0:total])
    other[...] = toward[:, first_size:]


def first_body(sizes, side, total, cells, own_terms, other, first, below, above, pieces):
    peers, count = pieces.shape[:2]
    first_size = sizes[1]
    reach = cells.shape[1]
    after = cells[(side + 1) * count : (side + 2) * count, :]
    before = cells[0:count, :]
    below_order = below[first_size : first_size + 1, 0 : sum(sizes)]
    below_order = split_order(below_order, sizes)[1]
    number = numbers(side, "in") + float(side - 1)
    from_before = times_weights(before, one_hot(number, below_order))
    through = product(after, above[:, total : total + 2 * first_size])
    terms = own_terms[...] - product(through[:, first_size:], first[0:first_size, 0:total])
    terms = terms + product(from_before - other[...], below[0:first_size, 0:total])
    terms = terms - product(through[:, :first_size], above[0:first_size, 0:total])
    pieces[...] = jnp.zeros_like(pieces)
    place = lax.axis_index("gz")
    for p in range(peers):
        pieces[p, :, 0:first_size] = terms[:, p * first_size : (p + 1) * first_size]
        pieces[p, :, AFTER : AFTER + reach] = jnp.where(place + 1 == p, after, 0.0)
        pieces[p, :, BEFORE : BEFORE + reach] = jnp.where(place - 1 == p, before, 0.0)


def second_body(
    sizes, side, gz, received, cells, from_x, pack, second, below, pieces, leaf_out, first_out,
    toward_out, top_out,
):
    peers, count = pieces.shape[:2]
    leaf_size, first_size, second_size, top_size = sizes
    reach = cells.shape[1]
    total = received[0]
    for p in range(1, received.shape[0]):
        total = total + received[p]
    first_own = total[:, 0:first_size]
    cells = cells[...]
    after = total[:, AFTER : AFTER + reach]
    before = total[:, BEFORE : BEFORE + reach]
    cells = jnp.concatenate(
        [
            cells[0:count],
            cells[count : 2 * count] + after,
            cells[2 * count : side * count],
            cells[side * count : (side + 1) * count] + before,
            cells[(side + 1) * count :],
        ],
        axis=0,
    )
    leaf_order, _, second_order, top_order = packed_order(pack, sizes)
    number = numbers(side, "in")
    leaf = pack[LEAF : LEAF + leaf_size, 0:leaf_size]
    to_second = pack[TO_SECOND : TO_SECOND + 2 * second_size, 0:leaf_size]
    to_top = pack[TO_TOP : TO_TOP + 2 * top_size, 0:leaf_size]
    first_second = pack[FIRST_SECOND : FIRST_SECOND + first_size, 0 : 2 * second_size]
    first_top = pack[FIRST_TOP : FIRST_TOP + first_size, 0 : 2 * top_size]
    leaf_solved = product(picked(cells, count, side, number, leaf_order), leaf)
    second_rhs = picked(cells, count, side, number, second_order)
    top_out[...] = picked(cells, count, side, number, top_order)
    below_order = below[second_size : second_size + 1, 0 : sum(sizes)]
    _, _, below_second, below_top = split_order(below_order, sizes)
    number = numbers(side, "before_y")
    from_before = picked(cells, count, side, number, below_second)
    top_before = picked(cells, count, side, number, below_top)
    toward = product_back(leaf_solved, to_second) + product(first_own, first_second)
    terms = product(second_rhs - toward[:, :second_size], second[0:second_size, :])
    terms = terms + product(from_before - toward[:, second_size:], below[0:second_size, :])
    pieces[...] = jnp.zeros_like(pieces)
    place = (lax.axis_index("gy") - 1) * gz + lax.axis_index("gz")
    for p in range(peers):
        pieces[p, :, 0:second_size] = terms[:, p * second_size : (p + 1) * second_size]
        riding = jnp.where(place == p, top_before, 0.0)
        pieces[p, :, RIDING : RIDING + top_size] = riding
    leaf_out[...] = leaf_solved
    first_out[...] = first_own
    toward = product_back(leaf_solved, to_top) + product(first_own, first_top)
    order_x = from_x[8:9, 0:top_size]
    before_x = picked(cells, count, side, numbers(side, "before_x"), order_x)
    toward_out[:, :top_size] = toward[:, :top_size]
    toward_out[:, top_size:] = toward[:, top_size:] - before_x


def fold_body(top, out):
    rows, columns = top.shape
    full = rows // 8
    for g in range(full):
        out[:, g * columns : (g + 1) * columns] = top[8 * g : 8 * g + 8, :]
    half = columns // 2
    start = full * columns
    out[0:4, start : start + half] = top[8 * full : rows, 0:half]
    out[4:8, start : start + half] = top[8 * full : rows, half:columns]


def folded(top):
    rows, columns = top.shape
    assert rows % 8 == 4
    return pl.pallas_call(
        fold_body,
        out_shape=jax.ShapeDtypeStruct((8, columns * rows // 8), jnp.float32),
        in_specs=[VMEM],
        out_specs=VMEM,
        compiler_params=LIMIT,
        name="fold",
    )(top)


def unfolded(folds, rows, columns, start, width):
    full = rows // 8
    parts = []
    for g in range(full):
        at = g * columns + start
        parts.append(folds[:, at : at + width])
    half = start // (columns // 2)
    at = full * columns + start - half * (columns // 2)
    parts.append(folds[4 * half : 4 * half + 4, at : at + width])
    return jnp.concatenate(parts, axis=0)


def top_body(used, received, toward, rhs, pack, top, below, pieces, second_out):
    count = toward.shape[0]
    second_size = second_out.shape[1]
    top_size = rhs.shape[1]
    total = received[0]
    for p in range(1, received.shape[0]):
        total = total + received[p]
    second_own = total[:, 0:second_size]
    second_out[...] = second_own
    second_top = pack[SECOND_TOP : SECOND_TOP + second_size, 0 : 2 * top_size]
    toward = toward[...] + product(second_own, second_top)
    own = rhs[...] + total[:, RIDING : RIDING + top_size] - toward[:, :top_size]
    other = toward[:, top_size:]
    width = pieces.shape[2]
    vectors = []
    for vector in (own, -other):
        high, low = parts_of(vector)
        both = jnp.concatenate([high.astype(jnp.float32), low.astype(jnp.float32)], axis=0)
        vectors.append((both.astype(jnp.bfloat16), high))
    for p in range(used):
        at = slice(p * width, (p + 1) * width)
        total = None
        lower = unfolded(below, *top.shape, p * width, width)
        for (both, high), rows in zip(vectors, (top[:, at], lower)):
            first, second = parts_of(rows)
            term = dot(both, first)
            term = term[:count] + (term[count:] + dot(high, second))
            total = term if total is None else total + term
        pieces[p] = total
    for p in range(used, pieces.shape[0]):
        pieces[p] = jnp.zeros(pieces.shape[1:], jnp.float32)


def spread_sum_body(received, out):
    total = received[0]
    for p in range(1, received.shape[0]):
        total = total + received[p]
    for p in range(out.shape[0]):
        out[p] = total


def top_back_body(
    used, whole, top, below, second_own, first_own, leaf_solved, pack, pair_out, second_gap,
    first_gap, leaf_gap,
):
    count = whole.shape[1]
    width = whole.shape[2]
    top_size = top.shape[0]

    halves = []
    for fold in (False, True):
        total = None
        for p in range(used):
            at = slice(p * width, (p + 1) * width)
            high, low = parts_of(whole[p])
            both = jnp.concatenate([high.astype(jnp.float32), low.astype(jnp.float32)], axis=0)
            rows = unfolded(below, *top.shape, p * width, width) if fold else top[:, at]
            first, second = parts_of(rows)
            term = dot_back(both.astype(jnp.bfloat16), first)
            term = term[:count] + (term[count:] + dot_back(high, second))
            total = term if total is None else total + term
        halves.append(total)
    own, lower = halves
    pair_out[...] = own

    def against(matrix):
        return product_back(own, matrix[:, :top_size]) + product_back(lower, matrix[:, top_size:])

    second_rows, first_rows = second_own.shape[1], first_own.shape[1]
    second_gap[...] = second_own[...] - against(
        pack[SECOND_TOP : SECOND_TOP + second_rows, 0 : 2 * top_size]
    )
    first_gap[...] = first_own[...] - against(
        pack[FIRST_TOP : FIRST_TOP + first_rows, 0 : 2 * top_size]
    )
    rows = pack[TO_TOP : TO_TOP + 2 * top_size, 0 : leaf_solved.shape[1]]
    leaf_gap[...] = leaf_solved[...] - (
        product(own, rows[:top_size]) + product(lower, rows[top_size:])
    )


def second_back_body(
    sizes, side, whole, second, below, first_gap, leaf_gap, top_back, pack, sent, base_out,
    second_out,
):
    leaf_size, first_size, second_size, _ = sizes
    reach = side * 8
    own = product_back(whole[...], second[0:second_size, :])
    lower = product_back(whole[...], below[0:second_size, :])
    second_out[...] = own
    weights = pack[FIRST_SECOND : FIRST_SECOND + first_size, 0 : 2 * second_size]
    gap = first_gap[...] - product_back(own, weights[:, :second_size])
    gap = gap - product_back(lower, weights[:, second_size:])
    rows = pack[TO_SECOND : TO_SECOND + 2 * second_size, 0:leaf_size]
    rest = leaf_gap[...] - product(own, rows[:second_size]) - product(lower, rows[second_size:])
    base = product_back(rest, pack[LEAF : LEAF + leaf_size, 0:leaf_size])
    base_out[...] = base
    leaf_order, _, second_order, top_order = packed_order(pack, sizes)
    number = numbers(side, "out")
    face = times_weights_back(base, one_hot(number, leaf_order))
    face = face + times_weights_back(own, one_hot(number, second_order))
    face = face + times_weights_back(top_back[...], one_hot(number, top_order))
    sent[...] = jnp.zeros_like(sent)
    sent[:, 0:first_size] = gap
    sent[:, RIDING : RIDING + reach] = face


def leaf_back_body(
    sizes, side, received, base, second_back, top_back, pack, first, below, above, window,
):
    count = base.shape[0]
    peers = received.shape[0]
    leaf_size, first_size, _, _ = sizes
    reach = side * 8
    whole = jnp.concatenate([received[p, :, 0:first_size] for p in range(peers)], axis=1)
    total = whole.shape[1]
    own = product_back(whole, first[0:first_size, 0:total])
    lower = product_back(whole, below[0:first_size, 0:total])
    following = product_back(whole, above[0:first_size, 0:total])
    rows = pack[TO_FIRST : TO_FIRST + 2 * first_size, 0:leaf_size]
    rest = product(own, rows[:first_size]) + product(lower, rows[first_size:])
    leaf_back = base[...] - product_back(rest, pack[LEAF : LEAF + leaf_size, 0:leaf_size])
    face = jnp.zeros((count, reach), jnp.float32)
    place = lax.axis_index("gz") + 1
    for p in range(peers):
        riding = received[p, :, RIDING : RIDING + reach]
        face = face + jnp.where(place == p, riding, 0.0)
    through = above[:, total : total + 2 * first_size]
    moved = product_back(following, through[:, :first_size])
    moved = moved + product_back(own, through[:, first_size:])
    lane = lax.broadcasted_iota(jnp.int32, (through.shape[0], reach), 0)
    other = lax.broadcasted_iota(jnp.int32, (through.shape[0], reach), 1)
    shift = jnp.where(lane == other + 9, 1.0, 0.0)
    face = face - times_weights(moved, shift.astype(jnp.bfloat16))
    orders = packed_order(pack, sizes)
    number = numbers(side, "out")
    layers = placed(leaf_back, count, side, number, orders[0])
    layers = layers + placed(own, count, side, number, orders[1])
    layers = layers + placed(second_back[...], count, side, number, orders[2])
    layers = layers + placed(top_back[...], count, side, number, orders[3])
    cells = jnp.concatenate([layers, face, jnp.zeros_like(face)], axis=0)
    turned = weights_times_back(eye(reach), cells)
    window[...] = turned.reshape(window.shape)


def tent(at, cell):
    distance = jnp.abs(at - 4 * cell).astype(jnp.float32)
    return jnp.maximum(1.0 - 0.25 * distance, 0.0)


def prolong_body(inner, after_x, after_y, target, out, sent):
    count, fine = out.shape[:2]
    copies = []
    half = inner.shape[0] // 2
    cells = inner.shape[0] + 1
    window = jnp.concatenate([inner[...], after_x[...][None]], axis=0)
    row = lax.broadcasted_iota(jnp.int32, window.shape, 1)
    window = jnp.where(row == cells - 1, after_y[...][:, None, :], window)
    flat = window.reshape(cells * window.shape[1], window.shape[2])
    rows = lax.broadcasted_iota(jnp.int32, (cells * fine, cells * 8), 0)
    columns = lax.broadcasted_iota(jnp.int32, (cells * fine, cells * 8), 1)
    at = rows - (columns >> 3) * fine
    inside = (at >= 0) & (at < fine) & ((columns & 7) < cells)
    y_weights = jnp.where(inside, tent(at, columns & 7), 0.0).astype(jnp.bfloat16)
    along_y = weights_times(y_weights, flat)
    lane = lax.broadcasted_iota(jnp.int32, (window.shape[2], fine), 0)
    at = lax.broadcasted_iota(jnp.int32, (window.shape[2], fine), 1)
    for r in range(count):
        inside = ((lane & 3) == r) & ((lane >> 2) < cells)
        z_weights = jnp.where(inside, tent(at, lane >> 2), 0.0).astype(jnp.bfloat16)
        along_z = times_weights(along_y, z_weights)
        planes = [along_z[i * fine : (i + 1) * fine] for i in range(cells)]
        for i in range(cells - 1):
            for q in range(4):
                value = planes[i]
                if q:
                    value = (1.0 - q / 4.0) * value + (q / 4.0) * planes[i + 1]
                out[r, 4 * i + q] = value
            if (i + 1) % half == 0:
                part = pl.ds(4 * (i + 1 - half), 4 * half)
                copies.append(
                    pltpu.make_async_copy(
                        out.at[r, part], target.at[r, part], sent.at[len(copies)]
                    )
                )
                copies[-1].start()
    for copy in copies:
        copy.wait()


def prolonged(inner, after_x, after_y, count, fine):
    return pl.pallas_call(
        prolong_body,
        out_shape=jax.ShapeDtypeStruct((count, fine, fine, fine), jnp.float32),
        in_specs=[VMEM] * 3,
        out_specs=HBM,
        scratch_shapes=[
            pltpu.VMEM((count, fine, fine, fine), jnp.float32),
            pltpu.SemaphoreType.DMA((2 * count,)),
        ],
        compiler_params=LIMIT,
        name="prolong_twice",
    )(inner, after_x, after_y)


def call(body, outs, *operands):
    shapes = tuple(jax.ShapeDtypeStruct(o, jnp.float32) for o in outs)
    return pl.pallas_call(
        body,
        out_shape=shapes,
        in_specs=[VMEM] * len(operands),
        out_specs=(VMEM,) * len(shapes),
        compiler_params=LIMIT,
    )(*operands)


def per_device(
    right_side,
    iterate,
    coefficient,
    ordering,
    leaf_inverse,
    leaf_first,
    leaf_second,
    leaf_top,
    first_inverse,
    first_second,
    first_top,
    second_inverse,
    second_top,
    top_inverse,
):
    count, fine = right_side.shape[:2]
    leaf_size = leaf_inverse.shape[-1]
    first_size = first_second.shape[3]
    second_size = second_top.shape[3]
    top_size, top_total = top_inverse.shape
    sizes = (leaf_size, first_size, second_size, top_size)
    side = fine // 4
    cells = side**3
    lanes = (side + 2) * count
    gz = lax.axis_size("gz")
    plane_peers = lax.axis_size(PLANE)

    def rows_of(block):
        return jnp.transpose(block, (0, 1, 3, 2, 4)).reshape(block.shape[3], 1, block.shape[4])

    def columns_of(block):
        return jnp.transpose(block, (0, 1, 4, 2, 3)).reshape(block.shape[4], 1, block.shape[3])

    leaf = rows_of(leaf_inverse)
    to_first = columns_of(leaf_first)
    to_second = columns_of(leaf_second)
    to_top = jnp.swapaxes(leaf_top[0, 0, 0], 0, 1)
    first_to_second = rows_of(first_second)
    first_to_top = rows_of(first_top)
    second_to_top = rows_of(second_top)
    first = jnp.transpose(first_inverse, (0, 2, 1, 3)).reshape(first_size, 1, -1)
    second = jnp.transpose(second_inverse, (1, 0, 2))
    order = ordering.reshape(1, cells)

    inner, upper = restricted(order, right_side, iterate, coefficient)
    from_x = shifted(upper, "gx", 1)
    whole_first = -(-max(first.shape[2] + 2 * first_size, cells) // 128) * 128
    up, down, beside, pack = prepared(
        sizes,
        side,
        whole_first,
        order,
        leaf,
        to_first,
        first,
        second,
        to_second,
        to_top,
        first_to_second,
        first_to_top,
        second_to_top,
    )
    first_below = shifted(up, "gz", 1)
    first_above = shifted(down, "gz", -1)
    folds = folded(top_inverse)
    top_below = shifted(folds, "gx", 1)
    beside = with_layer(inner, from_x, beside)
    second_below = shifted(beside, "gy", 1)

    total = first.shape[2]
    turned, own_terms, other = call(
        functools.partial(own_body, sizes, side, total),
        [(lanes, lanes_of(side)), (count, total), (count, first_size)],
        inner,
        from_x,
        second_below,
        pack,
        up,
    )
    (pieces,) = call(
        functools.partial(first_body, sizes, side, total),
        [(gz, count, 256)],
        turned,
        own_terms,
        other,
        up,
        first_below,
        first_above,
    )
    received = exchanged(pieces, "gz")
    pieces, leaf_solved, first_own, toward, top_rhs = call(
        functools.partial(second_body, sizes, side, gz),
        [
            (plane_peers, count, 128),
            (count, leaf_size),
            (count, first_size),
            (count, 2 * top_size),
            (count, top_size),
        ],
        received,
        turned,
        from_x,
        pack,
        beside,
        second_below,
    )
    received = exchanged(pieces, PLANE)
    width = 128 * -(-top_total // (128 * plane_peers))
    used = top_total // width
    pieces, second_own = call(
        functools.partial(top_body, used),
        [(plane_peers, count, width), (count, second_size)],
        received,
        toward,
        top_rhs,
        pack,
        top_inverse,
        top_below,
    )
    received = exchanged(pieces, PLANE)
    (pieces,) = call(spread_sum_body, [(lax.axis_size("gx"), count, width)], received)
    received = exchanged(pieces, "gx")
    (pieces,) = call(spread_sum_body, [(plane_peers, count, width)], received)
    received = exchanged(pieces, PLANE)
    top_back, second_gap, first_gap, leaf_gap = call(
        functools.partial(top_back_body, used),
        [(count, top_size), (count, second_size), (count, first_size), (count, leaf_size)],
        received,
        top_inverse,
        top_below,
        second_own,
        first_own,
        leaf_solved,
        pack,
    )
    second_whole = jnp.moveaxis(sent_to_all(second_gap, PLANE), 0, 1).reshape(count, -1)
    sent, base, second_back = call(
        functools.partial(second_back_body, sizes, side),
        [(count, 128), (count, leaf_size), (count, second_size)],
        second_whole,
        beside,
        second_below,
        first_gap,
        leaf_gap,
        top_back,
        pack,
    )
    received = sent_to_all(sent, "gz")
    (window,) = call(
        functools.partial(leaf_back_body, sizes, side),
        [(side, 8, lanes)],
        received,
        base,
        second_back,
        top_back,
        pack,
        up,
        first_below,
        first_above,
    )
    after_x = shifted(window[0], "gx", -1)
    layer = jnp.concatenate([window[:, 0], after_x[0:1]], axis=0)
    after_y = shifted(layer, "gy", -1)
    return prolonged(window, after_x, after_y, count, fine)


def solution(mesh):
    blocks = P("gx", "gy", "gz")
    return jax.shard_map(
        per_device,
        mesh=mesh,
        in_specs=(
            P(None, "gx", "gy", "gz"),
            P(None, "gx", "gy", "gz"),
            blocks,
            blocks,
            blocks,
            blocks,
            blocks,
            blocks,
            blocks,
            blocks,
            blocks,
            P("gx", PLANE, None),
            blocks,
            P(("gx", "gy", "gz"), None),
        ),
        out_specs=P(None, "gx", "gy", "gz"),
        check_vma=False,
    )
```

```python
import functools

import jax
import jax.numpy as jnp
from jax import lax
from jax.experimental import pallas as pl
from jax.experimental.pallas import tpu as pltpu
from jax.sharding import PartitionSpec as P

PLANE = ("gy", "gz")
AXES = ("gx", "gy", "gz")
VMEM = pl.BlockSpec(memory_space=pltpu.VMEM)
HBM = pl.BlockSpec(memory_space=pltpu.HBM)
LIMIT = pltpu.CompilerParams(vmem_limit_bytes=16 * 1024 * 1024)


def in_hbm(values):
    return pltpu.with_memory_space_constraint(values, pltpu.HBM)


def shifted(shard, axis, by):
    peers = lax.axis_size(axis)
    pairs = [(i, i + by) for i in range(peers) if 0 <= i + by < peers]
    return lax.ppermute(shard, axis, pairs)


def exchanged(pieces, axis):
    return lax.all_to_all(pieces, axis, split_axis=0, concat_axis=0, tiled=True)


def sent_to_all(shard, axis):
    copies = jnp.broadcast_to(shard, (lax.axis_size(axis), *shard.shape))
    return exchanged(copies, axis)


def parts_of(values):
    first = values.astype(jnp.bfloat16)
    second = (values - first.astype(jnp.float32)).astype(jnp.bfloat16)
    return first, second


def dot(left, right):
    return jnp.dot(left, right, preferred_element_type=jnp.float32)


def dot_back(left, right):
    return lax.dot_general(
        left, right, (((1,), (1,)), ((), ())), preferred_element_type=jnp.float32
    )


def product(operand, matrix):
    high, low = parts_of(operand)
    first, second = parts_of(matrix)
    return dot(high, first) + (dot(high, second) + dot(low, first))


def product_back(operand, matrix):
    high, low = parts_of(operand)
    first, second = parts_of(matrix)
    return dot_back(high, first) + (dot_back(high, second) + dot_back(low, first))


def times_weights(values, weights):
    first, second = parts_of(values)
    return dot(first, weights) + dot(second, weights)


def weights_times(weights, values):
    first, second = parts_of(values)
    return dot(weights, first) + dot(weights, second)


def times_weights_back(values, weights):
    first, second = parts_of(values)
    return dot_back(first, weights) + dot_back(second, weights)


def weights_times_back(weights, values):
    first, second = parts_of(values)
    return dot_back(weights, first) + dot_back(weights, second)


def weight_rows(coarse, fine, kind, missing):
    rows = lax.broadcasted_iota(jnp.int32, (coarse * coarse, coarse * fine), 0)
    columns = lax.broadcasted_iota(jnp.int32, (coarse * coarse, coarse * fine), 1)
    at = columns - (rows >> 3) * fine
    weights = weights_at(4 * ((rows & 7) - 1), at, kind, missing)
    return jnp.where((at >= 0) & (at < fine), weights, 0.0).astype(jnp.bfloat16)


def weight_lanes(coarse, fine, count, r, kind, missing):
    at = lax.broadcasted_iota(jnp.int32, (fine, coarse * count), 0)
    lane = lax.broadcasted_iota(jnp.int32, (fine, coarse * count), 1)
    weights = weights_at(4 * ((lane >> 2) - 1), at, kind, missing)
    return jnp.where((lane & 3) == r, weights, 0.0).astype(jnp.bfloat16)


def weights_at(cell, at, kind, missing):
    def weight(distance):
        return jnp.maximum(4.0 - jnp.abs(distance).astype(jnp.float32), 0.0) * 0.0625

    if kind == "own":
        return weight(cell - at)
    before = jnp.where(at == 0, missing, 0.0)
    return weight(cell - at - 1) + (1.0 - before) * weight(cell - at + 1)


def restricted_layers(layers):
    out = {}
    for x, layer in layers.items():
        if x % 2 == 0:
            shares = [(x // 2, 0.5)]
        else:
            shares = [((x - 1) // 2, 0.25), ((x + 1) // 2, 0.25)]
        for cell, weight in shares:
            term = weight * layer
            out[cell] = out[cell] + term if cell in out else term
    return out


def restrict_body(
    order_in, rhs_in, iterate_in, coefficient_in, top_in, inner, upper, folds,
    rhs, iterate, coefficient, order, top, arrived,
):
    count, fine = rhs.shape[:2]
    coarse = inner.shape[1]
    half = fine // 2
    copies = [pltpu.make_async_copy(coefficient_in, coefficient, arrived.at[0])]
    for r in range(count):
        for source, room in ((iterate_in, iterate), (rhs_in, rhs)):
            for start in (0, half):
                part = pl.ds(start, half)
                copies.append(
                    pltpu.make_async_copy(
                        source.at[r, part], room.at[r, part], arrived.at[len(copies)]
                    )
                )
    copies.append(pltpu.make_async_copy(order_in, order, arrived.at[len(copies)]))
    copies.append(pltpu.make_async_copy(top_in, top, arrived.at[len(copies)]))
    for copy in copies:
        copy.start()
    at_x, at_y, at_z = [jnp.where(lax.axis_index(a) == 0, 1.0, 0.0) for a in AXES]
    layer, lanes = inner.shape[1:]
    top_size = coarse - 2
    top_size = top_size * top_size
    upper[...] = jnp.zeros_like(upper)
    y_cell = weight_rows(coarse, fine, "own", None)
    y_pair = weight_rows(coarse, fine, "beside", at_y)
    z_cells = [weight_lanes(coarse, fine, count, r, "own", None) for r in range(count)]
    z_pairs = [weight_lanes(coarse, fine, count, r, "beside", at_z) for r in range(count)]
    copies[0].wait()
    beside_sum = None
    own_sum = None
    for r in range(count):
        for copy in copies[4 * r + 1 : 4 * r + 5]:
            copy.wait()
        planes = [iterate[r, x] for x in range(fine)]
        gaps = [rhs[r, x] - (6.0 + coefficient[x]) * planes[x] for x in range(fine)]
        sums = {-1: (1.0 - at_x) * planes[0], fine: planes[-1]}
        for x in range(fine):
            total = gaps[x]
            for beside in (x - 1, x + 1):
                if 0 <= beside < fine:
                    total = total + planes[beside]
            sums[x] = total
        values = restricted_layers(restricted_layers(sums))
        cells = restricted_layers(restricted_layers(dict(enumerate(planes))))
        values = [values[i] for i in range(-1, coarse - 1)]
        cells = [jnp.zeros_like(planes[0])] + [cells[i] for i in range(coarse - 1)]
        value = jnp.concatenate(values, axis=0)
        cell = jnp.concatenate(cells, axis=0)
        term = times_weights(value, z_cells[r]) + times_weights(cell, z_pairs[r])
        beside_sum = term if beside_sum is None else beside_sum + term
        term = times_weights(cell, z_cells[r])
        own_sum = term if own_sum is None else own_sum + term
    result = weights_times(y_cell, beside_sum) + weights_times(y_pair, own_sum)
    result = result.reshape(coarse, coarse, coarse * count)
    inner[...] = result[:-1]
    upper[0:layer, 0:lanes] = result[coarse - 1]
    copies[-2].wait()
    copies[-1].wait()
    fold_body(top, folds)
    orders = order[...].astype(jnp.float32)
    upper[layer : layer + 1, 0:top_size] = orders[:, orders.shape[1] - top_size :]


def restricted(order, right_side, iterate, coefficient, top):
    count, fine = right_side.shape[:2]
    coarse = fine // 4 + 2

    inner = jax.ShapeDtypeStruct((coarse - 1, coarse, coarse * count), jnp.float32)
    upper = jax.ShapeDtypeStruct((2 * coarse, 128), jnp.float32)
    folds = jax.ShapeDtypeStruct((8, top.size // 8), jnp.float32)
    return pl.pallas_call(
        restrict_body,
        out_shape=(inner, upper, folds),
        in_specs=[HBM] * 5,
        out_specs=(VMEM,) * 3,
        scratch_shapes=[
            pltpu.VMEM(right_side.shape, jnp.float32),
            pltpu.VMEM(iterate.shape, jnp.float32),
            pltpu.VMEM(coefficient.shape, jnp.float32),
            pltpu.VMEM(order.shape, order.dtype),
            pltpu.VMEM(top.shape, jnp.float32),
            pltpu.SemaphoreType.DMA((4 * count + 3,)),
        ],
        compiler_params=LIMIT,
        name="restrict_twice",
    )(*map(in_hbm, (order, right_side, iterate, coefficient, top)))


def numbers(side, kind):
    lane = lax.broadcasted_iota(jnp.int32, (lanes_of(side, kind), 1), 0)
    x, y = lane >> 3, lane & 7
    if kind == "out":
        number = jnp.where(y < side, x * side * side + y * side, -1000)
        return number.astype(jnp.float32)
    x, y = x - 1, y - 1
    last = side - 1
    along_y = (y >= 0) & (y < side)
    if kind == "in":
        number = jnp.where((x >= 0) & along_y, x * side * side + y * side, -1000)
    elif kind == "before_y":
        number = jnp.where((x >= 0) & (y < 0), x * side * side + last * side, -1000)
    else:
        number = jnp.where((x < 0) & along_y, last * side * side + y * side, -1000)
    return number.astype(jnp.float32)


def lanes_of(side, kind="in"):
    return side * 8 if kind == "out" else (side + 1) * 8


def one_hot(number, order):
    return jnp.where(number == order, 1.0, 0.0).astype(jnp.bfloat16)


def eye(size):
    rows = lax.broadcasted_iota(jnp.int32, (size, size), 0)
    return jnp.where(rows == lax.broadcasted_iota(jnp.int32, (size, size), 1), 1.0, 0.0).astype(
        jnp.bfloat16
    )


def layers_in(order, side):
    return order - side * jnp.floor((order + 0.5) * (1.0 / side))


def on_own_layer(rows, order, count, side):
    row = lax.broadcasted_iota(jnp.int32, (rows, order.shape[1]), 0)
    return (row // count).astype(jnp.float32) == layers_in(order, side)


def picked(cells, count, side, number, order):
    layers = cells[count : (side + 1) * count]
    lanes = one_hot(number, order - layers_in(order, side))
    values = times_weights(layers, lanes)
    values = jnp.where(on_own_layer(side * count, order, count, side), values, 0.0)
    total = values[0:count]
    for z in range(1, side):
        total = total + values[z * count : (z + 1) * count]
    return total


def placed(values, count, side, number, order):
    values = jnp.concatenate([values] * side, axis=0)
    values = jnp.where(on_own_layer(side * count, order, count, side), values, 0.0)
    return times_weights_back(values, one_hot(number, order - layers_in(order, side)))


LEAF, TO_FIRST, TO_SECOND, TO_TOP = 0, 128, 184, 248
FIRST_SECOND, FIRST_TOP, SECOND_TOP, ORDER, PACKED = 320, 352, 384, 416, 424


def split_order(order, sizes):
    out, start = [], 0
    for size in sizes:
        out.append(order[:, start : start + size])
        start += size
    return out


def packed_order(pack, sizes):
    leaf_size = sizes[0]
    leaf_order = pack[ORDER : ORDER + 1, 0:leaf_size]
    rest = pack[ORDER + 1 : ORDER + 2, 0 : sum(sizes[1:])]
    return [leaf_order] + split_order(rest, sizes[1:])


def prepare_body(sizes, side, *refs):
    order, leaf, to_first, first, second = refs[:5]
    to_second, to_top, first_second, first_top, second_top = refs[5:10]
    up, down, beside, pack = refs[10:]
    up[...] = jnp.zeros_like(up)
    down[...] = jnp.zeros_like(down)
    beside[sizes[2] :, :] = jnp.zeros_like(beside[sizes[2] :, :])
    order = order[...].astype(jnp.float32)
    leaf_size, first_size, second_size = sizes[:3]
    leaf_rows, first_columns = leaf[:, 0, :], to_first[:, 0, :]
    first_rows = first[:, 0, :]
    face = one_hot(numbers(side, "in"), order[:, :leaf_size])
    rows = weights_times(face, leaf_rows)
    up[0:first_size, 0 : first_rows.shape[1]] = first_rows
    up[first_size : first_size + 1, 0 : order.shape[1]] = order
    total = first_rows.shape[1]
    down[:, total : total + 2 * first_size] = product_back(rows, first_columns)
    down[0:first_size, 0:total] = first_rows
    beside[0:second_size, :] = second[:, 0, :]
    beside[second_size : second_size + 1, 0 : order.shape[1]] = order
    pack[ORDER : ORDER + 1, 0:leaf_size] = order[:, :leaf_size]
    pack[ORDER + 1 : ORDER + 2, 0 : order.shape[1] - leaf_size] = order[:, leaf_size:]
    for start, rows in (
        (LEAF, leaf_rows),
        (TO_FIRST, first_columns),
        (TO_SECOND, to_second[:, 0, :]),
        (TO_TOP, to_top[...]),
        (FIRST_SECOND, first_second[:, 0, :]),
        (FIRST_TOP, first_top[:, 0, :]),
        (SECOND_TOP, second_top[:, 0, :]),
    ):
        pack[start : start + rows.shape[0], 0 : rows.shape[1]] = rows


def prepared(sizes, side, width, *sources):
    leaf_size, first_size, second_size, top_size = sizes
    assert leaf_size <= 128 and first_size < 32 and second_size < 32 and top_size <= 36
    shapes = (
        (32, width),
        (lanes_of(side), width),
        (40, sources[4].shape[2]),
        (PACKED, 128),
    )
    return pl.pallas_call(
        functools.partial(prepare_body, sizes, side),
        out_shape=tuple(jax.ShapeDtypeStruct(o, jnp.float32) for o in shapes),
        in_specs=[VMEM] * len(sources),
        out_specs=(VMEM,) * len(shapes),
        compiler_params=LIMIT,
        name="prepare",
    )(*sources)


AFTER, BEFORE, RIDING = 32, 128, 64

LAYER = 32


def message_body(inner, from_x, _, message):
    along, lanes = inner.shape[1:]
    rows = inner[:, along - 1, :]
    row = lax.broadcasted_iota(jnp.int32, rows.shape, 0)
    rows = rows + jnp.where(row == 1, from_x[along - 1 : along, 0:lanes], 0.0)
    message[LAYER : LAYER + rows.shape[0], 0:lanes] = rows


def with_layer(inner, from_x, beside):
    return pl.pallas_call(
        message_body,
        out_shape=jax.ShapeDtypeStruct(beside.shape, jnp.float32),
        in_specs=[VMEM] * 3,
        out_specs=VMEM,
        input_output_aliases={2: 0},
        compiler_params=LIMIT,
        name="y_message",
    )(inner, from_x, beside)


def own_body(sizes, side, total, inner, from_x, from_y, pack, first, cells_out, terms, other):
    leaf_size, first_size = sizes[:2]
    leaf_order, first_order = packed_order(pack, sizes)[:2]
    values = inner[...]
    across, along, lanes = values.shape
    reach = across * along
    count = terms.shape[0]
    row = lax.broadcasted_iota(jnp.int32, values.shape, 0)
    values = values + jnp.where(row == 1, from_x[0:along, 0:lanes][None], 0.0)
    row = lax.broadcasted_iota(jnp.int32, values.shape, 1)
    layer = from_y[LAYER : LAYER + across, 0:lanes]
    values = values + jnp.where(row == 1, layer[:, None, :], 0.0)
    cells = weights_times_back(eye(lanes), values.reshape(reach, lanes))
    cells_out[...] = cells
    number = numbers(side, "in")
    leaf_rhs = picked(cells, count, side, number, leaf_order)
    first_rhs = picked(cells, count, side, number, first_order)
    leaf = pack[LEAF : LEAF + leaf_size, 0:leaf_size]
    to_first = pack[TO_FIRST : TO_FIRST + 2 * first_size, 0:leaf_size]
    toward = product_back(product(leaf_rhs, leaf), to_first)
    terms[...] = product(first_rhs - toward[:, :first_size], first[0:first_size, 0:total])
    other[...] = toward[:, first_size:]


def first_body(sizes, side, total, cells, own_terms, other, first, below, above, pieces):
    peers, count = pieces.shape[:2]
    first_size = sizes[1]
    reach = cells.shape[1]
    after = cells[(side + 1) * count : (side + 2) * count, :]
    before = cells[0:count, :]
    below_order = below[first_size : first_size + 1, 0 : sum(sizes)]
    below_order = split_order(below_order, sizes)[1]
    number = numbers(side, "in") + float(side - 1)
    from_before = times_weights(before, one_hot(number, below_order))
    through = product(after, above[:, total : total + 2 * first_size])
    terms = own_terms[...] - product(through[:, first_size:], first[0:first_size, 0:total])
    terms = terms + product(from_before - other[...], below[0:first_size, 0:total])
    terms = terms - product(through[:, :first_size], above[0:first_size, 0:total])
    pieces[...] = jnp.zeros_like(pieces)
    place = lax.axis_index("gz")
    for p in range(peers):
        pieces[p, :, 0:first_size] = terms[:, p * first_size : (p + 1) * first_size]
        pieces[p, :, AFTER : AFTER + reach] = jnp.where(place + 1 == p, after, 0.0)
        pieces[p, :, BEFORE : BEFORE + reach] = jnp.where(place - 1 == p, before, 0.0)


def second_body(
    sizes, side, gz, received, cells, from_x, pack, second, below, pieces, leaf_out, first_out,
    toward_out, top_out,
):
    peers, count = pieces.shape[:2]
    leaf_size, first_size, second_size, top_size = sizes
    reach = cells.shape[1]
    total = received[0]
    for p in range(1, received.shape[0]):
        total = total + received[p]
    first_own = total[:, 0:first_size]
    cells = cells[...]
    after = total[:, AFTER : AFTER + reach]
    before = total[:, BEFORE : BEFORE + reach]
    cells = jnp.concatenate(
        [
            cells[0:count],
            cells[count : 2 * count] + after,
            cells[2 * count : side * count],
            cells[side * count : (side + 1) * count] + before,
            cells[(side + 1) * count :],
        ],
        axis=0,
    )
    leaf_order, _, second_order, top_order = packed_order(pack, sizes)
    number = numbers(side, "in")
    leaf = pack[LEAF : LEAF + leaf_size, 0:leaf_size]
    to_second = pack[TO_SECOND : TO_SECOND + 2 * second_size, 0:leaf_size]
    to_top = pack[TO_TOP : TO_TOP + 2 * top_size, 0:leaf_size]
    first_second = pack[FIRST_SECOND : FIRST_SECOND + first_size, 0 : 2 * second_size]
    first_top = pack[FIRST_TOP : FIRST_TOP + first_size, 0 : 2 * top_size]
    leaf_solved = product(picked(cells, count, side, number, leaf_order), leaf)
    second_rhs = picked(cells, count, side, number, second_order)
    top_out[...] = picked(cells, count, side, number, top_order)
    below_order = below[second_size : second_size + 1, 0 : sum(sizes)]
    _, _, below_second, below_top = split_order(below_order, sizes)
    number = numbers(side, "before_y")
    from_before = picked(cells, count, side, number, below_second)
    top_before = picked(cells, count, side, number, below_top)
    toward = product_back(leaf_solved, to_second) + product(first_own, first_second)
    terms = product(second_rhs - toward[:, :second_size], second[0:second_size, :])
    terms = terms + product(from_before - toward[:, second_size:], below[0:second_size, :])
    pieces[...] = jnp.zeros_like(pieces)
    place = (lax.axis_index("gy") - 1) * gz + lax.axis_index("gz")
    for p in range(peers):
        pieces[p, :, 0:second_size] = terms[:, p * second_size : (p + 1) * second_size]
        riding = jnp.where(place == p, top_before, 0.0)
        pieces[p, :, RIDING : RIDING + top_size] = riding
    leaf_out[...] = leaf_solved
    first_out[...] = first_own
    toward = product_back(leaf_solved, to_top) + product(first_own, first_top)
    order_x = from_x[8:9, 0:top_size]
    before_x = picked(cells, count, side, numbers(side, "before_x"), order_x)
    toward_out[:, :top_size] = toward[:, :top_size]
    toward_out[:, top_size:] = toward[:, top_size:] - before_x


def fold_body(top, out):
    rows, columns = top.shape
    full = rows // 8
    for g in range(full):
        out[:, g * columns : (g + 1) * columns] = top[8 * g : 8 * g + 8, :]
    half = columns // 2
    start = full * columns
    out[0:4, start : start + half] = top[8 * full : rows, 0:half]
    out[4:8, start : start + half] = top[8 * full : rows, half:columns]


def unfolded(folds, rows, columns, start, width):
    full = rows // 8
    parts = []
    for g in range(full):
        at = g * columns + start
        parts.append(folds[:, at : at + width])
    half = start // (columns // 2)
    at = full * columns + start - half * (columns // 2)
    parts.append(folds[4 * half : 4 * half + 4, at : at + width])
    return jnp.concatenate(parts, axis=0)


def top_body(used, shape, received, toward, rhs, pack, top, below, pieces, second_out):
    count = toward.shape[0]
    second_size = second_out.shape[1]
    top_size = rhs.shape[1]
    total = received[0]
    for p in range(1, received.shape[0]):
        total = total + received[p]
    second_own = total[:, 0:second_size]
    second_out[...] = second_own
    second_top = pack[SECOND_TOP : SECOND_TOP + second_size, 0 : 2 * top_size]
    toward = toward[...] + product(second_own, second_top)
    own = rhs[...] + total[:, RIDING : RIDING + top_size] - toward[:, :top_size]
    other = toward[:, top_size:]
    width = pieces.shape[2]
    vectors = []
    for vector in (own, -other):
        high, low = parts_of(vector)
        both = jnp.concatenate([high.astype(jnp.float32), low.astype(jnp.float32)], axis=0)
        vectors.append((both.astype(jnp.bfloat16), high))
    for p in range(used):
        total = None
        for (both, high), folds in zip(vectors, (top, below)):
            first, second = parts_of(unfolded(folds, *shape, p * width, width))
            term = dot(both, first)
            term = term[:count] + (term[count:] + dot(high, second))
            total = term if total is None else total + term
        pieces[p] = total
    for p in range(used, pieces.shape[0]):
        pieces[p] = jnp.zeros(pieces.shape[1:], jnp.float32)


def spread_sum_body(received, out):
    total = received[0]
    for p in range(1, received.shape[0]):
        total = total + received[p]
    for p in range(out.shape[0]):
        out[p] = total


def top_back_body(
    used, shape, whole, top, below, second_own, first_own, leaf_solved, pack, pair_out, second_gap,
    first_gap, leaf_gap,
):
    count = whole.shape[1]
    width = whole.shape[2]
    top_size = shape[0]

    halves = []
    for folds in (top, below):
        total = None
        for p in range(used):
            high, low = parts_of(whole[p])
            both = jnp.concatenate([high.astype(jnp.float32), low.astype(jnp.float32)], axis=0)
            first, second = parts_of(unfolded(folds, *shape, p * width, width))
            term = dot_back(both.astype(jnp.bfloat16), first)
            term = term[:count] + (term[count:] + dot_back(high, second))
            total = term if total is None else total + term
        halves.append(total)
    own, lower = halves
    pair_out[...] = own

    def against(matrix):
        return product_back(own, matrix[:, :top_size]) + product_back(lower, matrix[:, top_size:])

    second_rows, first_rows = second_own.shape[1], first_own.shape[1]
    second_gap[...] = second_own[...] - against(
        pack[SECOND_TOP : SECOND_TOP + second_rows, 0 : 2 * top_size]
    )
    first_gap[...] = first_own[...] - against(
        pack[FIRST_TOP : FIRST_TOP + first_rows, 0 : 2 * top_size]
    )
    rows = pack[TO_TOP : TO_TOP + 2 * top_size, 0 : leaf_solved.shape[1]]
    leaf_gap[...] = leaf_solved[...] - (
        product(own, rows[:top_size]) + product(lower, rows[top_size:])
    )


def second_back_body(
    sizes, side, whole, second, below, first_gap, leaf_gap, top_back, pack, sent, base_out,
    second_out,
):
    leaf_size, first_size, second_size, _ = sizes
    reach = side * 8
    own = product_back(whole[...], second[0:second_size, :])
    lower = product_back(whole[...], below[0:second_size, :])
    second_out[...] = own
    weights = pack[FIRST_SECOND : FIRST_SECOND + first_size, 0 : 2 * second_size]
    gap = first_gap[...] - product_back(own, weights[:, :second_size])
    gap = gap - product_back(lower, weights[:, second_size:])
    rows = pack[TO_SECOND : TO_SECOND + 2 * second_size, 0:leaf_size]
    rest = leaf_gap[...] - product(own, rows[:second_size]) - product(lower, rows[second_size:])
    base = product_back(rest, pack[LEAF : LEAF + leaf_size, 0:leaf_size])
    base_out[...] = base
    leaf_order, _, second_order, top_order = packed_order(pack, sizes)
    number = numbers(side, "out")
    face = times_weights_back(base, one_hot(number, leaf_order))
    face = face + times_weights_back(own, one_hot(number, second_order))
    face = face + times_weights_back(top_back[...], one_hot(number, top_order))
    sent[...] = jnp.zeros_like(sent)
    sent[:, 0:first_size] = gap
    sent[:, RIDING : RIDING + reach] = face


def leaf_back_body(
    sizes, side, received, base, second_back, top_back, pack, first, below, above, window,
):
    count = base.shape[0]
    peers = received.shape[0]
    leaf_size, first_size, _, _ = sizes
    reach = side * 8
    whole = jnp.concatenate([received[p, :, 0:first_size] for p in range(peers)], axis=1)
    total = whole.shape[1]
    own = product_back(whole, first[0:first_size, 0:total])
    lower = product_back(whole, below[0:first_size, 0:total])
    following = product_back(whole, above[0:first_size, 0:total])
    rows = pack[TO_FIRST : TO_FIRST + 2 * first_size, 0:leaf_size]
    rest = product(own, rows[:first_size]) + product(lower, rows[first_size:])
    leaf_back = base[...] - product_back(rest, pack[LEAF : LEAF + leaf_size, 0:leaf_size])
    face = jnp.zeros((count, reach), jnp.float32)
    place = lax.axis_index("gz") + 1
    for p in range(peers):
        riding = received[p, :, RIDING : RIDING + reach]
        face = face + jnp.where(place == p, riding, 0.0)
    through = above[:, total : total + 2 * first_size]
    moved = product_back(following, through[:, :first_size])
    moved = moved + product_back(own, through[:, first_size:])
    lane = lax.broadcasted_iota(jnp.int32, (through.shape[0], reach), 0)
    other = lax.broadcasted_iota(jnp.int32, (through.shape[0], reach), 1)
    shift = jnp.where(lane == other + 9, 1.0, 0.0)
    face = face - times_weights(moved, shift.astype(jnp.bfloat16))
    orders = packed_order(pack, sizes)
    number = numbers(side, "out")
    layers = placed(leaf_back, count, side, number, orders[0])
    layers = layers + placed(own, count, side, number, orders[1])
    layers = layers + placed(second_back[...], count, side, number, orders[2])
    layers = layers + placed(top_back[...], count, side, number, orders[3])
    cells = jnp.concatenate([layers, face, jnp.zeros_like(face)], axis=0)
    turned = weights_times_back(eye(reach), cells)
    window[...] = turned.reshape(window.shape)


def tent(at, cell):
    distance = jnp.abs(at - 4 * cell).astype(jnp.float32)
    return jnp.maximum(1.0 - 0.25 * distance, 0.0)


def prolong_body(inner, after_x, after_y, target, out, sent):
    count, fine = out.shape[:2]
    copies = []
    half = inner.shape[0] // 2
    cells = inner.shape[0] + 1
    window = jnp.concatenate([inner[...], after_x[...][None]], axis=0)
    row = lax.broadcasted_iota(jnp.int32, window.shape, 1)
    window = jnp.where(row == cells - 1, after_y[...][:, None, :], window)
    flat = window.reshape(cells * window.shape[1], window.shape[2])
    rows = lax.broadcasted_iota(jnp.int32, (cells * fine, cells * 8), 0)
    columns = lax.broadcasted_iota(jnp.int32, (cells * fine, cells * 8), 1)
    at = rows - (columns >> 3) * fine
    inside = (at >= 0) & (at < fine) & ((columns & 7) < cells)
    y_weights = jnp.where(inside, tent(at, columns & 7), 0.0).astype(jnp.bfloat16)
    along_y = weights_times(y_weights, flat)
    lane = lax.broadcasted_iota(jnp.int32, (window.shape[2], fine), 0)
    at = lax.broadcasted_iota(jnp.int32, (window.shape[2], fine), 1)
    for r in range(count):
        inside = ((lane & 3) == r) & ((lane >> 2) < cells)
        z_weights = jnp.where(inside, tent(at, lane >> 2), 0.0).astype(jnp.bfloat16)
        along_z = times_weights(along_y, z_weights)
        planes = [along_z[i * fine : (i + 1) * fine] for i in range(cells)]
        for i in range(cells - 1):
            for q in range(4):
                value = planes[i]
                if q:
                    value = (1.0 - q / 4.0) * value + (q / 4.0) * planes[i + 1]
                out[r, 4 * i + q] = value
            if (i + 1) % half == 0:
                part = pl.ds(4 * (i + 1 - half), 4 * half)
                copies.append(
                    pltpu.make_async_copy(
                        out.at[r, part], target.at[r, part], sent.at[len(copies)]
                    )
                )
                copies[-1].start()
    for copy in copies:
        copy.wait()


def prolonged(inner, after_x, after_y, count, fine):
    return pl.pallas_call(
        prolong_body,
        out_shape=jax.ShapeDtypeStruct((count, fine, fine, fine), jnp.float32),
        in_specs=[VMEM] * 3,
        out_specs=HBM,
        scratch_shapes=[
            pltpu.VMEM((count, fine, fine, fine), jnp.float32),
            pltpu.SemaphoreType.DMA((2 * count,)),
        ],
        compiler_params=LIMIT,
        name="prolong_twice",
    )(inner, after_x, after_y)


def call(body, outs, *operands):
    shapes = tuple(jax.ShapeDtypeStruct(o, jnp.float32) for o in outs)
    return pl.pallas_call(
        body,
        out_shape=shapes,
        in_specs=[VMEM] * len(operands),
        out_specs=(VMEM,) * len(shapes),
        compiler_params=LIMIT,
    )(*operands)


def per_device(
    right_side,
    iterate,
    coefficient,
    ordering,
    leaf_inverse,
    leaf_first,
    leaf_second,
    leaf_top,
    first_inverse,
    first_second,
    first_top,
    second_inverse,
    second_top,
    top_inverse,
):
    count, fine = right_side.shape[:2]
    leaf_size = leaf_inverse.shape[-1]
    first_size = first_second.shape[3]
    second_size = second_top.shape[3]
    top_size, top_total = top_inverse.shape
    sizes = (leaf_size, first_size, second_size, top_size)
    side = fine // 4
    cells = side**3
    lanes = (side + 2) * count
    gz = lax.axis_size("gz")
    plane_peers = lax.axis_size(PLANE)

    def rows_of(block):
        return jnp.transpose(block, (0, 1, 3, 2, 4)).reshape(block.shape[3], 1, block.shape[4])

    def columns_of(block):
        return jnp.transpose(block, (0, 1, 4, 2, 3)).reshape(block.shape[4], 1, block.shape[3])

    leaf = rows_of(leaf_inverse)
    to_first = columns_of(leaf_first)
    to_second = columns_of(leaf_second)
    to_top = jnp.swapaxes(leaf_top[0, 0, 0], 0, 1)
    first_to_second = rows_of(first_second)
    first_to_top = rows_of(first_top)
    second_to_top = rows_of(second_top)
    first = jnp.transpose(first_inverse, (0, 2, 1, 3)).reshape(first_size, 1, -1)
    second = jnp.transpose(second_inverse, (1, 0, 2))
    order = ordering.reshape(1, cells)

    inner, upper, folds = restricted(order, right_side, iterate, coefficient, top_inverse)
    from_x = shifted(upper, "gx", 1)
    whole_first = -(-max(first.shape[2] + 2 * first_size, cells) // 128) * 128
    up, down, beside, pack = prepared(
        sizes,
        side,
        whole_first,
        order,
        leaf,
        to_first,
        first,
        second,
        to_second,
        to_top,
        first_to_second,
        first_to_top,
        second_to_top,
    )
    first_below = shifted(up, "gz", 1)
    first_above = shifted(down, "gz", -1)
    top_below = shifted(folds, "gx", 1)
    beside = with_layer(inner, from_x, beside)
    second_below = shifted(beside, "gy", 1)

    total = first.shape[2]
    turned, own_terms, other = call(
        functools.partial(own_body, sizes, side, total),
        [(lanes, lanes_of(side)), (count, total), (count, first_size)],
        inner,
        from_x,
        second_below,
        pack,
        up,
    )
    (pieces,) = call(
        functools.partial(first_body, sizes, side, total),
        [(gz, count, 256)],
        turned,
        own_terms,
        other,
        up,
        first_below,
        first_above,
    )
    received = exchanged(pieces, "gz")
    pieces, leaf_solved, first_own, toward, top_rhs = call(
        functools.partial(second_body, sizes, side, gz),
        [
            (plane_peers, count, 128),
            (count, leaf_size),
            (count, first_size),
            (count, 2 * top_size),
            (count, top_size),
        ],
        received,
        turned,
        from_x,
        pack,
        beside,
        second_below,
    )
    received = exchanged(pieces, PLANE)
    width = 128 * -(-top_total // (128 * plane_peers))
    used = top_total // width
    pieces, second_own = call(
        functools.partial(top_body, used, top_inverse.shape),
        [(plane_peers, count, width), (count, second_size)],
        received,
        toward,
        top_rhs,
        pack,
        folds,
        top_below,
    )
    received = exchanged(pieces, PLANE)
    (pieces,) = call(spread_sum_body, [(lax.axis_size("gx"), count, width)], received)
    received = exchanged(pieces, "gx")
    (pieces,) = call(spread_sum_body, [(plane_peers, count, width)], received)
    received = exchanged(pieces, PLANE)
    top_back, second_gap, first_gap, leaf_gap = call(
        functools.partial(top_back_body, used, top_inverse.shape),
        [(count, top_size), (count, second_size), (count, first_size), (count, leaf_size)],
        received,
        folds,
        top_below,
        second_own,
        first_own,
        leaf_solved,
        pack,
    )
    second_whole = jnp.moveaxis(sent_to_all(second_gap, PLANE), 0, 1).reshape(count, -1)
    sent, base, second_back = call(
        functools.partial(second_back_body, sizes, side),
        [(count, 128), (count, leaf_size), (count, second_size)],
        second_whole,
        beside,
        second_below,
        first_gap,
        leaf_gap,
        top_back,
        pack,
    )
    received = sent_to_all(sent, "gz")
    (window,) = call(
        functools.partial(leaf_back_body, sizes, side),
        [(side, 8, lanes)],
        received,
        base,
        second_back,
        top_back,
        pack,
        up,
        first_below,
        first_above,
    )
    after_x = shifted(window[0], "gx", -1)
    layer = jnp.concatenate([window[:, 0], after_x[0:1]], axis=0)
    after_y = shifted(layer, "gy", -1)
    return prolonged(window, after_x, after_y, count, fine)


def solution(mesh):
    blocks = P("gx", "gy", "gz")
    return jax.shard_map(
        per_device,
        mesh=mesh,
        in_specs=(
            P(None, "gx", "gy", "gz"),
            P(None, "gx", "gy", "gz"),
            blocks,
            blocks,
            blocks,
            blocks,
            blocks,
            blocks,
            blocks,
            blocks,
            blocks,
            P("gx", PLANE, None),
            blocks,
            P(("gx", "gy", "gz"), None),
        ),
        out_specs=P(None, "gx", "gy", "gz"),
        check_vma=False,
    )
```

```python
import functools

import jax
import jax.numpy as jnp
from jax import lax
from jax.experimental import pallas as pl
from jax.experimental.pallas import tpu as pltpu
from jax.sharding import PartitionSpec as P

PLANE = ("gy", "gz")
AXES = ("gx", "gy", "gz")
VMEM = pl.BlockSpec(memory_space=pltpu.VMEM)
HBM = pl.BlockSpec(memory_space=pltpu.HBM)
LIMIT = pltpu.CompilerParams(vmem_limit_bytes=16 * 1024 * 1024)


def in_hbm(values):
    return pltpu.with_memory_space_constraint(values, pltpu.HBM)


def shifted(shard, axis, by):
    peers = lax.axis_size(axis)
    pairs = [(i, i + by) for i in range(peers) if 0 <= i + by < peers]
    return lax.ppermute(shard, axis, pairs)


def exchanged(pieces, axis):
    return lax.all_to_all(pieces, axis, split_axis=0, concat_axis=0, tiled=True)


def sent_to_all(shard, axis):
    copies = jnp.broadcast_to(shard, (lax.axis_size(axis), *shard.shape))
    return exchanged(copies, axis)


def parts_of(values):
    first = values.astype(jnp.bfloat16)
    second = (values - first.astype(jnp.float32)).astype(jnp.bfloat16)
    return first, second


def dot(left, right):
    return jnp.dot(left, right, preferred_element_type=jnp.float32)


def dot_back(left, right):
    return lax.dot_general(
        left, right, (((1,), (1,)), ((), ())), preferred_element_type=jnp.float32
    )


def product(operand, matrix):
    high, low = parts_of(operand)
    first, second = parts_of(matrix)
    return dot(high, first) + (dot(high, second) + dot(low, first))


def product_back(operand, matrix):
    high, low = parts_of(operand)
    first, second = parts_of(matrix)
    return dot_back(high, first) + (dot_back(high, second) + dot_back(low, first))


def times_weights(values, weights):
    first, second = parts_of(values)
    return dot(first, weights) + dot(second, weights)


def weights_times(weights, values):
    first, second = parts_of(values)
    return dot(weights, first) + dot(weights, second)


def times_weights_back(values, weights):
    first, second = parts_of(values)
    return dot_back(first, weights) + dot_back(second, weights)


def weights_times_back(weights, values):
    first, second = parts_of(values)
    return dot_back(weights, first) + dot_back(weights, second)


def weight_rows(coarse, fine, kind, missing):
    rows = lax.broadcasted_iota(jnp.int32, (coarse * coarse, coarse * fine), 0)
    columns = lax.broadcasted_iota(jnp.int32, (coarse * coarse, coarse * fine), 1)
    at = columns - (rows >> 3) * fine
    weights = weights_at(4 * ((rows & 7) - 1), at, kind, missing)
    return jnp.where((at >= 0) & (at < fine), weights, 0.0).astype(jnp.bfloat16)


def weight_lanes(coarse, fine, count, r, kind, missing):
    at = lax.broadcasted_iota(jnp.int32, (fine, coarse * count), 0)
    lane = lax.broadcasted_iota(jnp.int32, (fine, coarse * count), 1)
    weights = weights_at(4 * ((lane >> 2) - 1), at, kind, missing)
    return jnp.where((lane & 3) == r, weights, 0.0).astype(jnp.bfloat16)


def weights_at(cell, at, kind, missing):
    def weight(distance):
        return jnp.maximum(4.0 - jnp.abs(distance).astype(jnp.float32), 0.0) * 0.0625

    if kind == "own":
        return weight(cell - at)
    before = jnp.where(at == 0, missing, 0.0)
    return weight(cell - at - 1) + (1.0 - before) * weight(cell - at + 1)


def restricted_layers(layers):
    out = {}
    for x, layer in layers.items():
        if x % 2 == 0:
            shares = [(x // 2, 0.5)]
        else:
            shares = [((x - 1) // 2, 0.25), ((x + 1) // 2, 0.25)]
        for cell, weight in shares:
            term = weight * layer
            out[cell] = out[cell] + term if cell in out else term
    return out


def restrict_body(
    order_in, rhs_in, iterate_in, coefficient_in, top_in, inner, upper, folds,
    rhs, iterate, coefficient, order, top, arrived,
):
    count, fine = rhs.shape[:2]
    coarse = inner.shape[1]
    half = fine // 2
    copies = [pltpu.make_async_copy(coefficient_in, coefficient, arrived.at[0])]
    for r in range(count):
        for source, room in ((iterate_in, iterate), (rhs_in, rhs)):
            for start in (0, half):
                part = pl.ds(start, half)
                copies.append(
                    pltpu.make_async_copy(
                        source.at[r, part], room.at[r, part], arrived.at[len(copies)]
                    )
                )
    copies.append(pltpu.make_async_copy(order_in, order, arrived.at[len(copies)]))
    copies.append(pltpu.make_async_copy(top_in, top, arrived.at[len(copies)]))
    for copy in copies:
        copy.start()
    at_x, at_y, at_z = [jnp.where(lax.axis_index(a) == 0, 1.0, 0.0) for a in AXES]
    layer, lanes = inner.shape[1:]
    top_size = coarse - 2
    top_size = top_size * top_size
    upper[...] = jnp.zeros_like(upper)
    y_cell = weight_rows(coarse, fine, "own", None)
    y_pair = weight_rows(coarse, fine, "beside", at_y)
    z_cells = [weight_lanes(coarse, fine, count, r, "own", None) for r in range(count)]
    z_pairs = [weight_lanes(coarse, fine, count, r, "beside", at_z) for r in range(count)]
    copies[0].wait()
    beside_sum = None
    own_sum = None
    for r in range(count):
        for copy in copies[4 * r + 1 : 4 * r + 5]:
            copy.wait()
        planes = [iterate[r, x] for x in range(fine)]
        gaps = [rhs[r, x] - (6.0 + coefficient[x]) * planes[x] for x in range(fine)]
        sums = {-1: (1.0 - at_x) * planes[0], fine: planes[-1]}
        for x in range(fine):
            total = gaps[x]
            for beside in (x - 1, x + 1):
                if 0 <= beside < fine:
                    total = total + planes[beside]
            sums[x] = total
        values = restricted_layers(restricted_layers(sums))
        cells = restricted_layers(restricted_layers(dict(enumerate(planes))))
        values = [values[i] for i in range(-1, coarse - 1)]
        cells = [jnp.zeros_like(planes[0])] + [cells[i] for i in range(coarse - 1)]
        value = jnp.concatenate(values, axis=0)
        cell = jnp.concatenate(cells, axis=0)
        term = times_weights(value, z_cells[r]) + times_weights(cell, z_pairs[r])
        beside_sum = term if beside_sum is None else beside_sum + term
        term = times_weights(cell, z_cells[r])
        own_sum = term if own_sum is None else own_sum + term
    result = weights_times(y_cell, beside_sum) + weights_times(y_pair, own_sum)
    result = result.reshape(coarse, coarse, coarse * count)
    inner[...] = result[:-1]
    upper[0:layer, 0:lanes] = result[coarse - 1]
    copies[-2].wait()
    copies[-1].wait()
    fold_body(top, folds)
    orders = order[...].astype(jnp.float32)
    upper[layer : layer + 1, 0:top_size] = orders[:, orders.shape[1] - top_size :]


def restricted(order, right_side, iterate, coefficient, top):
    count, fine = right_side.shape[:2]
    coarse = fine // 4 + 2

    inner = jax.ShapeDtypeStruct((coarse - 1, coarse, coarse * count), jnp.float32)
    upper = jax.ShapeDtypeStruct((2 * coarse, 128), jnp.float32)
    folds = jax.ShapeDtypeStruct((8, top.size // 8), jnp.float32)
    return pl.pallas_call(
        restrict_body,
        out_shape=(inner, upper, folds),
        in_specs=[HBM] * 5,
        out_specs=(VMEM,) * 3,
        scratch_shapes=[
            pltpu.VMEM(right_side.shape, jnp.float32),
            pltpu.VMEM(iterate.shape, jnp.float32),
            pltpu.VMEM(coefficient.shape, jnp.float32),
            pltpu.VMEM(order.shape, order.dtype),
            pltpu.VMEM(top.shape, jnp.float32),
            pltpu.SemaphoreType.DMA((4 * count + 3,)),
        ],
        compiler_params=LIMIT,
        name="restrict_twice",
    )(*map(in_hbm, (order, right_side, iterate, coefficient, top)))


def numbers(side, kind):
    lane = lax.broadcasted_iota(jnp.int32, (lanes_of(side, kind), 1), 0)
    x, y = lane >> 3, lane & 7
    if kind == "out":
        number = jnp.where(y < side, x * side * side + y * side, -1000)
        return number.astype(jnp.float32)
    x, y = x - 1, y - 1
    last = side - 1
    along_y = (y >= 0) & (y < side)
    if kind == "in":
        number = jnp.where((x >= 0) & along_y, x * side * side + y * side, -1000)
    elif kind == "before_y":
        number = jnp.where((x >= 0) & (y < 0), x * side * side + last * side, -1000)
    else:
        number = jnp.where((x < 0) & along_y, last * side * side + y * side, -1000)
    return number.astype(jnp.float32)


def lanes_of(side, kind="in"):
    return side * 8 if kind == "out" else (side + 1) * 8


def one_hot(number, order):
    return jnp.where(number == order, 1.0, 0.0).astype(jnp.bfloat16)


def eye(size):
    rows = lax.broadcasted_iota(jnp.int32, (size, size), 0)
    return jnp.where(rows == lax.broadcasted_iota(jnp.int32, (size, size), 1), 1.0, 0.0).astype(
        jnp.bfloat16
    )


def layers_in(order, side):
    return order - side * jnp.floor((order + 0.5) * (1.0 / side))


def on_own_layer(rows, order, count, side):
    row = lax.broadcasted_iota(jnp.int32, (rows, order.shape[1]), 0)
    return (row // count).astype(jnp.float32) == layers_in(order, side)


def picked(cells, count, side, number, order):
    layers = cells[count : (side + 1) * count]
    lanes = one_hot(number, order - layers_in(order, side))
    values = times_weights(layers, lanes)
    values = jnp.where(on_own_layer(side * count, order, count, side), values, 0.0)
    total = values[0:count]
    for z in range(1, side):
        total = total + values[z * count : (z + 1) * count]
    return total


def placed(values, count, side, number, order):
    values = jnp.concatenate([values] * side, axis=0)
    values = jnp.where(on_own_layer(side * count, order, count, side), values, 0.0)
    return times_weights_back(values, one_hot(number, order - layers_in(order, side)))


LEAF, TO_FIRST, TO_SECOND, TO_TOP = 0, 128, 184, 248
FIRST_SECOND, FIRST_TOP, SECOND_TOP, ORDER, PACKED = 320, 352, 384, 416, 424


def split_order(order, sizes):
    out, start = [], 0
    for size in sizes:
        out.append(order[:, start : start + size])
        start += size
    return out


def packed_order(pack, sizes):
    leaf_size = sizes[0]
    leaf_order = pack[ORDER : ORDER + 1, 0:leaf_size]
    rest = pack[ORDER + 1 : ORDER + 2, 0 : sum(sizes[1:])]
    return [leaf_order] + split_order(rest, sizes[1:])


def prepare_body(sizes, side, *refs):
    order, leaf, to_first, first, second = refs[:5]
    up, down, beside, pack = refs[5:]
    up[...] = jnp.zeros_like(up)
    down[...] = jnp.zeros_like(down)
    beside[sizes[2] :, :] = jnp.zeros_like(beside[sizes[2] :, :])
    order = order[...].astype(jnp.float32)
    leaf_size, first_size, second_size = sizes[:3]
    leaf_rows, first_columns = leaf[:, 0, :], to_first[:, 0, :]
    first_rows = first[:, 0, :]
    face = one_hot(numbers(side, "in"), order[:, :leaf_size])
    rows = weights_times(face, leaf_rows)
    up[0:first_size, 0 : first_rows.shape[1]] = first_rows
    up[first_size : first_size + 1, 0 : order.shape[1]] = order
    total = first_rows.shape[1]
    down[:, total : total + 2 * first_size] = product_back(rows, first_columns)
    down[0:first_size, 0:total] = first_rows
    beside[0:second_size, :] = second[:, 0, :]
    beside[second_size : second_size + 1, 0 : order.shape[1]] = order
    pack[ORDER : ORDER + 1, 0:leaf_size] = order[:, :leaf_size]
    pack[ORDER + 1 : ORDER + 2, 0 : order.shape[1] - leaf_size] = order[:, leaf_size:]
    for start, rows in ((LEAF, leaf_rows), (TO_FIRST, first_columns)):
        pack[start : start + rows.shape[0], 0 : rows.shape[1]] = rows


def pack_later(pack, to_second, to_top, first_second, first_top, second_top):
    for start, rows in (
        (TO_SECOND, to_second[:, 0, :]),
        (TO_TOP, to_top[...]),
        (FIRST_SECOND, first_second[:, 0, :]),
        (FIRST_TOP, first_top[:, 0, :]),
        (SECOND_TOP, second_top[:, 0, :]),
    ):
        pack[start : start + rows.shape[0], 0 : rows.shape[1]] = rows


def prepared(sizes, side, width, *sources):
    leaf_size, first_size, second_size, top_size = sizes
    assert leaf_size <= 128 and first_size < 32 and second_size < 32 and top_size <= 36
    shapes = (
        (32, width),
        (lanes_of(side), width),
        (40, sources[4].shape[2]),
        (PACKED, 128),
    )
    return pl.pallas_call(
        functools.partial(prepare_body, sizes, side),
        out_shape=tuple(jax.ShapeDtypeStruct(o, jnp.float32) for o in shapes),
        in_specs=[VMEM] * len(sources),
        out_specs=(VMEM,) * len(shapes),
        compiler_params=LIMIT,
        name="prepare",
    )(*sources)


AFTER, BEFORE, RIDING = 32, 128, 64

LAYER = 32


def message_body(inner, from_x, _, message):
    along, lanes = inner.shape[1:]
    rows = inner[:, along - 1, :]
    row = lax.broadcasted_iota(jnp.int32, rows.shape, 0)
    rows = rows + jnp.where(row == 1, from_x[along - 1 : along, 0:lanes], 0.0)
    message[LAYER : LAYER + rows.shape[0], 0:lanes] = rows


def with_layer(inner, from_x, beside):
    return pl.pallas_call(
        message_body,
        out_shape=jax.ShapeDtypeStruct(beside.shape, jnp.float32),
        in_specs=[VMEM] * 3,
        out_specs=VMEM,
        input_output_aliases={2: 0},
        compiler_params=LIMIT,
        name="y_message",
    )(inner, from_x, beside)


def own_body(
    sizes, side, total, inner, from_x, from_y, pack, first, *refs
):
    later, (cells_out, terms, other, pack_out) = refs[:5], refs[5:]
    pack_later(pack_out, *later)
    leaf_size, first_size = sizes[:2]
    leaf_order, first_order = packed_order(pack, sizes)[:2]
    values = inner[...]
    across, along, lanes = values.shape
    reach = across * along
    count = terms.shape[0]
    row = lax.broadcasted_iota(jnp.int32, values.shape, 0)
    values = values + jnp.where(row == 1, from_x[0:along, 0:lanes][None], 0.0)
    row = lax.broadcasted_iota(jnp.int32, values.shape, 1)
    layer = from_y[LAYER : LAYER + across, 0:lanes]
    values = values + jnp.where(row == 1, layer[:, None, :], 0.0)
    cells = weights_times_back(eye(lanes), values.reshape(reach, lanes))
    cells_out[...] = cells
    number = numbers(side, "in")
    leaf_rhs = picked(cells, count, side, number, leaf_order)
    first_rhs = picked(cells, count, side, number, first_order)
    leaf = pack[LEAF : LEAF + leaf_size, 0:leaf_size]
    to_first = pack[TO_FIRST : TO_FIRST + 2 * first_size, 0:leaf_size]
    toward = product_back(product(leaf_rhs, leaf), to_first)
    terms[...] = product(first_rhs - toward[:, :first_size], first[0:first_size, 0:total])
    other[...] = toward[:, first_size:]


def first_body(sizes, side, total, cells, own_terms, other, first, below, above, pieces):
    peers, count = pieces.shape[:2]
    first_size = sizes[1]
    reach = cells.shape[1]
    after = cells[(side + 1) * count : (side + 2) * count, :]
    before = cells[0:count, :]
    below_order = below[first_size : first_size + 1, 0 : sum(sizes)]
    below_order = split_order(below_order, sizes)[1]
    number = numbers(side, "in") + float(side - 1)
    from_before = times_weights(before, one_hot(number, below_order))
    through = product(after, above[:, total : total + 2 * first_size])
    terms = own_terms[...] - product(through[:, first_size:], first[0:first_size, 0:total])
    terms = terms + product(from_before - other[...], below[0:first_size, 0:total])
    terms = terms - product(through[:, :first_size], above[0:first_size, 0:total])
    pieces[...] = jnp.zeros_like(pieces)
    place = lax.axis_index("gz")
    for p in range(peers):
        pieces[p, :, 0:first_size] = terms[:, p * first_size : (p + 1) * first_size]
        pieces[p, :, AFTER : AFTER + reach] = jnp.where(place + 1 == p, after, 0.0)
        pieces[p, :, BEFORE : BEFORE + reach] = jnp.where(place - 1 == p, before, 0.0)


def second_body(
    sizes, side, gz, received, cells, from_x, pack, second, below, pieces, leaf_out, first_out,
    toward_out, top_out,
):
    peers, count = pieces.shape[:2]
    leaf_size, first_size, second_size, top_size = sizes
    reach = cells.shape[1]
    total = received[0]
    for p in range(1, received.shape[0]):
        total = total + received[p]
    first_own = total[:, 0:first_size]
    cells = cells[...]
    after = total[:, AFTER : AFTER + reach]
    before = total[:, BEFORE : BEFORE + reach]
    cells = jnp.concatenate(
        [
            cells[0:count],
            cells[count : 2 * count] + after,
            cells[2 * count : side * count],
            cells[side * count : (side + 1) * count] + before,
            cells[(side + 1) * count :],
        ],
        axis=0,
    )
    leaf_order, _, second_order, top_order = packed_order(pack, sizes)
    number = numbers(side, "in")
    leaf = pack[LEAF : LEAF + leaf_size, 0:leaf_size]
    to_second = pack[TO_SECOND : TO_SECOND + 2 * second_size, 0:leaf_size]
    to_top = pack[TO_TOP : TO_TOP + 2 * top_size, 0:leaf_size]
    first_second = pack[FIRST_SECOND : FIRST_SECOND + first_size, 0 : 2 * second_size]
    first_top = pack[FIRST_TOP : FIRST_TOP + first_size, 0 : 2 * top_size]
    leaf_solved = product(picked(cells, count, side, number, leaf_order), leaf)
    second_rhs = picked(cells, count, side, number, second_order)
    top_out[...] = picked(cells, count, side, number, top_order)
    below_order = below[second_size : second_size + 1, 0 : sum(sizes)]
    _, _, below_second, below_top = split_order(below_order, sizes)
    number = numbers(side, "before_y")
    from_before = picked(cells, count, side, number, below_second)
    top_before = picked(cells, count, side, number, below_top)
    toward = product_back(leaf_solved, to_second) + product(first_own, first_second)
    terms = product(second_rhs - toward[:, :second_size], second[0:second_size, :])
    terms = terms + product(from_before - toward[:, second_size:], below[0:second_size, :])
    pieces[...] = jnp.zeros_like(pieces)
    place = (lax.axis_index("gy") - 1) * gz + lax.axis_index("gz")
    for p in range(peers):
        pieces[p, :, 0:second_size] = terms[:, p * second_size : (p + 1) * second_size]
        riding = jnp.where(place == p, top_before, 0.0)
        pieces[p, :, RIDING : RIDING + top_size] = riding
    leaf_out[...] = leaf_solved
    first_out[...] = first_own
    toward = product_back(leaf_solved, to_top) + product(first_own, first_top)
    order_x = from_x[8:9, 0:top_size]
    before_x = picked(cells, count, side, numbers(side, "before_x"), order_x)
    toward_out[:, :top_size] = toward[:, :top_size]
    toward_out[:, top_size:] = toward[:, top_size:] - before_x


def fold_body(top, out):
    rows, columns = top.shape
    full = rows // 8
    for g in range(full):
        out[:, g * columns : (g + 1) * columns] = top[8 * g : 8 * g + 8, :]
    half = columns // 2
    start = full * columns
    out[0:4, start : start + half] = top[8 * full : rows, 0:half]
    out[4:8, start : start + half] = top[8 * full : rows, half:columns]


def unfolded(folds, rows, columns, start, width):
    full = rows // 8
    parts = []
    for g in range(full):
        at = g * columns + start
        parts.append(folds[:, at : at + width])
    half = start // (columns // 2)
    at = full * columns + start - half * (columns // 2)
    parts.append(folds[4 * half : 4 * half + 4, at : at + width])
    return jnp.concatenate(parts, axis=0)


def top_body(used, shape, received, toward, rhs, pack, top, below, pieces, second_out):
    count = toward.shape[0]
    second_size = second_out.shape[1]
    top_size = rhs.shape[1]
    total = received[0]
    for p in range(1, received.shape[0]):
        total = total + received[p]
    second_own = total[:, 0:second_size]
    second_out[...] = second_own
    second_top = pack[SECOND_TOP : SECOND_TOP + second_size, 0 : 2 * top_size]
    toward = toward[...] + product(second_own, second_top)
    own = rhs[...] + total[:, RIDING : RIDING + top_size] - toward[:, :top_size]
    other = toward[:, top_size:]
    width = pieces.shape[2]
    vectors = []
    for vector in (own, -other):
        high, low = parts_of(vector)
        both = jnp.concatenate([high.astype(jnp.float32), low.astype(jnp.float32)], axis=0)
        vectors.append((both.astype(jnp.bfloat16), high))
    for p in range(used):
        total = None
        for (both, high), folds in zip(vectors, (top, below)):
            first, second = parts_of(unfolded(folds, *shape, p * width, width))
            term = dot(both, first)
            term = term[:count] + (term[count:] + dot(high, second))
            total = term if total is None else total + term
        pieces[p] = total
    for p in range(used, pieces.shape[0]):
        pieces[p] = jnp.zeros(pieces.shape[1:], jnp.float32)


def spread_sum_body(received, out):
    total = received[0]
    for p in range(1, received.shape[0]):
        total = total + received[p]
    for p in range(out.shape[0]):
        out[p] = total


def top_back_body(
    used, shape, whole, top, below, second_own, first_own, leaf_solved, pack, pair_out, second_gap,
    first_gap, leaf_gap,
):
    count = whole.shape[1]
    width = whole.shape[2]
    top_size = shape[0]

    halves = []
    for folds in (top, below):
        total = None
        for p in range(used):
            high, low = parts_of(whole[p])
            both = jnp.concatenate([high.astype(jnp.float32), low.astype(jnp.float32)], axis=0)
            first, second = parts_of(unfolded(folds, *shape, p * width, width))
            term = dot_back(both.astype(jnp.bfloat16), first)
            term = term[:count] + (term[count:] + dot_back(high, second))
            total = term if total is None else total + term
        halves.append(total)
    own, lower = halves
    pair_out[...] = own

    def against(matrix):
        return product_back(own, matrix[:, :top_size]) + product_back(lower, matrix[:, top_size:])

    second_rows, first_rows = second_own.shape[1], first_own.shape[1]
    second_gap[...] = second_own[...] - against(
        pack[SECOND_TOP : SECOND_TOP + second_rows, 0 : 2 * top_size]
    )
    first_gap[...] = first_own[...] - against(
        pack[FIRST_TOP : FIRST_TOP + first_rows, 0 : 2 * top_size]
    )
    rows = pack[TO_TOP : TO_TOP + 2 * top_size, 0 : leaf_solved.shape[1]]
    leaf_gap[...] = leaf_solved[...] - (
        product(own, rows[:top_size]) + product(lower, rows[top_size:])
    )


def second_back_body(
    sizes, side, whole, second, below, first_gap, leaf_gap, top_back, pack, sent, base_out,
    second_out,
):
    leaf_size, first_size, second_size, _ = sizes
    reach = side * 8
    own = product_back(whole[...], second[0:second_size, :])
    lower = product_back(whole[...], below[0:second_size, :])
    second_out[...] = own
    weights = pack[FIRST_SECOND : FIRST_SECOND + first_size, 0 : 2 * second_size]
    gap = first_gap[...] - product_back(own, weights[:, :second_size])
    gap = gap - product_back(lower, weights[:, second_size:])
    rows = pack[TO_SECOND : TO_SECOND + 2 * second_size, 0:leaf_size]
    rest = leaf_gap[...] - product(own, rows[:second_size]) - product(lower, rows[second_size:])
    base = product_back(rest, pack[LEAF : LEAF + leaf_size, 0:leaf_size])
    base_out[...] = base
    leaf_order, _, second_order, top_order = packed_order(pack, sizes)
    number = numbers(side, "out")
    face = times_weights_back(base, one_hot(number, leaf_order))
    face = face + times_weights_back(own, one_hot(number, second_order))
    face = face + times_weights_back(top_back[...], one_hot(number, top_order))
    sent[...] = jnp.zeros_like(sent)
    sent[:, 0:first_size] = gap
    sent[:, RIDING : RIDING + reach] = face


def leaf_back_body(
    sizes, side, received, base, second_back, top_back, pack, first, below, above, window,
):
    count = base.shape[0]
    peers = received.shape[0]
    leaf_size, first_size, _, _ = sizes
    reach = side * 8
    whole = jnp.concatenate([received[p, :, 0:first_size] for p in range(peers)], axis=1)
    total = whole.shape[1]
    own = product_back(whole, first[0:first_size, 0:total])
    lower = product_back(whole, below[0:first_size, 0:total])
    following = product_back(whole, above[0:first_size, 0:total])
    rows = pack[TO_FIRST : TO_FIRST + 2 * first_size, 0:leaf_size]
    rest = product(own, rows[:first_size]) + product(lower, rows[first_size:])
    leaf_back = base[...] - product_back(rest, pack[LEAF : LEAF + leaf_size, 0:leaf_size])
    face = jnp.zeros((count, reach), jnp.float32)
    place = lax.axis_index("gz") + 1
    for p in range(peers):
        riding = received[p, :, RIDING : RIDING + reach]
        face = face + jnp.where(place == p, riding, 0.0)
    through = above[:, total : total + 2 * first_size]
    moved = product_back(following, through[:, :first_size])
    moved = moved + product_back(own, through[:, first_size:])
    lane = lax.broadcasted_iota(jnp.int32, (through.shape[0], reach), 0)
    other = lax.broadcasted_iota(jnp.int32, (through.shape[0], reach), 1)
    shift = jnp.where(lane == other + 9, 1.0, 0.0)
    face = face - times_weights(moved, shift.astype(jnp.bfloat16))
    orders = packed_order(pack, sizes)
    number = numbers(side, "out")
    layers = placed(leaf_back, count, side, number, orders[0])
    layers = layers + placed(own, count, side, number, orders[1])
    layers = layers + placed(second_back[...], count, side, number, orders[2])
    layers = layers + placed(top_back[...], count, side, number, orders[3])
    cells = jnp.concatenate([layers, face, jnp.zeros_like(face)], axis=0)
    turned = weights_times_back(eye(reach), cells)
    window[...] = turned.reshape(window.shape)


def tent(at, cell):
    distance = jnp.abs(at - 4 * cell).astype(jnp.float32)
    return jnp.maximum(1.0 - 0.25 * distance, 0.0)


def prolong_body(inner, after_x, after_y, target, out, sent):
    count, fine = out.shape[:2]
    copies = []
    half = inner.shape[0] // 2
    cells = inner.shape[0] + 1
    window = jnp.concatenate([inner[...], after_x[...][None]], axis=0)
    row = lax.broadcasted_iota(jnp.int32, window.shape, 1)
    window = jnp.where(row == cells - 1, after_y[...][:, None, :], window)
    flat = window.reshape(cells * window.shape[1], window.shape[2])
    rows = lax.broadcasted_iota(jnp.int32, (cells * fine, cells * 8), 0)
    columns = lax.broadcasted_iota(jnp.int32, (cells * fine, cells * 8), 1)
    at = rows - (columns >> 3) * fine
    inside = (at >= 0) & (at < fine) & ((columns & 7) < cells)
    y_weights = jnp.where(inside, tent(at, columns & 7), 0.0).astype(jnp.bfloat16)
    along_y = weights_times(y_weights, flat)
    lane = lax.broadcasted_iota(jnp.int32, (window.shape[2], fine), 0)
    at = lax.broadcasted_iota(jnp.int32, (window.shape[2], fine), 1)
    for r in range(count):
        inside = ((lane & 3) == r) & ((lane >> 2) < cells)
        z_weights = jnp.where(inside, tent(at, lane >> 2), 0.0).astype(jnp.bfloat16)
        along_z = times_weights(along_y, z_weights)
        planes = [along_z[i * fine : (i + 1) * fine] for i in range(cells)]
        for i in range(cells - 1):
            for q in range(4):
                value = planes[i]
                if q:
                    value = (1.0 - q / 4.0) * value + (q / 4.0) * planes[i + 1]
                out[r, 4 * i + q] = value
            if (i + 1) % half == 0:
                part = pl.ds(4 * (i + 1 - half), 4 * half)
                copies.append(
                    pltpu.make_async_copy(
                        out.at[r, part], target.at[r, part], sent.at[len(copies)]
                    )
                )
                copies[-1].start()
    for copy in copies:
        copy.wait()


def prolonged(inner, after_x, after_y, count, fine):
    return pl.pallas_call(
        prolong_body,
        out_shape=jax.ShapeDtypeStruct((count, fine, fine, fine), jnp.float32),
        in_specs=[VMEM] * 3,
        out_specs=HBM,
        scratch_shapes=[
            pltpu.VMEM((count, fine, fine, fine), jnp.float32),
            pltpu.SemaphoreType.DMA((2 * count,)),
        ],
        compiler_params=LIMIT,
        name="prolong_twice",
    )(inner, after_x, after_y)


def call(body, outs, *operands, aliases={}):
    shapes = tuple(jax.ShapeDtypeStruct(o, jnp.float32) for o in outs)
    return pl.pallas_call(
        body,
        out_shape=shapes,
        in_specs=[VMEM] * len(operands),
        out_specs=(VMEM,) * len(shapes),
        input_output_aliases=aliases,
        compiler_params=LIMIT,
    )(*operands)


def per_device(
    right_side,
    iterate,
    coefficient,
    ordering,
    leaf_inverse,
    leaf_first,
    leaf_second,
    leaf_top,
    first_inverse,
    first_second,
    first_top,
    second_inverse,
    second_top,
    top_inverse,
):
    count, fine = right_side.shape[:2]
    leaf_size = leaf_inverse.shape[-1]
    first_size = first_second.shape[3]
    second_size = second_top.shape[3]
    top_size, top_total = top_inverse.shape
    sizes = (leaf_size, first_size, second_size, top_size)
    side = fine // 4
    cells = side**3
    lanes = (side + 2) * count
    gz = lax.axis_size("gz")
    plane_peers = lax.axis_size(PLANE)

    def rows_of(block):
        return jnp.transpose(block, (0, 1, 3, 2, 4)).reshape(block.shape[3], 1, block.shape[4])

    def columns_of(block):
        return jnp.transpose(block, (0, 1, 4, 2, 3)).reshape(block.shape[4], 1, block.shape[3])

    leaf = rows_of(leaf_inverse)
    to_first = columns_of(leaf_first)
    to_second = columns_of(leaf_second)
    to_top = jnp.swapaxes(leaf_top[0, 0, 0], 0, 1)
    first_to_second = rows_of(first_second)
    first_to_top = rows_of(first_top)
    second_to_top = rows_of(second_top)
    first = jnp.transpose(first_inverse, (0, 2, 1, 3)).reshape(first_size, 1, -1)
    second = jnp.transpose(second_inverse, (1, 0, 2))
    order = ordering.reshape(1, cells)

    inner, upper, folds = restricted(order, right_side, iterate, coefficient, top_inverse)
    from_x = shifted(upper, "gx", 1)
    whole_first = -(-max(first.shape[2] + 2 * first_size, cells) // 128) * 128
    up, down, beside, pack = prepared(
        sizes,
        side,
        whole_first,
        order,
        leaf,
        to_first,
        first,
        second,
    )
    first_below = shifted(up, "gz", 1)
    first_above = shifted(down, "gz", -1)
    top_below = shifted(folds, "gx", 1)
    beside = with_layer(inner, from_x, beside)
    second_below = shifted(beside, "gy", 1)

    total = first.shape[2]
    turned, own_terms, other, pack = call(
        functools.partial(own_body, sizes, side, total),
        [(lanes, lanes_of(side)), (count, total), (count, first_size), pack.shape],
        inner,
        from_x,
        second_below,
        pack,
        up,
        to_second,
        to_top,
        first_to_second,
        first_to_top,
        second_to_top,
        aliases={3: 3},
    )
    (pieces,) = call(
        functools.partial(first_body, sizes, side, total),
        [(gz, count, 256)],
        turned,
        own_terms,
        other,
        up,
        first_below,
        first_above,
    )
    received = exchanged(pieces, "gz")
    pieces, leaf_solved, first_own, toward, top_rhs = call(
        functools.partial(second_body, sizes, side, gz),
        [
            (plane_peers, count, 128),
            (count, leaf_size),
            (count, first_size),
            (count, 2 * top_size),
            (count, top_size),
        ],
        received,
        turned,
        from_x,
        pack,
        beside,
        second_below,
    )
    received = exchanged(pieces, PLANE)
    width = 128 * -(-top_total // (128 * plane_peers))
    used = top_total // width
    pieces, second_own = call(
        functools.partial(top_body, used, top_inverse.shape),
        [(plane_peers, count, width), (count, second_size)],
        received,
        toward,
        top_rhs,
        pack,
        folds,
        top_below,
    )
    received = exchanged(pieces, PLANE)
    (pieces,) = call(spread_sum_body, [(lax.axis_size("gx"), count, width)], received)
    received = exchanged(pieces, "gx")
    (pieces,) = call(spread_sum_body, [(plane_peers, count, width)], received)
    received = exchanged(pieces, PLANE)
    top_back, second_gap, first_gap, leaf_gap = call(
        functools.partial(top_back_body, used, top_inverse.shape),
        [(count, top_size), (count, second_size), (count, first_size), (count, leaf_size)],
        received,
        folds,
        top_below,
        second_own,
        first_own,
        leaf_solved,
        pack,
    )
    second_whole = jnp.moveaxis(sent_to_all(second_gap, PLANE), 0, 1).reshape(count, -1)
    sent, base, second_back = call(
        functools.partial(second_back_body, sizes, side),
        [(count, 128), (count, leaf_size), (count, second_size)],
        second_whole,
        beside,
        second_below,
        first_gap,
        leaf_gap,
        top_back,
        pack,
    )
    received = sent_to_all(sent, "gz")
    (window,) = call(
        functools.partial(leaf_back_body, sizes, side),
        [(side, 8, lanes)],
        received,
        base,
        second_back,
        top_back,
        pack,
        up,
        first_below,
        first_above,
    )
    after_x = shifted(window[0], "gx", -1)
    layer = jnp.concatenate([window[:, 0], after_x[0:1]], axis=0)
    after_y = shifted(layer, "gy", -1)
    return prolonged(window, after_x, after_y, count, fine)


def solution(mesh):
    blocks = P("gx", "gy", "gz")
    return jax.shard_map(
        per_device,
        mesh=mesh,
        in_specs=(
            P(None, "gx", "gy", "gz"),
            P(None, "gx", "gy", "gz"),
            blocks,
            blocks,
            blocks,
            blocks,
            blocks,
            blocks,
            blocks,
            blocks,
            blocks,
            P("gx", PLANE, None),
            blocks,
            P(("gx", "gy", "gz"), None),
        ),
        out_specs=P(None, "gx", "gy", "gz"),
        check_vma=False,
    )
```
